128 devices in a mesh: seq: 64 (over y, z_hi, x, core), tp: 2 (over z_lo).
Axes of the slice: x: 4, y: 4, z: 4 (z_hi: 2, z_lo: 2; z = z_hi * 2 + z_lo), core: 2. Of those that a mesh axis runs over, the one named last changes fastest.
Arguments:
- query_rows: bfloat16 [8192, 2048], P('seq', 'tp'), may hold values from -350 to 350
- key_rows: bfloat16 [8192, 512], P('seq', 'tp'), may hold values from -6 to 6
- stored_value_rows: bfloat16 [8192, 512], P('seq', 'tp'), may hold values from -6 to 6
- output_grad: bfloat16 [8192, 2048], P('seq', 'tp'), may hold values from -96 to 96
- layer_input: bfloat16 [8192, 4096], P('seq', 'tp'), may hold values from -16 to 16
- key_matrix: bfloat16 [4096, 512], P(None, 'tp'), may hold values from -0.09375 to 0.09375
- value_matrix: bfloat16 [4096, 512], P(None, 'tp'), may hold values from -0.09375 to 0.09375
- run_placement: int32 [64, 64], replicated, may hold values from 0 to 63, as said below
Outputs:
- query_grad: bfloat16 [8192, 2048], P('seq', 'tp')
- input_grad: bfloat16 [8192, 4096], P('seq', 'tp')
- key_weight_grad: float32 [4096, 512], P('seq', 'tp')
- value_weight_grad: float32 [4096, 512], P('seq', 'tp')
The draws below stay inside these ranges and needn't reach their ends.
Inputs may be any that keep to these rules, and one draw needn't show every extreme that they name: `run_placement`: row j gives, for each storing index d of seq, the slot within sequence block j of the 2 consecutive positions that d holds; every row is a permutation of 0 to 63.
All inputs are finite; a program needn't handle non-finite values.
Results may differ from the reference program's by a relative error of at most 0.0081.
Values may be sent and summed in bfloat16 or wider, within the bound.
A program may use at most 128 MiB of HBM per device.

```python
import math
import jax
import jax.numpy as jnp
from jax import lax

MODEL_WIDTH = 4096
HEAD_SIZE = 128
WINDOW_LENGTH = 4096
QUERY_HEADS = 16
KEY_VALUE_HEADS = 4
TOK_DEV = 128
SEQUENCE_TOKENS = 8192
N_SEQ = 64


def slot_table(key):
    row_keys = jax.random.split(jax.random.fold_in(key, 101), N_SEQ)
    return jax.vmap(lambda row_key: jax.random.permutation(row_key, N_SEQ))(row_keys).astype(jnp.int32)


def key_sample(key):
    start_offset = jnp.clip(jax.random.normal(jax.random.fold_in(key, 202), (SEQUENCE_TOKENS, KEY_VALUE_HEADS, HEAD_SIZE), jnp.float32), -4.0, 4.0)
    return start_offset


def draw_run_placement(key, part):
    return slot_table(key)


def draw_key_rows(key, part):
    return key_sample(key).reshape(SEQUENCE_TOKENS, KEY_VALUE_HEADS * HEAD_SIZE).astype(jnp.bfloat16)


def draw_query_rows(key, part):
    start_offset = jnp.clip(jax.random.normal(jax.random.fold_in(key, 303), (SEQUENCE_TOKENS, QUERY_HEADS * HEAD_SIZE), jnp.float32), -4.0, 4.0)
    return start_offset.astype(jnp.bfloat16)


def spiked(drawn, key, source, target, parts, factor):
    owner, partner = [(jnp.arange(drawn.shape[dim]) // (drawn.shape[dim] // parts)).reshape([-1 if axis == dim else 1 for axis in range(drawn.ndim)]) for dim in (source, target)]
    chosen = jax.random.permutation(key, parts)[partner]
    strong = (owner == chosen) | (owner == (partner + parts // 2) % parts)
    return jnp.where(strong, factor * drawn, drawn)


def level_of(own_key, dims, shards, low, largest):
    def one(dim, blocks):
        steps = jax.random.uniform(jax.random.fold_in(jax.random.fold_in(own_key, 6), dim), (blocks,), jnp.float32, low / len(shards), largest / len(shards))
        return jnp.repeat(jnp.exp(steps), dims[dim] // blocks).reshape((-1,) + (1,) * (len(dims) - dim - 1))

    level = one(*shards[0])
    for cut in shards[1:]:
        level = level * one(*cut)
    return level


def normal_values(key, dims, width, reach, cuts=(), kind=jnp.bfloat16):
    drawn = width * jax.random.normal(key, dims, jnp.float32)
    if cuts:
        drawn = drawn * level_of(key, dims, cuts, -0.22, 0.18)
    return jnp.clip(drawn, -reach, reach).astype(kind)


def gaussian_with(rng, extent, scale, bound, cuts, heavy, held_as=jnp.bfloat16):
    array = scale * jax.random.normal(rng, extent, jnp.float32)
    if cuts:
        array = array * level_of(rng, extent, cuts, -0.22, 0.18)
    return jnp.clip(spiked(array, jax.random.fold_in(rng, 3), *heavy), -bound, bound).astype(held_as)


def setup_inputs(seed: int = 0) -> dict:
    key_list = jax.random.split(jax.random.key(seed), 9)
    return {
        "query_rows": draw_query_rows(jax.random.fold_in(key_list[8], 71), 0),
        "key_rows": draw_key_rows(jax.random.fold_in(key_list[8], 71), 0),
        "stored_value_rows": normal_values(key_list[2], (SEQUENCE_TOKENS, KEY_VALUE_HEADS * HEAD_SIZE), 1.0, 6.0, ((0, 64), (1, 2))),
        "output_grad": normal_values(key_list[3], (SEQUENCE_TOKENS, QUERY_HEADS * HEAD_SIZE), 16.0, 96.0, ((0, 64), (1, 2))),
        "layer_input": gaussian_with(key_list[4], (SEQUENCE_TOKENS, MODEL_WIDTH), 1.0, 16.0, ((0, 64), (1, 2)), (0, 1, 64, 4.0)),
        "key_matrix": normal_values(key_list[5], (MODEL_WIDTH, KEY_VALUE_HEADS * HEAD_SIZE), MODEL_WIDTH ** -0.5, 0.09375, ((1, 2),)),
        "value_matrix": normal_values(key_list[6], (MODEL_WIDTH, KEY_VALUE_HEADS * HEAD_SIZE), MODEL_WIDTH ** -0.5, 0.09375, ((1, 2),)),
        "run_placement": draw_run_placement(jax.random.fold_in(key_list[8], 71), 0),
    }


masked_value = -1e+30

def to_sequence(matrix, run_placement):
    run_rows = TOK_DEV // N_SEQ
    columns = matrix.shape[1]
    stored = matrix.reshape(N_SEQ, N_SEQ, run_rows, columns).transpose(1, 0, 2, 3)
    inverse = jnp.argsort(run_placement, axis=1).astype(jnp.int32)
    picked = jnp.take_along_axis(stored, inverse[:, :, None, None], axis=1)
    return picked.reshape(SEQUENCE_TOKENS, columns)

def into_stored_order(matrix, run_placement):
    run_rows = TOK_DEV // N_SEQ
    columns = matrix.shape[1]
    blocks = matrix.reshape(N_SEQ, N_SEQ, run_rows, columns)
    picked = jnp.take_along_axis(blocks, run_placement.astype(jnp.int32)[:, :, None, None], axis=1)
    return picked.transpose(1, 0, 2, 3).reshape(SEQUENCE_TOKENS, columns)

def rounded(values):
    return lax.optimization_barrier(values.astype(jnp.bfloat16)).astype(jnp.float32)

def reference(query_rows, key_rows, stored_value_rows, output_grad, layer_input, key_matrix, value_matrix, run_placement):
    score_scale = 1.0 / math.sqrt(HEAD_SIZE)
    query_group = QUERY_HEADS // KEY_VALUE_HEADS
    queries = to_sequence(query_rows, run_placement)
    grads = to_sequence(output_grad, run_placement)
    empty_rows = jnp.zeros((WINDOW_LENGTH, KEY_VALUE_HEADS * HEAD_SIZE), jnp.bfloat16)
    padded_keys = jnp.concatenate([empty_rows, to_sequence(key_rows, run_placement)], axis=0)
    padded_values = jnp.concatenate([empty_rows, to_sequence(stored_value_rows, run_placement)], axis=0)
    window_keys = WINDOW_LENGTH + TOK_DEV

    def one_block(carry, block_index):
        leading_row = block_index * TOK_DEV
        q_block = lax.dynamic_slice_in_dim(queries, leading_row, TOK_DEV, 0).astype(jnp.float32).reshape(TOK_DEV, QUERY_HEADS, HEAD_SIZE)
        g_block = lax.dynamic_slice_in_dim(grads, leading_row, TOK_DEV, 0).astype(jnp.float32).reshape(TOK_DEV, QUERY_HEADS, HEAD_SIZE)
        key_block = lax.dynamic_slice_in_dim(padded_keys, leading_row, window_keys, 0).astype(jnp.float32).reshape(window_keys, KEY_VALUE_HEADS, HEAD_SIZE)
        value_block = lax.dynamic_slice_in_dim(padded_values, leading_row, window_keys, 0).astype(jnp.float32).reshape(window_keys, KEY_VALUE_HEADS, HEAD_SIZE)
        k_heads = jnp.repeat(key_block, query_group, axis=1)
        v_heads = jnp.repeat(value_block, query_group, axis=1)
        query_pos = leading_row + jnp.arange(TOK_DEV, dtype=jnp.int32)
        key_pos = leading_row - WINDOW_LENGTH + jnp.arange(window_keys, dtype=jnp.int32)
        in_window = (key_pos[None, :] <= query_pos[:, None]) & (key_pos[None, :] > query_pos[:, None] - WINDOW_LENGTH) & (key_pos[None, :] >= 0)
        logits = jnp.einsum('qhd,khd->hqk', q_block, k_heads) * score_scale
        row_top = lax.optimization_barrier(jnp.max(jnp.where(in_window[None], logits, masked_value), axis=2))
        exponent = jnp.where(in_window[None], jnp.exp(logits - row_top[:, :, None]), 0.0)
        row_total = lax.optimization_barrier(jnp.sum(exponent, axis=2))
        log_total = row_top + jnp.log(row_total)
        prob_grad = jnp.einsum('qhd,khd->hqk', g_block, v_heads)
        row_delta = lax.optimization_barrier(jnp.sum(exponent * prob_grad, axis=2)) / row_total
        probs = jnp.where(in_window[None], jnp.exp(logits - log_total[:, :, None]), 0.0)
        score_grad = probs * (prob_grad - row_delta[:, :, None])
        probs_b = rounded(probs)
        score_b = rounded(score_grad)
        query_part = (jnp.einsum('hqk,khd->qhd', score_b, k_heads) * score_scale).astype(jnp.bfloat16)
        key_portion = jnp.einsum('hqk,qhd->khd', score_b, q_block) * score_scale
        key_portion = key_portion.reshape(window_keys, KEY_VALUE_HEADS, query_group, HEAD_SIZE).sum(axis=2).reshape(window_keys, KEY_VALUE_HEADS * HEAD_SIZE)
        value_portion = jnp.einsum('hqk,qhd->khd', probs_b, g_block)
        value_portion = value_portion.reshape(window_keys, KEY_VALUE_HEADS, query_group, HEAD_SIZE).sum(axis=2).reshape(window_keys, KEY_VALUE_HEADS * HEAD_SIZE)
        update = jnp.concatenate([key_portion, value_portion], axis=1)
        current = lax.dynamic_slice_in_dim(carry, leading_row, window_keys, 0)
        carry = lax.dynamic_update_slice_in_dim(carry, current + update, leading_row, 0)
        return (carry, query_part.reshape(TOK_DEV, QUERY_HEADS * HEAD_SIZE))
    gradient_start = jnp.zeros((WINDOW_LENGTH + SEQUENCE_TOKENS, 2 * KEY_VALUE_HEADS * HEAD_SIZE), jnp.float32)
    final, query_parts = lax.scan(one_block, gradient_start, jnp.arange(N_SEQ, dtype=jnp.int32))
    key_value_pair = final[WINDOW_LENGTH:]
    key_gradient = into_stored_order(key_value_pair[:, :KEY_VALUE_HEADS * HEAD_SIZE].astype(jnp.bfloat16), run_placement)
    value_gradient = into_stored_order(key_value_pair[:, KEY_VALUE_HEADS * HEAD_SIZE:].astype(jnp.bfloat16), run_placement)
    query_grad = into_stored_order(query_parts.reshape(SEQUENCE_TOKENS, QUERY_HEADS * HEAD_SIZE), run_placement)
    key_weight_grad = jnp.dot(layer_input.T, key_gradient, preferred_element_type=jnp.float32)
    value_weight_grad = jnp.dot(layer_input.T, value_gradient, preferred_element_type=jnp.float32)
    input_grad = jnp.dot(key_gradient, key_matrix.T, preferred_element_type=jnp.float32)
    input_grad = (input_grad + jnp.dot(value_gradient, value_matrix.T, preferred_element_type=jnp.float32)).astype(jnp.bfloat16)
    return (query_grad, input_grad, key_weight_grad, value_weight_grad)
```

```python
import math

import jax
import jax.numpy as jnp
from jax import lax
from jax.experimental import pallas as pl
from jax.experimental.pallas import tpu as pltpu
from jax.sharding import Mesh
from jax.sharding import PartitionSpec as P

F32 = jnp.float32
BF16 = jnp.bfloat16
Y, ZH, X, CORE, ZL = "seq_0", "seq_1", "seq_2", "seq_3", "tp"
SEQ = (Y, ZH, X, CORE)
MESH = pl.DeviceIdType.MESH

HEAD = 128
GROUP = 4
WINDOW = 4096
CHUNKS = 8
BAND = 4
FEATS = 4096
SCALE = 1.0 / math.sqrt(HEAD)
SCALE2 = SCALE * math.log2(math.e)
MASKED = -1e30
QROWS = 256
KROWS = 128
NSEM = 96
NLOCAL = 24


def key_chunks(cq):
    return list(range(max(0, cq - BAND), cq + 1))


TILE_AT = [KROWS * sum(len(key_chunks(c)) for c in range(cq)) for cq in range(CHUNKS)]
TILE_ROWS = KROWS * sum(len(key_chunks(c)) for c in range(CHUNKS))

UNIT_KV = (2, 4, 2, 16, HEAD)
UNIT_W = (2, 64, HEAD)


def reduce_buffers(name, unit):
    half = unit[1:]
    return {
        name + "_far": ((2, 4) + unit, BF16),
        name + "_rfar": ((2, 2, 2) + unit, BF16),
        name + "_near": ((2, 2, 4) + unit, BF16),
        name + "_rnear": ((2, 2, 4) + unit, BF16),
        name + "_row": ((2, 4) + unit, F32),
        name + "_far2": ((2,) + unit, BF16),
        name + "_rfar2": ((2, 2) + half, BF16),
        name + "_near2": ((2, 2) + unit, BF16),
        name + "_rnear2": ((2, 2) + unit, BF16),
    }


BUFFERS = {
    "kv": ((2, 4, 4) + UNIT_KV, BF16),
    "qg": ((2, CHUNKS, 4, GROUP, 16, HEAD), BF16),
    "kpb": ((32, KROWS, 128), F32),
    "e": ((4, TILE_ROWS, QROWS), F32),
    "dp": ((4, TILE_ROWS, QROWS), F32),
    "st": ((3, 4, CHUNKS, QROWS), F32),
    "ss": ((3, CHUNKS, QROWS), F32),
    "sr": ((3, CHUNKS, QROWS), F32),
    "fac": ((4, CHUNKS, QROWS), F32),
    "delta": ((CHUNKS, QROWS), F32),
    "acc": ((2, 4) + UNIT_KV, F32),
    "dqt": ((CHUNKS, HEAD, QROWS), F32),
    "dqf": ((CHUNKS, 2, 2, GROUP, 16, HEAD), F32),
    "dqr": ((CHUNKS, 2, GROUP, 16, HEAD), F32),
    "dqs": ((CHUNKS, GROUP, 16, HEAD), BF16),
    "dqz": ((CHUNKS, GROUP, 16, HEAD), BF16),
    "xg": ((CHUNKS, 2, 16, FEATS), BF16),
    "mat": ((2, FEATS, 2 * HEAD), BF16),
    "d2": ((2, CHUNKS, 2, 16, HEAD), BF16),
    "dd": ((4, CHUNKS, 16, HEAD), BF16),
    "wown": ((2, 4, 4) + UNIT_W, F32),
    "wsend": ((2, 4, 4) + UNIT_W, BF16),
    "wrecv": ((2, 4, 4) + UNIT_W, BF16),
    "wfin": ((2,) + UNIT_W, F32),
    "wswap": ((2, 64, HEAD), F32),
    "igs": ((128, FEATS // 2), BF16),
    "igr": ((128, FEATS // 2), BF16),
    "igo": ((128, FEATS // 2), F32),
    **reduce_buffers("a", UNIT_KV),
    **reduce_buffers("w", UNIT_W),
}


def dot_tt(a, b):
    return lax.dot_general(a, b, (((1,), (1,)), ((), ())), preferred_element_type=F32)


def dot_nn(a, b):
    return lax.dot_general(a, b, (((1,), (0,)), ((), ())), preferred_element_type=F32)


def dot_tn(a, b):
    return lax.dot_general(a, b, (((0,), (0,)), ((), ())), preferred_element_type=F32)


def stack_rows(parts):
    return parts[0] if len(parts) == 1 else jnp.concatenate(parts, axis=0)


def kernel(
    q_in, g_in, k_in, v_in, x_in, mk_in, mv_in, kp_in, qp_in, dq_out, ig_out, w_out, *scratch
):
    ssem, rsem, lsem = scratch[-3:]
    b = dict(zip(BUFFERS, scratch[:-3]))
    y, zh, x, core, zl = (lax.axis_index(a) for a in (Y, ZH, X, CORE, ZL))

    def turn(i, by):
        return lax.rem(i + by, 4)

    z = 2 * zh + zl
    zp, zm = turn(z, 1), turn(z, 3)
    zp_h, zp_l = lax.div(zp, 2), lax.rem(zp, 2)
    zm_h, zm_l = lax.div(zm, 2), lax.rem(zm, 2)
    oh, oc, ol = 1 - zh, 1 - core, 1 - zl
    d_zh, d_core, d_tp = {ZH: oh}, {CORE: oc}, {ZL: ol}
    d_zp, d_zm = {ZH: zp_h, ZL: zp_l}, {ZH: zm_h, ZL: zm_l}
    step_of = {a: ({a: turn(i, 1)}, {a: turn(i, 3)}) for a, i in ((X, x), (Y, y))}
    qi, pi = (y, x), (x, y)
    q_to = (step_of[Y], step_of[X])
    p_to = (step_of[X], step_of[Y])

    names = {}
    pending = []

    def remote(name, src, dst, dev):
        i = names.setdefault(name, len(names))
        return pltpu.make_async_remote_copy(
            src_ref=src,
            dst_ref=dst,
            send_sem=ssem.at[i],
            recv_sem=rsem.at[i],
            device_id=dev,
            device_id_type=MESH,
        )

    def send(name, src, dst, dev):
        remote(name, src, dst, dev).start()
        pending.append((name, src, dst, dev))

    def arrived(name, dst):
        remote(name, dst, dst, d_core).wait_recv()

    local_names = {}

    def local(name, src, dst):
        i = local_names.setdefault(name, len(local_names))
        return pltpu.make_async_copy(src, dst, lsem.at[i])

    def lanes(start, width=128):
        return pl.ds(pl.multiple_of(start, 128), width)

    kv, qg, xg, mat = b["kv"], b["qg"], b["xg"], b["mat"]
    own_kv = []
    for h in range(2):
        for t, ref in enumerate((k_in, v_in)):
            own_kv.append(
                local(
                    ("kv", h, t),
                    ref.at[pl.ds(4 * h, 4), :, lanes(zh * HEAD)],
                    kv.at[h, qi[h], pi[h], t, :, zh],
                )
            )
    own_q = []
    for t, ref in enumerate((q_in, g_in)):
        for g in range(GROUP):
            own_q.append(
                local(
                    ("qg", t, g),
                    ref.at[:, :, lanes(zh * GROUP * HEAD + g * HEAD)],
                    qg.at[t, :, 2 * zh + core, g],
                )
            )
    own_x = local("x", x_in, xg.at[:, zh, :, lanes(zl * (FEATS // 2), FEATS // 2)])
    own_m = [local("mk", mk_in, mat.at[0]), local("mv", mv_in, mat.at[1])]
    for c in own_kv + own_q:
        c.start()

    barrier = pltpu.get_barrier_semaphore()
    peers = [d_zh, d_core, *step_of[X], *step_of[Y], d_zp, d_zm]
    for dev in peers:
        pl.semaphore_signal(barrier, inc=1, device_id=dev, device_id_type=MESH)
    pl.semaphore_wait(barrier, len(peers))

    for h in range(2):
        for t, ref in enumerate((k_in, v_in)):
            send(
                ("zkv", h, t),
                ref.at[pl.ds(4 * h, 4), :, lanes(oh * HEAD)],
                kv.at[h, qi[h], pi[h], t, :, zh],
                d_zh,
            )
    for t, ref in enumerate((q_in, g_in)):
        for g in range(GROUP):
            send(
                ("qz", t, g),
                ref.at[:, :, lanes(oh * GROUP * HEAD + g * HEAD)],
                qg.at[t, :, 2 * zh + core, g],
                d_zh,
            )
    for t, ref in enumerate((q_in, g_in)):
        for g in range(GROUP):
            send(
                ("qc", t, g),
                ref.at[:, :, lanes(zh * GROUP * HEAD + g * HEAD)],
                qg.at[t, :, 2 * zh + core, g],
                d_core,
            )
    for c in own_kv:
        c.wait()

    for h in range(2):
        for t in range(2):
            arrived(("zkv", h, t), kv.at[h, qi[h], pi[h], t, :, oh])
        for side in range(2):
            unit = kv.at[h, qi[h], pi[h]]
            send(("p", h, side), unit, unit, p_to[h][side])
    own_x.start()
    for c in own_m:
        c.start()
    dqt = b["dqt"]
    dqt[...] = jnp.zeros(dqt.shape, F32)
    kpt = kp_in[...].T
    for i in range(32):
        b["kpb"][i] = jnp.broadcast_to(kpt[:, i : i + 1], (KROWS, 128))
    for h in range(2):
        for side in range(2):
            src = kv.at[h, qi[h], turn(pi[h], 3 if side == 0 else 1)]
            arrived(("p", h, side), src)
            send(("pf", h, side), src.at[side], src.at[side], p_to[h][side])
    for h in range(2):
        for side in range(2):
            arrived(("pf", h, side), kv.at[h, qi[h], turn(pi[h], 2), side])
        for side in range(2):
            row = kv.at[h, qi[h]]
            send(("q", h, side), row, row, q_to[h][side])

    for t in range(2):
        for g in range(GROUP):
            arrived(("qz", t, g), qg.at[t, :, 2 * oh + core, g])
        src = qg.at[t, :, 2 * oh + core]
        send(("qf", t), src, src, d_core)
    half_feats = FEATS // 2
    quarter_feats = FEATS // 4
    mine = xg.at[:, zh, :, lanes(zl * half_feats, half_feats)]
    send("x+", x_in, mine, d_zp)
    send("x-", x_in, mine, d_zm)
    for c in own_q:
        c.wait()
    for t in range(2):
        for g in range(GROUP):
            arrived(("qc", t, g), qg.at[t, :, 2 * zh + oc, g])
        arrived(("qf", t), qg.at[t, :, 2 * oh + oc])

    def queries(t, cq):
        return qg[t, cq].reshape(QROWS, HEAD)

    def keys(t, at, cks):
        return stack_rows(
            [kv[ck // 4, at[ck // 4], :, t, ck % 4].reshape(KROWS, HEAD) for ck in cks]
        )

    def row_far(h, side):
        return kv.at[h, turn(qi[h], 2), pl.ds(2 * side, 2)]

    def row_near(h, side):
        return kv.at[h, turn(qi[h], 3 if side == 0 else 1)]

    def forward(h, side):
        src = row_near(h, side).at[pl.ds(2 * side, 2)]
        return ("qfar", h, side), src, src, q_to[h][side]

    st, e_ref, dp_ref = b["st"], b["e"], b["dp"]

    def first_pass(s, carry):
        late = lax.div(s, 2)
        off = (1 - late) * s + late * (5 - s)

        @pl.when(s == 1)
        def _():
            for h in range(2):
                for side in range(2):
                    arrived(("q", h, side), row_near(h, side))
                    remote(*forward(h, side)).start()

        @pl.when(s == 3)
        def _():
            for h in range(2):
                for side in range(2):
                    arrived(("qfar", h, side), row_far(h, side))

        at = (turn(y, off), turn(x, off))
        for cq in range(CHUNKS):
            cks = key_chunks(cq)
            rows = pl.ds(TILE_AT[cq], KROWS * len(cks))
            score = dot_tt(keys(0, at, cks), queries(0, cq)) * SCALE2
            qpos = qp_in[cq : cq + 1, :]
            parts = []
            for n, ck in enumerate(cks):
                part = score[n * KROWS : (n + 1) * KROWS]
                if ck == cq or ck == cq - BAND:
                    kpb = b["kpb"][ck // 4 * 16 + at[ck // 4] * 4 + ck % 4]
                    kpos = jnp.concatenate([kpb, kpb], axis=1)
                    seen = kpos <= qpos if ck == cq else kpos > qpos - WINDOW
                    part = jnp.where(seen, part, MASKED)
                parts.append(part)
            score = stack_rows(parts)
            top = jnp.max(score, axis=0, keepdims=True)
            expo = jnp.exp2(score - top)
            dprob = dot_tt(keys(1, at, cks), queries(1, cq))
            e_ref[off, rows, :] = expo
            dp_ref[off, rows, :] = dprob
            st[0, off, cq : cq + 1, :] = top
            st[1, off, cq : cq + 1, :] = jnp.sum(expo, axis=0, keepdims=True)
            st[2, off, cq : cq + 1, :] = jnp.sum(expo * dprob, axis=0, keepdims=True)
        return carry

    lax.fori_loop(0, 4, first_pass, 0)
    for h in range(2):
        for side in range(2):
            pending.append(forward(h, side))

    ss, sr = b["ss"], b["sr"]
    top_l = jnp.max(st[0], axis=0)
    fac_l = jnp.exp2(st[0] - top_l[None])
    sum_l = jnp.sum(st[1] * fac_l, axis=0)
    wgt_l = jnp.sum(st[2] * fac_l, axis=0)
    ss[0] = top_l
    ss[1] = sum_l
    ss[2] = wgt_l
    send("stat", ss, sr, d_core)
    arrived("x+", xg.at[:, zm_h, :, lanes(zm_l * half_feats, half_feats)])
    src = xg.at[:, zm_h, :, lanes(zm_l * half_feats, quarter_feats)]
    send("xf+", src, src, d_zp)
    arrived("x-", xg.at[:, zp_h, :, lanes(zp_l * half_feats, half_feats)])
    src = xg.at[:, zp_h, :, lanes(zp_l * half_feats + quarter_feats, quarter_feats)]
    send("xf-", src, src, d_zm)
    arrived("stat", sr)
    top = jnp.maximum(top_l, sr[0])
    mine_f = jnp.exp2(top_l - top)
    other_f = jnp.exp2(sr[0] - top)
    total = sum_l * mine_f + sr[1] * other_f
    b["delta"][...] = (wgt_l * mine_f + sr[2] * other_f) / total
    b["fac"][...] = fac_l * (mine_f / total)[None]

    def reducer(name, row):
        far, rfar = b[name + "_far"], b[name + "_rfar"]
        near, rnear = b[name + "_near"], b[name + "_rnear"]
        rows = b[name + "_row"]
        far2, rfar2 = b[name + "_far2"], b[name + "_rfar2"]
        near2, rnear2 = b[name + "_near2"], b[name + "_rnear2"]

        def far_copy(h, side):
            return (
                (name, "far", h, side),
                far.at[h, pl.ds(2 * side, 2)],
                rfar.at[h, side],
                q_to[h][side],
            )

        def near_copy(h, side):
            return (name, "near", h, side), near.at[h, side], rnear.at[h, side], q_to[h][side]

        def start_far():
            for h in range(2):
                far[h] = row(h, turn(qi[h], 2)).astype(BF16)
                for side in range(2):
                    remote(*far_copy(h, side)).start()

        def start_near(side):
            for h in range(2):
                value = row(h, turn(qi[h], 1 if side == 0 else 3))
                arrived((name, "far", h, side), rfar.at[h, side])
                lo, hi = value[:2], value[2:]
                if side == 0:
                    lo = lo + rfar[h, side].astype(F32)
                else:
                    hi = hi + rfar[h, side].astype(F32)
                near[h, side, :2] = lo.astype(BF16)
                near[h, side, 2:] = hi.astype(BF16)
                remote(*near_copy(h, side)).start()

        def note_sends():
            for h in range(2):
                for side in range(2):
                    pending.append(far_copy(h, side))
                    pending.append(near_copy(h, side))

        def own_row():
            for h in range(2):
                for side in range(2):
                    arrived((name, "near", h, side), rnear.at[h, side])
                rows[h] = row(h, qi[h]) + rnear[h, 0].astype(F32) + rnear[h, 1].astype(F32)
                far2[h] = rows[h, turn(pi[h], 2)].astype(BF16)
                for side in range(2):
                    send(
                        (name, "far2", h, side),
                        far2.at[h, side],
                        rfar2.at[h, side],
                        p_to[h][side],
                    )

        def near_unit():
            for h in range(2):
                for side in range(2):
                    arrived((name, "far2", h, side), rfar2.at[h, side])
                    at = turn(pi[h], 1 if side == 0 else 3)
                    near2[h, side, 1 - side] = rows[h, at, 1 - side].astype(BF16)
                    near2[h, side, side] = (
                        rows[h, at, side] + rfar2[h, side].astype(F32)
                    ).astype(BF16)
                    send(
                        (name, "near2", h, side), near2.at[h, side], rnear2.at[h, side], p_to[h][side]
                    )

        def final(h):
            for side in range(2):
                arrived((name, "near2", h, side), rnear2.at[h, side])
            return rows[h, pi[h]] + rnear2[h, 0].astype(F32) + rnear2[h, 1].astype(F32)

        return start_far, start_near, note_sends, own_row, near_unit, final

    acc = b["acc"]
    start_far, start_near, note_sends, own_row, near_unit, final = reducer(
        "a", lambda h, at: acc[h]
    )

    fac, delta = b["fac"], b["delta"]

    def second_pass(s, carry):
        late = lax.div(s, 2)
        off = (1 - late) * (2 + s) + late * (3 - s)
        at = (turn(y, off), turn(x, off))
        for cq in range(CHUNKS):
            cks = key_chunks(cq)
            rows = pl.ds(TILE_AT[cq], KROWS * len(cks))
            prob = e_ref[off, rows, :] * fac[off, cq : cq + 1, :]
            dscore = (prob * (dp_ref[off, rows, :] - delta[cq : cq + 1, :])).astype(BF16)
            grads = (dot_nn(dscore, queries(0, cq)), dot_nn(prob.astype(BF16), queries(1, cq)))
            for t in range(2):
                for n, ck in enumerate(cks):
                    part = grads[t][n * KROWS : (n + 1) * KROWS].reshape(4, 2, 16, HEAD)
                    if ck == cq:
                        acc[ck // 4, :, t, ck % 4] = part
                    else:
                        acc[ck // 4, :, t, ck % 4] = acc[ck // 4, :, t, ck % 4] + part
            dqt[cq] = dqt[cq] + dot_tn(keys(0, at, cks), dscore)

        @pl.when(s == 0)
        def _():
            start_far()

        @pl.when(s == 1)
        def _():
            start_near(1)

        @pl.when(s == 2)
        def _():
            start_near(0)

        return carry

    lax.fori_loop(0, 4, second_pass, 0)
    note_sends()

    dqf, dqr, dqs, dqz = b["dqf"], b["dqr"], b["dqs"], b["dqz"]
    for cq in range(CHUNKS):
        dqf[cq] = (dqt[cq].T * SCALE).reshape(2, 2, GROUP, 16, HEAD)
    send("dqc", dqf.at[:, :, oc], dqr, d_core)
    own_row()
    arrived("dqc", dqr)
    dqs[...] = (dqf[:, oh, core] + dqr[:, oh]).astype(BF16)
    send("dqz", dqs, dqz, d_zh)
    dq_out[zh] = (dqf[:, zh, core] + dqr[:, zh]).astype(BF16)
    near_unit()
    own_x.wait()
    for c in own_m:
        c.wait()
    far_h = 1 - zh
    arrived("xf+", xg.at[:, far_h, :, lanes(zl * half_feats, quarter_feats)])
    arrived("xf-", xg.at[:, far_h, :, lanes(zl * half_feats + quarter_feats, quarter_feats)])
    arrived("dqz", dqz)
    dq_out[oh] = dqz[...]
    d2, dd = b["d2"], b["dd"]
    for h in range(2):
        value = final(h)
        d2[0, 4 * h : 4 * h + 4] = (value[0] * SCALE).astype(BF16)
        d2[1, 4 * h : 4 * h + 4] = value[1].astype(BF16)
    for t in range(2):
        send(("dz", t), d2.at[t, :, oh], dd.at[2 * t + zh], d_zh)
        dd[2 * t + zh] = d2[t, :, zh]

    wown, wsend, wrecv = b["wown"], b["wsend"], b["wrecv"]
    grad_cols = jnp.concatenate([d2[0].reshape(256, HEAD), d2[1].reshape(256, HEAD)], axis=1)

    def weight_block(i, carry):
        wx = lax.rem(i, 4)
        wz = lax.rem(lax.div(i, 4), 2)
        wy = lax.div(i, 8)
        block = xg[:, :, :, lanes(i * 128)].reshape(256, 128)
        part = dot_tn(block, grad_cols)
        for h, (wq, wp) in enumerate(((wy, wx), (wx, wy))):
            cols = part[:, h * HEAD : (h + 1) * HEAD]
            wown[h, wq, wp, wz] = jnp.where(core == 0, cols[:64], cols[64:])
            wsend[h, wq, wp, wz] = jnp.where(core == 0, cols[64:], cols[:64]).astype(BF16)
        return carry

    lax.fori_loop(0, 32, weight_block, 0)
    send("wc", wsend, wrecv, d_core)

    igs, igr, igo = b["igs"], b["igr"], b["igo"]
    for t in range(2):
        arrived(("dz", t), dd.at[2 * t + oh])
    dk_dv = [
        jnp.concatenate([dd[2 * t].reshape(128, HEAD), dd[2 * t + 1].reshape(128, HEAD)], axis=1)
        for t in range(2)
    ]

    def input_block(base, out):
        def body(i, carry):
            rows = pl.ds(pl.multiple_of(base + i * 512, 512), 512)
            part = dot_tt(dk_dv[0], mat[0, rows, :]) + dot_tt(dk_dv[1], mat[1, rows, :])
            out[:, lanes(i * 512, 512)] = part.astype(out.dtype)
            return carry

        lax.fori_loop(0, 4, body, 0)

    input_block(ol * half_feats, igs)
    send("ig", igs, igr, d_tp)

    arrived("wc", wrecv)
    w_far, w_near, w_note, w_own, w_unit, w_final = reducer(
        "w", lambda h, at: wown[h, at] + wrecv[h, at].astype(F32)
    )
    w_far()
    input_block(zl * half_feats, igo)
    w_near(0)
    w_near(1)
    w_note()
    w_own()
    w_unit()
    wfin, wswap = b["wfin"], b["wswap"]
    for h in range(2):
        wfin[h] = w_final(h)
    for h in range(2):
        send(("ws", h), wfin.at[h, oh], wswap.at[h], d_zh)
        w_out[h, zh] = wfin[h, zh]
    arrived("ig", igr)
    ig_out[...] = (igo[...] + igr[...].astype(F32)).astype(BF16)
    for h in range(2):
        arrived(("ws", h), wswap.at[h])
        w_out[h, oh] = wswap[h]

    for copy in pending:
        remote(*copy).wait_send()
    assert len(names) <= NSEM and len(local_names) <= NLOCAL


def local_step(q, k, v, g, x, mk, mv, placement):
    core = lax.axis_index(CORE)
    pos = (
        (jnp.arange(64, dtype=jnp.int32) * 128)[:, None, None]
        + placement[:, :, None] * 2
        + jnp.arange(2, dtype=jnp.int32)
    ).astype(F32)
    pos = pos.reshape(CHUNKS, 8, 4, 2, 4, 2, 2)
    kpos = lax.dynamic_index_in_dim(pos, core, 5, keepdims=False)
    kpos = kpos.reshape(2, 4, 8, 4, 2, 4, 2)
    half_a = kpos[0].transpose(2, 0, 4, 3, 1, 5)
    half_b = kpos[1].transpose(4, 0, 2, 3, 1, 5)
    kp = jnp.stack([half_a, half_b]).reshape(32, KROWS)
    qpos = lax.dynamic_index_in_dim(pos, lax.axis_index(Y), 2, keepdims=False)
    qpos = lax.dynamic_index_in_dim(qpos, lax.axis_index(X), 3, keepdims=False)
    qpos = qpos.transpose(0, 2, 3, 1, 4).reshape(CHUNKS, 4, 1, 16)
    qp = jnp.broadcast_to(qpos, (CHUNKS, 4, GROUP, 16)).reshape(CHUNKS, QROWS)

    anywhere = pl.BlockSpec(memory_space=pl.ANY)
    vmem = pl.BlockSpec(memory_space=pltpu.VMEM)
    dq, ig, w = pl.pallas_call(
        kernel,
        out_shape=(
            jax.ShapeDtypeStruct((2, CHUNKS, GROUP, 16, HEAD), BF16),
            jax.ShapeDtypeStruct((128, FEATS // 2), BF16),
            jax.ShapeDtypeStruct((2, 2, 64, HEAD), F32),
        ),
        in_specs=[anywhere] * 7 + [vmem] * 2,
        out_specs=(vmem, vmem, vmem),
        scratch_shapes=[pltpu.VMEM(shape, dtype) for shape, dtype in BUFFERS.values()]
        + [
            pltpu.SemaphoreType.DMA((NSEM,)),
            pltpu.SemaphoreType.DMA((NSEM,)),
            pltpu.SemaphoreType.DMA((NLOCAL,)),
        ],
        compiler_params=pltpu.CompilerParams(
            collective_id=0, has_side_effects=True, vmem_limit_bytes=67043328
        ),
    )(
        q.reshape(CHUNKS, 16, -1),
        g.reshape(CHUNKS, 16, -1),
        k.reshape(CHUNKS, 16, -1),
        v.reshape(CHUNKS, 16, -1),
        x.reshape(CHUNKS, 16, -1),
        mk,
        mv,
        kp,
        qp,
    )
    query_grad = dq.transpose(1, 3, 0, 2, 4).reshape(128, -1)
    weights = [w[t].transpose(1, 0, 2).reshape(64, 2 * HEAD) for t in range(2)]
    return (query_grad, ig, weights[0], weights[1])


def solution(mesh):
    torus = Mesh(
        mesh.devices.reshape(4, 2, 4, 2, mesh.shape["tp"]), ("seq_0", "seq_1", "seq_2", "seq_3", "tp")
    )
    rows = P(SEQ, "tp")
    return jax.shard_map(
        local_step,
        mesh=torus,
        in_specs=(rows, rows, rows, rows, rows, P(None, "tp"), P(None, "tp"), P()),
        out_specs=(rows, rows, rows, rows),
        check_vma=False,
    )
```

```python
import math

import jax
import jax.numpy as jnp
from jax import lax
from jax.experimental import pallas as pl
from jax.experimental.pallas import tpu as pltpu
from jax.sharding import Mesh
from jax.sharding import PartitionSpec as P

F32 = jnp.float32
BF16 = jnp.bfloat16
Y, ZH, X, CORE, ZL = "seq_0", "seq_1", "seq_2", "seq_3", "tp"
SEQ = (Y, ZH, X, CORE)
MESH = pl.DeviceIdType.MESH

HEAD = 128
GROUP = 4
WINDOW = 4096
CHUNKS = 8
BAND = 4
FEATS = 4096
SCALE = 1.0 / math.sqrt(HEAD)
SCALE2 = SCALE * math.log2(math.e)
MASKED = -1e30
QROWS = 256
KROWS = 128
NSEM = 96
NLOCAL = 24


def key_chunks(cq):
    return list(range(max(0, cq - BAND), cq + 1))


TILE_AT = [KROWS * sum(len(key_chunks(c)) for c in range(cq)) for cq in range(CHUNKS)]
TILE_ROWS = KROWS * sum(len(key_chunks(c)) for c in range(CHUNKS))

UNIT_KV = (2, 4, 2, 16, HEAD)
UNIT_W = (2, 64, HEAD)


def reduce_buffers(name, unit):
    half = unit[1:]
    return {
        name + "_far": ((2, 4) + unit, BF16),
        name + "_rfar": ((2, 2, 2) + unit, BF16),
        name + "_near": ((2, 2, 4) + unit, BF16),
        name + "_rnear": ((2, 2, 4) + unit, BF16),
        name + "_row": ((2, 4) + unit, F32),
        name + "_far2": ((2,) + unit, BF16),
        name + "_rfar2": ((2, 2) + half, BF16),
        name + "_near2": ((2, 2) + unit, BF16),
        name + "_rnear2": ((2, 2) + unit, BF16),
    }


BUFFERS = {
    "kv": ((2, 4, 4) + UNIT_KV, BF16),
    "qg": ((2, CHUNKS, 4, GROUP, 16, HEAD), BF16),
    "kpb": ((32, KROWS, 128), F32),
    "e": ((4, TILE_ROWS, QROWS), F32),
    "dp": ((4, TILE_ROWS, QROWS), F32),
    "st": ((3, 4, BAND + 1, CHUNKS, QROWS), F32),
    "ss": ((3, CHUNKS, QROWS), F32),
    "sr": ((3, CHUNKS, QROWS), F32),
    "fac": ((4, BAND + 1, CHUNKS, QROWS), F32),
    "delta": ((CHUNKS, QROWS), F32),
    "acc": ((2, 4) + UNIT_KV, F32),
    "dqt": ((CHUNKS, HEAD, QROWS), F32),
    "dqf": ((CHUNKS, 2, 2, GROUP, 16, HEAD), F32),
    "dqr": ((CHUNKS, 2, GROUP, 16, HEAD), F32),
    "dqs": ((CHUNKS, GROUP, 16, HEAD), BF16),
    "dqz": ((CHUNKS, GROUP, 16, HEAD), BF16),
    "kt": ((CHUNKS, HEAD, KROWS), BF16),
    "qp": ((CHUNKS, QROWS), F32),
    "xg": ((CHUNKS, 2, 16, FEATS), BF16),
    "xt": ((FEATS, 256), BF16),
    "mat": ((2, FEATS, 2 * HEAD), BF16),
    "d2": ((2, CHUNKS, 2, 16, HEAD), BF16),
    "dd": ((4, CHUNKS, 16, HEAD), BF16),
    "wown": ((2, 4, 4) + UNIT_W, F32),
    "wsend": ((2, 4, 4) + UNIT_W, BF16),
    "wrecv": ((2, 4, 4) + UNIT_W, BF16),
    "wfin": ((2,) + UNIT_W, F32),
    "wswap": ((2, 64, HEAD), F32),
    "igs": ((128, FEATS // 2), BF16),
    "igr": ((128, FEATS // 2), BF16),
    "igo": ((128, FEATS // 2), F32),
    **reduce_buffers("a", UNIT_KV),
    **reduce_buffers("w", UNIT_W),
}


def dot_tt(a, b):
    return lax.dot_general(a, b, (((1,), (1,)), ((), ())), preferred_element_type=F32)


def dot_nn(a, b):
    return lax.dot_general(a, b, (((1,), (0,)), ((), ())), preferred_element_type=F32)


def dot_tn(a, b):
    return lax.dot_general(a, b, (((0,), (0,)), ((), ())), preferred_element_type=F32)


def stack_rows(parts):
    return parts[0] if len(parts) == 1 else jnp.concatenate(parts, axis=0)


def positions(rp_in, kpb, qp, y, x, core):
    slots = rp_in[...].astype(F32).astype(BF16)

    def iota(shape, dim):
        return lax.broadcasted_iota(jnp.int32, shape, dim)

    def bits(a, at, width):
        return jnp.bitwise_and(jnp.right_shift(a, at), (1 << width) - 1)

    row, dev = iota((KROWS, 64), 0), iota((KROWS, 64), 1)
    p, zh, jj = bits(row, 5, 2), bits(row, 4, 1), bits(row, 1, 3)
    wide = iota((KROWS, 128), 0)
    inside = (bits(wide, 1, 3) * 128 + bits(wide, 0, 1)).astype(F32)
    ones = jnp.ones((64, 128), BF16)
    owner = [
        [((q * 2 + zh) * 4 + p) * 2 + core == dev for q in range(4)],
        [((p * 2 + zh) * 4 + q) * 2 + core == dev for q in range(4)],
    ]
    for c in range(CHUNKS):
        block = (dev == jj + 8 * c).astype(F32).astype(BF16)
        rows = dot_nn(block, slots)
        for q in range(4):
            picked = jnp.where(owner[c // 4][q], rows, 0.0).astype(BF16)
            kpb[c // 4 * 16 + q * 4 + c % 4] = (
                dot_nn(picked, ones) * 2.0 + (inside + float(c * 1024))
            )

    dev, lane = iota((64, QROWS), 0), iota((64, QROWS), 1)
    zh, co, jj = bits(lane, 7, 1), bits(lane, 6, 1), bits(lane, 1, 3)
    pick = (((y * 2 + zh) * 4 + x) * 2 + co == dev).astype(F32).astype(BF16)
    slot = dot_nn(slots, pick)
    here = bits(dev, 0, 3) == jj
    pos = jnp.where(here, slot * 2.0 + (dev * 128 + bits(lane, 0, 1)).astype(F32), 0.0)
    qp[...] = jnp.sum(pos.reshape(CHUNKS, 8, QROWS), axis=1)


def kernel(
    q_in, g_in, k_in, v_in, x_in, mk_in, mv_in, rp_in, dq_out, ig_out, w_out, *scratch
):
    ssem, rsem, lsem = scratch[-3:]
    b = dict(zip(BUFFERS, scratch[:-3]))
    y, zh, x, core, zl = (lax.axis_index(a) for a in (Y, ZH, X, CORE, ZL))

    def turn(i, by):
        return lax.rem(i + by, 4)

    z = 2 * zh + zl
    zp, zm = turn(z, 1), turn(z, 3)
    zp_h, zp_l = lax.div(zp, 2), lax.rem(zp, 2)
    zm_h, zm_l = lax.div(zm, 2), lax.rem(zm, 2)
    oh, oc, ol = 1 - zh, 1 - core, 1 - zl
    d_zh, d_core, d_tp = {ZH: oh}, {CORE: oc}, {ZL: ol}
    d_zp, d_zm = {ZH: zp_h, ZL: zp_l}, {ZH: zm_h, ZL: zm_l}
    step_of = {a: ({a: turn(i, 1)}, {a: turn(i, 3)}) for a, i in ((X, x), (Y, y))}
    qi, pi = (y, x), (x, y)
    q_to = (step_of[Y], step_of[X])
    p_to = (step_of[X], step_of[Y])

    names = {}
    pending = []

    def remote(name, src, dst, dev):
        i = names.setdefault(name, len(names))
        return pltpu.make_async_remote_copy(
            src_ref=src,
            dst_ref=dst,
            send_sem=ssem.at[i],
            recv_sem=rsem.at[i],
            device_id=dev,
            device_id_type=MESH,
        )

    def send(name, src, dst, dev):
        remote(name, src, dst, dev).start()
        pending.append((name, src, dst, dev))

    def arrived(name, dst):
        remote(name, dst, dst, d_core).wait_recv()

    local_names = {}

    def local(name, src, dst):
        i = local_names.setdefault(name, len(local_names))
        return pltpu.make_async_copy(src, dst, lsem.at[i])

    def lanes(start, width=128):
        return pl.ds(pl.multiple_of(start, 128), width)

    kv, qg, xg, mat = b["kv"], b["qg"], b["xg"], b["mat"]
    own_kv = []
    for h in range(2):
        for t, ref in enumerate((k_in, v_in)):
            own_kv.append(
                local(
                    ("kv", h, t),
                    ref.at[pl.ds(4 * h, 4), :, lanes(zh * HEAD)],
                    kv.at[h, qi[h], pi[h], t, :, zh],
                )
            )
    own_q = []
    for t, ref in enumerate((q_in, g_in)):
        for g in range(GROUP):
            own_q.append(
                local(
                    ("qg", t, g),
                    ref.at[:, :, lanes(zh * GROUP * HEAD + g * HEAD)],
                    qg.at[t, :, 2 * zh + core, g],
                )
            )
    own_x = local("x", x_in, xg.at[:, zh, :, lanes(zl * (FEATS // 2), FEATS // 2)])
    own_m = [local("mk", mk_in, mat.at[0]), local("mv", mv_in, mat.at[1])]
    for c in own_kv + own_q:
        c.start()

    barrier = pltpu.get_barrier_semaphore()
    peers = [d_zh, d_core, *step_of[X], *step_of[Y], d_zp, d_zm]
    for dev in peers:
        pl.semaphore_signal(barrier, inc=1, device_id=dev, device_id_type=MESH)
    pl.semaphore_wait(barrier, len(peers))

    for h in range(2):
        for t, ref in enumerate((k_in, v_in)):
            send(
                ("zkv", h, t),
                ref.at[pl.ds(4 * h, 4), :, lanes(oh * HEAD)],
                kv.at[h, qi[h], pi[h], t, :, zh],
                d_zh,
            )
    for t, ref in enumerate((q_in, g_in)):
        for g in range(GROUP):
            send(
                ("qz", t, g),
                ref.at[:, :, lanes(oh * GROUP * HEAD + g * HEAD)],
                qg.at[t, :, 2 * zh + core, g],
                d_zh,
            )
    for t, ref in enumerate((q_in, g_in)):
        for g in range(GROUP):
            send(
                ("qc", t, g),
                ref.at[:, :, lanes(zh * GROUP * HEAD + g * HEAD)],
                qg.at[t, :, 2 * zh + core, g],
                d_core,
            )
    for c in own_kv:
        c.wait()

    for h in range(2):
        for t in range(2):
            arrived(("zkv", h, t), kv.at[h, qi[h], pi[h], t, :, oh])
        for side in range(2):
            unit = kv.at[h, qi[h], pi[h]]
            send(("p", h, side), unit, unit, p_to[h][side])
    own_x.start()
    for c in own_m:
        c.start()
    dqt = b["dqt"]
    dqt[...] = jnp.zeros(dqt.shape, F32)
    b["st"][0] = jnp.full(b["st"].shape[1:], MASKED, F32)
    b["st"][1:] = jnp.zeros((2,) + b["st"].shape[1:], F32)
    positions(rp_in, b["kpb"], b["qp"], y, x, core)
    for h in range(2):
        for side in range(2):
            src = kv.at[h, qi[h], turn(pi[h], 3 if side == 0 else 1)]
            arrived(("p", h, side), src)
            send(("pf", h, side), src.at[side], src.at[side], p_to[h][side])
    for h in range(2):
        for side in range(2):
            arrived(("pf", h, side), kv.at[h, qi[h], turn(pi[h], 2), side])
        for side in range(2):
            row = kv.at[h, qi[h]]
            send(("q", h, side), row, row, q_to[h][side])

    for t in range(2):
        for g in range(GROUP):
            arrived(("qz", t, g), qg.at[t, :, 2 * oh + core, g])
        src = qg.at[t, :, 2 * oh + core]
        send(("qf", t), src, src, d_core)
    half_feats = FEATS // 2
    quarter_feats = FEATS // 4
    mine = xg.at[:, zh, :, lanes(zl * half_feats, half_feats)]
    send("x+", x_in, mine, d_zp)
    send("x-", x_in, mine, d_zm)
    for c in own_q:
        c.wait()
    for t in range(2):
        for g in range(GROUP):
            arrived(("qc", t, g), qg.at[t, :, 2 * zh + oc, g])
        arrived(("qf", t), qg.at[t, :, 2 * oh + oc])

    def queries(t, cq):
        return qg[t, cq].reshape(QROWS, HEAD)

    def keys(t, at, cks):
        return stack_rows(
            [kv[ck // 4, at[ck // 4], :, t, ck % 4].reshape(KROWS, HEAD) for ck in cks]
        )

    def row_far(h, side):
        return kv.at[h, turn(qi[h], 2), pl.ds(2 * side, 2)]

    def row_near(h, side):
        return kv.at[h, turn(qi[h], 3 if side == 0 else 1)]

    def forward(h, side):
        src = row_near(h, side).at[pl.ds(2 * side, 2)]
        return ("qfar", h, side), src, src, q_to[h][side]

    st, e_ref, dp_ref = b["st"], b["e"], b["dp"]

    def first_pass(s, carry):
        late = lax.div(s, 2)
        off = (1 - late) * s + late * (5 - s)

        @pl.when(s == 1)
        def _():
            for h in range(2):
                for side in range(2):
                    arrived(("q", h, side), row_near(h, side))
                    remote(*forward(h, side)).start()

        @pl.when(s == 3)
        def _():
            for h in range(2):
                for side in range(2):
                    arrived(("qfar", h, side), row_far(h, side))

        at = (turn(y, off), turn(x, off))
        for cq in range(CHUNKS):
            cks = key_chunks(cq)
            scores = dot_tt(keys(0, at, cks), queries(0, cq))
            dprobs = dot_tt(keys(1, at, cks), queries(1, cq))
            qpos = b["qp"][cq : cq + 1, :]
            for n, ck in enumerate(cks):
                part = slice(n * KROWS, (n + 1) * KROWS)
                score, dprob = scores[part] * SCALE2, dprobs[part]
                if ck == cq or ck == cq - BAND:
                    kpb = b["kpb"][ck // 4 * 16 + at[ck // 4] * 4 + ck % 4]
                    kpos = jnp.concatenate([kpb, kpb], axis=1)
                    seen = kpos <= qpos if ck == cq else kpos > qpos - WINDOW
                    score = jnp.where(seen, score, MASKED)
                top = jnp.max(score, axis=0, keepdims=True)
                expo = jnp.exp2(score - top)
                rows = pl.ds(TILE_AT[cq] + n * KROWS, KROWS)
                e_ref[off, rows, :] = expo
                dp_ref[off, rows, :] = dprob
                row = slice(cq, cq + 1)
                st[0, off, cq - ck, row, :] = top
                st[1, off, cq - ck, row, :] = jnp.sum(expo, axis=0, keepdims=True)
                st[2, off, cq - ck, row, :] = jnp.sum(expo * dprob, axis=0, keepdims=True)
        return carry

    lax.fori_loop(0, 4, first_pass, 0)
    for h in range(2):
        for side in range(2):
            pending.append(forward(h, side))

    ss, sr = b["ss"], b["sr"]
    top_l = jnp.max(st[0], axis=(0, 1))
    fac_l = jnp.exp2(st[0] - top_l[None, None])
    sum_l = jnp.sum(st[1] * fac_l, axis=(0, 1))
    wgt_l = jnp.sum(st[2] * fac_l, axis=(0, 1))
    ss[0] = top_l
    ss[1] = sum_l
    ss[2] = wgt_l
    send("stat", ss, sr, d_core)
    arrived("x+", xg.at[:, zm_h, :, lanes(zm_l * half_feats, half_feats)])
    src = xg.at[:, zm_h, :, lanes(zm_l * half_feats, quarter_feats)]
    send("xf+", src, src, d_zp)
    arrived("x-", xg.at[:, zp_h, :, lanes(zp_l * half_feats, half_feats)])
    src = xg.at[:, zp_h, :, lanes(zp_l * half_feats + quarter_feats, quarter_feats)]
    send("xf-", src, src, d_zm)
    arrived("stat", sr)
    top = jnp.maximum(top_l, sr[0])
    mine_f = jnp.exp2(top_l - top)
    other_f = jnp.exp2(sr[0] - top)
    total = sum_l * mine_f + sr[1] * other_f
    b["delta"][...] = (wgt_l * mine_f + sr[2] * other_f) / total
    b["fac"][...] = fac_l * (mine_f / total)[None, None]

    def reducer(name, row):
        far, rfar = b[name + "_far"], b[name + "_rfar"]
        near, rnear = b[name + "_near"], b[name + "_rnear"]
        rows = b[name + "_row"]
        far2, rfar2 = b[name + "_far2"], b[name + "_rfar2"]
        near2, rnear2 = b[name + "_near2"], b[name + "_rnear2"]

        def far_copy(h, side):
            return (
                (name, "far", h, side),
                far.at[h, pl.ds(2 * side, 2)],
                rfar.at[h, side],
                q_to[h][side],
            )

        def near_copy(h, side):
            return (name, "near", h, side), near.at[h, side], rnear.at[h, side], q_to[h][side]

        def start_far():
            for h in range(2):
                far[h] = row(h, turn(qi[h], 2)).astype(BF16)
                for side in range(2):
                    remote(*far_copy(h, side)).start()

        def start_near(side):
            for h in range(2):
                value = row(h, turn(qi[h], 1 if side == 0 else 3))
                arrived((name, "far", h, side), rfar.at[h, side])
                lo, hi = value[:2], value[2:]
                if side == 0:
                    lo = lo + rfar[h, side].astype(F32)
                else:
                    hi = hi + rfar[h, side].astype(F32)
                near[h, side, :2] = lo.astype(BF16)
                near[h, side, 2:] = hi.astype(BF16)
                remote(*near_copy(h, side)).start()

        def note_sends():
            for h in range(2):
                for side in range(2):
                    pending.append(far_copy(h, side))
                    pending.append(near_copy(h, side))

        def own_row():
            for h in range(2):
                for side in range(2):
                    arrived((name, "near", h, side), rnear.at[h, side])
                rows[h] = row(h, qi[h]) + rnear[h, 0].astype(F32) + rnear[h, 1].astype(F32)
                far2[h] = rows[h, turn(pi[h], 2)].astype(BF16)
                for side in range(2):
                    send(
                        (name, "far2", h, side),
                        far2.at[h, side],
                        rfar2.at[h, side],
                        p_to[h][side],
                    )

        def near_unit():
            for h in range(2):
                for side in range(2):
                    arrived((name, "far2", h, side), rfar2.at[h, side])
                    at = turn(pi[h], 1 if side == 0 else 3)
                    near2[h, side, 1 - side] = rows[h, at, 1 - side].astype(BF16)
                    near2[h, side, side] = (
                        rows[h, at, side] + rfar2[h, side].astype(F32)
                    ).astype(BF16)
                    send(
                        (name, "near2", h, side), near2.at[h, side], rnear2.at[h, side], p_to[h][side]
                    )

        def final(h):
            for side in range(2):
                arrived((name, "near2", h, side), rnear2.at[h, side])
            return rows[h, pi[h]] + rnear2[h, 0].astype(F32) + rnear2[h, 1].astype(F32)

        return start_far, start_near, note_sends, own_row, near_unit, final

    acc = b["acc"]
    start_far, start_near, note_sends, own_row, near_unit, final = reducer(
        "a", lambda h, at: acc[h]
    )

    fac, delta, kt = b["fac"], b["delta"], b["kt"]

    def second_pass(s, carry):
        late = lax.div(s, 2)
        off = (1 - late) * (2 + s) + late * (3 - s)
        at = (turn(y, off), turn(x, off))
        for ck in range(CHUNKS):
            kt[ck] = keys(0, at, [ck]).T
        for cq in range(CHUNKS):
            cks = key_chunks(cq)
            probs, dscores = [], []
            for n, ck in enumerate(cks):
                rows = pl.ds(TILE_AT[cq] + n * KROWS, KROWS)
                prob = e_ref[off, rows, :] * fac[off, cq - ck, cq : cq + 1, :]
                diff = dp_ref[off, rows, :] - delta[cq : cq + 1, :]
                probs.append(prob.astype(BF16))
                dscores.append((prob * diff).astype(BF16))
            prob, dscore = stack_rows(probs), stack_rows(dscores)
            grads = (dot_nn(dscore, queries(0, cq)), dot_nn(prob, queries(1, cq)))
            for t in range(2):
                for n, ck in enumerate(cks):
                    part = grads[t][n * KROWS : (n + 1) * KROWS].reshape(4, 2, 16, HEAD)
                    if ck == cq:
                        acc[ck // 4, :, t, ck % 4] = part
                    else:
                        acc[ck // 4, :, t, ck % 4] = acc[ck // 4, :, t, ck % 4] + part
            flipped = jnp.concatenate([kt[ck] for ck in cks], axis=1)
            dqt[cq] = dqt[cq] + dot_nn(flipped, dscore)

        @pl.when(s == 0)
        def _():
            start_far()

        @pl.when(s == 1)
        def _():
            start_near(1)

        @pl.when(s == 2)
        def _():
            start_near(0)

        return carry

    lax.fori_loop(0, 4, second_pass, 0)
    note_sends()

    dqf, dqr, dqs, dqz = b["dqf"], b["dqr"], b["dqs"], b["dqz"]
    for cq in range(CHUNKS):
        dqf[cq] = (dqt[cq].T * SCALE).reshape(2, 2, GROUP, 16, HEAD)
    send("dqc", dqf.at[:, :, oc], dqr, d_core)
    own_x.wait()
    for c in own_m:
        c.wait()
    far_h = 1 - zh
    arrived("xf+", xg.at[:, far_h, :, lanes(zl * half_feats, quarter_feats)])
    arrived("xf-", xg.at[:, far_h, :, lanes(zl * half_feats + quarter_feats, quarter_feats)])
    xt = b["xt"]

    def flip_input(i, carry):
        for n in range(4):
            at = i * 512 + n * 128
            xt[pl.ds(pl.multiple_of(at, 128), 128), :] = xg[:, :, :, lanes(at)].reshape(256, 128).T
        return carry

    lax.fori_loop(0, 8, flip_input, 0)
    own_row()
    arrived("dqc", dqr)
    dqs[...] = (dqf[:, oh, core] + dqr[:, oh]).astype(BF16)
    send("dqz", dqs, dqz, d_zh)
    dq_out[zh] = (dqf[:, zh, core] + dqr[:, zh]).astype(BF16)
    near_unit()
    arrived("dqz", dqz)
    dq_out[oh] = dqz[...]
    d2, dd = b["d2"], b["dd"]
    for h in range(2):
        value = final(h)
        d2[0, 4 * h : 4 * h + 4] = (value[0] * SCALE).astype(BF16)
        d2[1, 4 * h : 4 * h + 4] = value[1].astype(BF16)
    for t in range(2):
        send(("dz", t), d2.at[t, :, oh], dd.at[2 * t + zh], d_zh)
        dd[2 * t + zh] = d2[t, :, zh]

    wown, wsend, wrecv = b["wown"], b["wsend"], b["wrecv"]
    grad_cols = jnp.concatenate([d2[0].reshape(256, HEAD), d2[1].reshape(256, HEAD)], axis=1)

    def weight_block(i, carry):
        wz = lax.rem(i, 2)
        wy = lax.div(i, 2)
        part = dot_nn(xt[pl.ds(pl.multiple_of(i * 512, 512), 512), :], grad_cols)
        for wx in range(4):
            for h, (wq, wp) in enumerate(((wy, wx), (wx, wy))):
                cols = part[wx * 128 : (wx + 1) * 128, h * HEAD : (h + 1) * HEAD]
                wown[h, wq, wp, wz] = jnp.where(core == 0, cols[:64], cols[64:])
                wsend[h, wq, wp, wz] = jnp.where(core == 0, cols[64:], cols[:64]).astype(BF16)
        return carry

    lax.fori_loop(0, 8, weight_block, 0)
    send("wc", wsend, wrecv, d_core)

    igs, igr, igo = b["igs"], b["igr"], b["igo"]
    for t in range(2):
        arrived(("dz", t), dd.at[2 * t + oh])
    dk_dv = [
        jnp.concatenate([dd[2 * t].reshape(128, HEAD), dd[2 * t + 1].reshape(128, HEAD)], axis=1)
        for t in range(2)
    ]

    def input_block(base, out):
        def body(i, carry):
            rows = pl.ds(pl.multiple_of(base + i * 512, 512), 512)
            part = dot_tt(dk_dv[0], mat[0, rows, :]) + dot_tt(dk_dv[1], mat[1, rows, :])
            out[:, lanes(i * 512, 512)] = part.astype(out.dtype)
            return carry

        lax.fori_loop(0, 4, body, 0)

    input_block(ol * half_feats, igs)
    send("ig", igs, igr, d_tp)

    arrived("wc", wrecv)
    w_far, w_near, w_note, w_own, w_unit, w_final = reducer(
        "w", lambda h, at: wown[h, at] + wrecv[h, at].astype(F32)
    )
    w_far()
    input_block(zl * half_feats, igo)
    w_near(0)
    w_near(1)
    w_note()
    w_own()
    w_unit()
    wfin, wswap = b["wfin"], b["wswap"]
    for h in range(2):
        wfin[h] = w_final(h)
    for h in range(2):
        send(("ws", h), wfin.at[h, oh], wswap.at[h], d_zh)
        w_out[h, zh] = wfin[h, zh]
    arrived("ig", igr)
    ig_out[...] = (igo[...] + igr[...].astype(F32)).astype(BF16)
    for h in range(2):
        arrived(("ws", h), wswap.at[h])
        w_out[h, oh] = wswap[h]

    for copy in pending:
        remote(*copy).wait_send()
    assert len(names) <= NSEM and len(local_names) <= NLOCAL


def finish(dq_in, ig_in, w_in, dq_out, ig_out, kw_out, vw_out):
    for c in range(CHUNKS):
        for kvh in range(2):
            for g in range(GROUP):
                at = (kvh * GROUP + g) * HEAD
                dq_out[c * 16 : (c + 1) * 16, at : at + HEAD] = dq_in[kvh, c, g]
    ig_out[...] = ig_in[...]
    for t, out in enumerate((kw_out, vw_out)):
        for n in range(2):
            out[:, n * HEAD : (n + 1) * HEAD] = w_in[t, n]


def local_step(q, k, v, g, x, mk, mv, placement):
    anywhere = pl.BlockSpec(memory_space=pl.ANY)
    vmem = pl.BlockSpec(memory_space=pltpu.VMEM)
    dq, ig, w = pl.pallas_call(
        kernel,
        out_shape=(
            jax.ShapeDtypeStruct((2, CHUNKS, GROUP, 16, HEAD), BF16),
            jax.ShapeDtypeStruct((128, FEATS // 2), BF16),
            jax.ShapeDtypeStruct((2, 2, 64, HEAD), F32),
        ),
        in_specs=[anywhere] * 7 + [vmem],
        out_specs=(vmem, vmem, vmem),
        scratch_shapes=[pltpu.VMEM(shape, dtype) for shape, dtype in BUFFERS.values()]
        + [
            pltpu.SemaphoreType.DMA((NSEM,)),
            pltpu.SemaphoreType.DMA((NSEM,)),
            pltpu.SemaphoreType.DMA((NLOCAL,)),
        ],
        compiler_params=pltpu.CompilerParams(
            collective_id=0, has_side_effects=True, vmem_limit_bytes=67043328
        ),
    )(
        q.reshape(CHUNKS, 16, -1),
        g.reshape(CHUNKS, 16, -1),
        k.reshape(CHUNKS, 16, -1),
        v.reshape(CHUNKS, 16, -1),
        x.reshape(CHUNKS, 16, -1),
        mk,
        mv,
        placement,
    )
    return pl.pallas_call(
        finish,
        out_shape=(
            jax.ShapeDtypeStruct((128, 2 * GROUP * HEAD), BF16),
            jax.ShapeDtypeStruct((128, FEATS // 2), BF16),
            jax.ShapeDtypeStruct((64, 2 * HEAD), F32),
            jax.ShapeDtypeStruct((64, 2 * HEAD), F32),
        ),
        in_specs=[vmem] * 3,
        out_specs=(vmem,) * 4,
    )(dq, ig, w)


def solution(mesh):
    torus = Mesh(
        mesh.devices.reshape(4, 2, 4, 2, mesh.shape["tp"]), ("seq_0", "seq_1", "seq_2", "seq_3", "tp")
    )
    rows = P(SEQ, "tp")
    return jax.shard_map(
        local_step,
        mesh=torus,
        in_specs=(rows, rows, rows, rows, rows, P(None, "tp"), P(None, "tp"), P()),
        out_specs=(rows, rows, rows, rows),
        check_vma=False,
    )
```

```python
import math

import jax
import jax.numpy as jnp
from jax import lax
from jax.experimental import pallas as pl
from jax.experimental.pallas import tpu as pltpu
from jax.sharding import Mesh
from jax.sharding import PartitionSpec as P

F32 = jnp.float32
BF16 = jnp.bfloat16
Y, ZH, X, CORE, ZL = "seq_0", "seq_1", "seq_2", "seq_3", "tp"
SEQ = (Y, ZH, X, CORE)
MESH = pl.DeviceIdType.MESH

HEAD = 128
GROUP = 4
WINDOW = 4096
CHUNKS = 8
BAND = 4
FEATS = 4096
SCALE = 1.0 / math.sqrt(HEAD)
SCALE2 = SCALE * math.log2(math.e)
MASKED = -1e30
QROWS = 256
KROWS = 128
NSEM = 192
NLOCAL = 24


def key_chunks(cq):
    return list(range(max(0, cq - BAND), cq + 1))


TILE_AT = [KROWS * sum(len(key_chunks(c)) for c in range(cq)) for cq in range(CHUNKS)]
TILE_ROWS = KROWS * sum(len(key_chunks(c)) for c in range(CHUNKS))

UNIT_KV = (2, 4, 2, 16, HEAD)
UNIT_W = (2, 64, HEAD)


def reduce_buffers(name, unit):
    half = unit[1:]
    return {
        name + "_far": ((2, 4) + unit, BF16),
        name + "_rfar": ((2, 2, 4) + half, BF16),
        name + "_near": ((2, 2, 4) + unit, BF16),
        name + "_rnear": ((2, 2, 4) + unit, BF16),
        name + "_far2": ((2,) + unit, BF16),
        name + "_rfar2": ((2, 2) + half, BF16),
        name + "_near2": ((2, 2) + unit, BF16),
        name + "_rnear2": ((2, 2) + unit, BF16),
    }


BUFFERS = {
    "kv": ((2, 4, 4) + UNIT_KV, BF16),
    "qg": ((2, CHUNKS, 4, GROUP, 16, HEAD), BF16),
    "kpb": ((32, KROWS, 128), F32),
    "e": ((4, TILE_ROWS, QROWS), F32),
    "dp": ((4, TILE_ROWS, QROWS), F32),
    "st": ((3, 4, BAND + 1, CHUNKS, QROWS), F32),
    "ss": ((3, CHUNKS, QROWS), F32),
    "sr": ((3, CHUNKS, QROWS), F32),
    "fac": ((4, BAND + 1, CHUNKS, QROWS), F32),
    "delta": ((CHUNKS, QROWS), F32),
    "acc": ((2, 4) + UNIT_KV, F32),
    "dqt": ((CHUNKS, HEAD, QROWS), F32),
    "dqf": ((CHUNKS, 2, 2, GROUP, 16, HEAD), F32),
    "dqr": ((CHUNKS, 2, GROUP, 16, HEAD), F32),
    "dqs": ((2, CHUNKS, GROUP, 16, HEAD), BF16),
    "dqz": ((2, CHUNKS, GROUP, 16, HEAD), BF16),
    "kt": ((CHUNKS, HEAD, KROWS), BF16),
    "qp": ((CHUNKS, QROWS), F32),
    "xg": ((CHUNKS, 2, 16, FEATS), BF16),
    "xt": ((32, 2, 64, 256), BF16),
    "xo": ((32, 64, 256), BF16),
    "mat": ((2, FEATS, 2 * HEAD), BF16),
    "d2": ((2, CHUNKS, 2, 16, HEAD), BF16),
    "d2o": ((2, CHUNKS, 2, 16, HEAD), BF16),
    "dd": ((4, CHUNKS, 16, HEAD), BF16),
    "wown": ((2, 4, 4) + UNIT_W, F32),
    "wfin": ((2,) + UNIT_W, BF16),
    "wz": ((2, 2, 64, HEAD), BF16),
    "igs": ((128, FEATS // 2), BF16),
    "igr": ((128, FEATS // 2), BF16),
    "igo": ((128, FEATS // 2), F32),
    **reduce_buffers("a", UNIT_KV),
    **reduce_buffers("w", UNIT_W),
}


def dot_tt(a, b):
    return lax.dot_general(a, b, (((1,), (1,)), ((), ())), preferred_element_type=F32)


def dot_nn(a, b):
    return lax.dot_general(a, b, (((1,), (0,)), ((), ())), preferred_element_type=F32)


def dot_tn(a, b):
    return lax.dot_general(a, b, (((0,), (0,)), ((), ())), preferred_element_type=F32)


def stack_rows(parts):
    return parts[0] if len(parts) == 1 else jnp.concatenate(parts, axis=0)


def positions(rp_in, kpb, qp, y, x, core):
    slots = rp_in[...].astype(F32).astype(BF16)

    def iota(shape, dim):
        return lax.broadcasted_iota(jnp.int32, shape, dim)

    def bits(a, at, width):
        return jnp.bitwise_and(jnp.right_shift(a, at), (1 << width) - 1)

    row, dev = iota((KROWS, 64), 0), iota((KROWS, 64), 1)
    p, zh, jj = bits(row, 5, 2), bits(row, 4, 1), bits(row, 1, 3)
    wide = iota((KROWS, 128), 0)
    inside = (bits(wide, 1, 3) * 128 + bits(wide, 0, 1)).astype(F32)
    ones = jnp.ones((64, 128), BF16)
    owner = [
        [((q * 2 + zh) * 4 + p) * 2 + core == dev for q in range(4)],
        [((p * 2 + zh) * 4 + q) * 2 + core == dev for q in range(4)],
    ]
    for c in range(CHUNKS):
        block = (dev == jj + 8 * c).astype(F32).astype(BF16)
        rows = dot_nn(block, slots)
        for q in range(4):
            picked = jnp.where(owner[c // 4][q], rows, 0.0).astype(BF16)
            kpb[c // 4 * 16 + q * 4 + c % 4] = (
                dot_nn(picked, ones) * 2.0 + (inside + float(c * 1024))
            )

    dev, lane = iota((64, QROWS), 0), iota((64, QROWS), 1)
    zh, co, jj = bits(lane, 7, 1), bits(lane, 6, 1), bits(lane, 1, 3)
    pick = (((y * 2 + zh) * 4 + x) * 2 + co == dev).astype(F32).astype(BF16)
    slot = dot_nn(slots, pick)
    here = bits(dev, 0, 3) == jj
    pos = jnp.where(here, slot * 2.0 + (dev * 128 + bits(lane, 0, 1)).astype(F32), 0.0)
    qp[...] = jnp.sum(pos.reshape(CHUNKS, 8, QROWS), axis=1)


def kernel(
    q_in, g_in, k_in, v_in, x_in, mk_in, mv_in, rp_in, dq_out, ig_out, w_out, *scratch
):
    ssem, rsem, lsem = scratch[-3:]
    b = dict(zip(BUFFERS, scratch[:-3]))
    y, zh, x, core, zl = (lax.axis_index(a) for a in (Y, ZH, X, CORE, ZL))

    def turn(i, by):
        return lax.rem(i + by, 4)

    z = 2 * zh + zl
    zp, zm = turn(z, 1), turn(z, 3)
    zp_h, zp_l = lax.div(zp, 2), lax.rem(zp, 2)
    zm_h, zm_l = lax.div(zm, 2), lax.rem(zm, 2)
    oh, oc, ol = 1 - zh, 1 - core, 1 - zl
    d_core, d_tp = {CORE: oc}, {ZL: ol}
    across = ((d_tp, zh), ({ZH: oh, ZL: ol}, oh))
    d_zp, d_zm = {ZH: zp_h, ZL: zp_l}, {ZH: zm_h, ZL: zm_l}
    step_of = {a: ({a: turn(i, 1)}, {a: turn(i, 3)}) for a, i in ((X, x), (Y, y))}
    qi, pi = (y, x), (x, y)
    q_to = (step_of[Y], step_of[X])
    p_to = (step_of[X], step_of[Y])

    names = {}
    pending = []

    def remote(name, src, dst, dev):
        i = names.setdefault(name, len(names))
        return pltpu.make_async_remote_copy(
            src_ref=src,
            dst_ref=dst,
            send_sem=ssem.at[i],
            recv_sem=rsem.at[i],
            device_id=dev,
            device_id_type=MESH,
        )

    def send(name, src, dst, dev):
        remote(name, src, dst, dev).start()
        pending.append((name, src, dst, dev))

    def arrived(name, dst):
        remote(name, dst, dst, d_core).wait_recv()

    local_names = {}

    def local(name, src, dst):
        i = local_names.setdefault(name, len(local_names))
        return pltpu.make_async_copy(src, dst, lsem.at[i])

    def lanes(start, width=128):
        return pl.ds(pl.multiple_of(start, 128), width)

    kv, qg, xg, mat = b["kv"], b["qg"], b["xg"], b["mat"]
    own_x = local("x", x_in, xg.at[:, zh, :, lanes(zl * (FEATS // 2), FEATS // 2)])
    own_m = [local("mk", mk_in, mat.at[0]), local("mv", mv_in, mat.at[1])]

    barrier = pltpu.get_barrier_semaphore()
    peers = [d_core, *step_of[X], *step_of[Y], d_zp, d_zm]
    for dev in peers:
        pl.semaphore_signal(barrier, inc=1, device_id=dev, device_id_type=MESH)
    pl.semaphore_wait(barrier, len(peers))

    for h in range(2):
        for r, (dev, head) in enumerate(across):
            for t, ref in enumerate((k_in, v_in)):
                send(
                    ("zkv", h, t, r),
                    ref.at[pl.ds(4 * h, 4), :, lanes(head * HEAD)],
                    kv.at[h, qi[h], pi[h], t, :, zh],
                    dev,
                )
    for t, ref in enumerate((q_in, g_in)):
        for r, (dev, head) in enumerate(across):
            for g in range(GROUP):
                send(
                    ("qz", t, r, g),
                    ref.at[:, :, lanes(head * GROUP * HEAD + g * HEAD)],
                    qg.at[t, :, 2 * zh + core, g],
                    dev,
                )

    unit_offs = (0, 3, 1, 2)

    def unit_piece(h, n, side):
        unit = kv.at[h, qi[h], turn(pi[h], unit_offs[n])]
        return ("q", h, n, side), unit, unit, q_to[h][side]

    def send_unit(h, n):
        for side in range(2):
            send(*unit_piece(h, n, side))

    def near_piece(h, n, side):
        return kv.at[h, turn(qi[h], 3 if side == 0 else 1), turn(pi[h], unit_offs[n])]

    def forward_piece(h, n, side):
        src = near_piece(h, n, side).at[side]
        return ("qf", h, n, side), src, src, q_to[h][side]

    def forward_unit(h, n):
        for side in range(2):
            arrived(("q", h, n, side), near_piece(h, n, side))
            remote(*forward_piece(h, n, side)).start()
            if n == 0:
                pending.append(forward_piece(h, n, side))

    for h in range(2):
        for r, (dev, head) in enumerate(across):
            for t in range(2):
                arrived(("zkv", h, t, r), kv.at[h, qi[h], pi[h], t, :, head])
        unit = kv.at[h, qi[h], pi[h]]
        for side in range(2):
            send(("p", h, side), unit, unit, p_to[h][side])
        send_unit(h, 0)
    own_x.start()
    for c in own_m:
        c.start()
    dqt = b["dqt"]
    dqt[...] = jnp.zeros(dqt.shape, F32)
    b["st"][0] = jnp.full(b["st"].shape[1:], MASKED, F32)
    b["st"][1:] = jnp.zeros((2,) + b["st"].shape[1:], F32)
    positions(rp_in, b["kpb"], b["qp"], y, x, core)
    for h in range(2):
        for side in range(2):
            src = kv.at[h, qi[h], turn(pi[h], 3 if side == 0 else 1)]
            arrived(("p", h, side), src)
            send(("pf", h, side), src.at[side], src.at[side], p_to[h][side])
        for side in range(2):
            send_unit(h, 1 + side)
    for h in range(2):
        forward_unit(h, 0)
    for t in range(2):
        for r, (dev, head) in enumerate(across):
            for g in range(GROUP):
                arrived(("qz", t, r, g), qg.at[t, :, 2 * head + core, g])
            src = qg.at[t, :, 2 * head + core]
            send(("qc", t, r), src, src, d_core)
    half_feats = FEATS // 2
    quarter_feats = FEATS // 4
    mine = xg.at[:, zh, :, lanes(zl * half_feats, half_feats)]
    send("x+", x_in, mine, d_zp)
    send("x-", x_in, mine, d_zm)
    for h in range(2):
        for side in range(2):
            arrived(("pf", h, side), kv.at[h, qi[h], turn(pi[h], 2), side])
        send_unit(h, 3)
    for t in range(2):
        for r, (dev, head) in enumerate(across):
            arrived(("qc", t, r), qg.at[t, :, 2 * head + oc])

    def queries(t, cq):
        return qg[t, cq].reshape(QROWS, HEAD)

    def keys(t, at, cks):
        return stack_rows(
            [kv[ck // 4, at[ck // 4], :, t, ck % 4].reshape(KROWS, HEAD) for ck in cks]
        )

    st, e_ref, dp_ref = b["st"], b["e"], b["dp"]

    def first_pass(s, carry):
        late = lax.div(s, 2)
        off = (1 - late) * s + late * (5 - s)

        @pl.when(s == 1)
        def _():
            for n in range(1, 4):
                for h in range(2):
                    forward_unit(h, n)

        @pl.when(s == 3)
        def _():
            for n in range(4):
                for h in range(2):
                    for side in range(2):
                        arrived(
                            ("qf", h, n, side),
                            kv.at[h, turn(qi[h], 2), turn(pi[h], unit_offs[n]), side],
                        )

        at = (turn(y, off), turn(x, off))
        for cq in range(CHUNKS):
            cks = key_chunks(cq)
            scores = dot_tt(keys(0, at, cks), queries(0, cq))
            dprobs = dot_tt(keys(1, at, cks), queries(1, cq))
            qpos = b["qp"][cq : cq + 1, :]
            for n, ck in enumerate(cks):
                part = slice(n * KROWS, (n + 1) * KROWS)
                score, dprob = scores[part] * SCALE2, dprobs[part]
                if ck == cq or ck == cq - BAND:
                    kpb = b["kpb"][ck // 4 * 16 + at[ck // 4] * 4 + ck % 4]
                    kpos = jnp.concatenate([kpb, kpb], axis=1)
                    seen = kpos <= qpos if ck == cq else kpos > qpos - WINDOW
                    score = jnp.where(seen, score, MASKED)
                top = jnp.max(score, axis=0, keepdims=True)
                expo = jnp.exp2(score - top)
                rows = pl.ds(TILE_AT[cq] + n * KROWS, KROWS)
                e_ref[off, rows, :] = expo
                dp_ref[off, rows, :] = dprob
                row = slice(cq, cq + 1)
                st[0, off, cq - ck, row, :] = top
                st[1, off, cq - ck, row, :] = jnp.sum(expo, axis=0, keepdims=True)
                st[2, off, cq - ck, row, :] = jnp.sum(expo * dprob, axis=0, keepdims=True)
        return carry

    lax.fori_loop(0, 4, first_pass, 0)
    for h in range(2):
        for n in range(4):
            for side in range(2):
                if n:
                    pending.append(forward_piece(h, n, side))

    ss, sr = b["ss"], b["sr"]
    top_l = jnp.max(st[0], axis=(0, 1))
    fac_l = jnp.exp2(st[0] - top_l[None, None])
    sum_l = jnp.sum(st[1] * fac_l, axis=(0, 1))
    wgt_l = jnp.sum(st[2] * fac_l, axis=(0, 1))
    ss[0] = top_l
    ss[1] = sum_l
    ss[2] = wgt_l
    send("stat", ss, sr, d_core)

    def forward_input(names_only=False):
        for name, src_h, src_l, start, dev in (
            ("x+", zm_h, zm_l, 0, d_zp),
            ("x-", zp_h, zp_l, quarter_feats, d_zm),
        ):
            src = xg.at[:, src_h, :, lanes(src_l * half_feats + start, quarter_feats)]
            if names_only:
                pending.append(("far " + name, src, src, dev))
            else:
                arrived(name, xg.at[:, src_h, :, lanes(src_l * half_feats, half_feats)])
                remote("far " + name, src, src, dev).start()

    arrived("stat", sr)
    top = jnp.maximum(top_l, sr[0])
    mine_f = jnp.exp2(top_l - top)
    other_f = jnp.exp2(sr[0] - top)
    total = sum_l * mine_f + sr[1] * other_f
    b["delta"][...] = (wgt_l * mine_f + sr[2] * other_f) / total
    b["fac"][...] = fac_l * (mine_f / total)[None, None]

    offs = (2, 1, 3, 0)

    def reducer(name, unit_at):
        far, rfar = b[name + "_far"], b[name + "_rfar"]
        near, rnear = b[name + "_near"], b[name + "_rnear"]
        far2, rfar2 = b[name + "_far2"], b[name + "_rfar2"]
        near2, rnear2 = b[name + "_near2"], b[name + "_rnear2"]

        def place(h, n):
            return turn(pi[h], offs[n])

        def far_copy(h, n, side):
            p = place(h, n)
            return (
                (name, "far", h, n, side),
                far.at[h, p, side],
                rfar.at[h, side, p],
                q_to[h][side],
            )

        def near_copy(h, n, side):
            p = place(h, n)
            return (
                (name, "near", h, n, side),
                near.at[h, side, p],
                rnear.at[h, side, p],
                q_to[h][side],
            )

        def start_far():
            for n in range(4):
                for h in range(2):
                    p = place(h, n)
                    far[h, p] = unit_at(h, turn(qi[h], 2), p).astype(BF16)
                    for side in range(2):
                        remote(*far_copy(h, n, side)).start()

        def start_near(side):
            for n in range(4):
                for h in range(2):
                    p = place(h, n)
                    value = unit_at(h, turn(qi[h], 1 if side == 0 else 3), p)
                    arrived((name, "far", h, n, side), rfar.at[h, side, p])
                    near[h, side, p, 1 - side] = value[1 - side].astype(BF16)
                    near[h, side, p, side] = (value[side] + rfar[h, side, p].astype(F32)).astype(
                        BF16
                    )
                    remote(*near_copy(h, n, side)).start()

        def note_sends():
            for h in range(2):
                for n in range(4):
                    for side in range(2):
                        pending.append(far_copy(h, n, side))
                        pending.append(near_copy(h, n, side))

        def own_unit(n):
            out = []
            for h in range(2):
                p = place(h, n)
                for side in range(2):
                    arrived((name, "near", h, n, side), rnear.at[h, side, p])
                value = (
                    unit_at(h, qi[h], p)
                    + rnear[h, 0, p].astype(F32)
                    + rnear[h, 1, p].astype(F32)
                )
                if n == 0:
                    far2[h] = value.astype(BF16)
                    for side in range(2):
                        send(
                            (name, "far2", h, side),
                            far2.at[h, side],
                            rfar2.at[h, side],
                            p_to[h][side],
                        )
                elif n < 3:
                    side = n - 1
                    arrived((name, "far2", h, side), rfar2.at[h, side])
                    near2[h, side, 1 - side] = value[1 - side].astype(BF16)
                    near2[h, side, side] = (value[side] + rfar2[h, side].astype(F32)).astype(BF16)
                    send(
                        (name, "near2", h, side),
                        near2.at[h, side],
                        rnear2.at[h, side],
                        p_to[h][side],
                    )
                else:
                    for side in range(2):
                        arrived((name, "near2", h, side), rnear2.at[h, side])
                    out.append(
                        value + rnear2[h, 0].astype(F32) + rnear2[h, 1].astype(F32)
                    )
            return out

        return start_far, start_near, note_sends, own_unit

    acc = b["acc"]
    start_far, start_near, note_sends, own_unit = reducer("a", lambda h, q, p: acc[h, p])

    fac, delta, kt = b["fac"], b["delta"], b["kt"]

    def second_pass(s, carry):
        late = lax.div(s, 2)
        off = (1 - late) * (2 + s) + late * (3 - s)
        at = (turn(y, off), turn(x, off))
        for ck in range(CHUNKS):
            kt[ck] = keys(0, at, [ck]).T
        for cq in range(CHUNKS):
            cks = key_chunks(cq)
            probs, dscores = [], []
            for n, ck in enumerate(cks):
                rows = pl.ds(TILE_AT[cq] + n * KROWS, KROWS)
                prob = e_ref[off, rows, :] * fac[off, cq - ck, cq : cq + 1, :]
                diff = dp_ref[off, rows, :] - delta[cq : cq + 1, :]
                probs.append(prob.astype(BF16))
                dscores.append((prob * diff).astype(BF16))
            prob, dscore = stack_rows(probs), stack_rows(dscores)
            grads = (dot_nn(dscore, queries(0, cq)), dot_nn(prob, queries(1, cq)))
            for t in range(2):
                for n, ck in enumerate(cks):
                    part = grads[t][n * KROWS : (n + 1) * KROWS].reshape(4, 2, 16, HEAD)
                    if ck == cq:
                        acc[ck // 4, :, t, ck % 4] = part
                    else:
                        acc[ck // 4, :, t, ck % 4] = acc[ck // 4, :, t, ck % 4] + part
            flipped = jnp.concatenate([kt[ck] for ck in cks], axis=1)
            dqt[cq] = dqt[cq] + dot_nn(flipped, dscore)

        @pl.when(s == 0)
        def _():
            start_far()

        @pl.when(s == 1)
        def _():
            start_near(1)
            forward_input()

        @pl.when(s == 2)
        def _():
            start_near(0)

        return carry

    lax.fori_loop(0, 4, second_pass, 0)
    note_sends()
    forward_input(names_only=True)

    dqf, dqr, dqs, dqz = b["dqf"], b["dqr"], b["dqs"], b["dqz"]
    for cq in range(CHUNKS):
        dqf[cq] = (dqt[cq].T * SCALE).reshape(2, 2, GROUP, 16, HEAD)
    send("dqc", dqf.at[:, :, oc], dqr, d_core)
    own_unit(0)
    own_x.wait()
    far_h = 1 - zh
    arrived("far x+", xg.at[:, far_h, :, lanes(zl * half_feats, quarter_feats)])
    arrived("far x-", xg.at[:, far_h, :, lanes(zl * half_feats + quarter_feats, quarter_feats)])
    xt, xo = b["xt"], b["xo"]

    def flip_input(i, carry):
        for n in range(4):
            at = i * 4 + n
            block = xg[:, :, :, lanes(at * 128)].reshape(256, 128)
            xt[at] = block.T.reshape(2, 64, 256)
        return carry

    lax.fori_loop(0, 8, flip_input, 0)
    send("xt", xt.at[:, oc], xo, d_core)
    own_unit(1)
    own_unit(2)
    arrived("dqc", dqr)
    for n in range(2):
        dqs[n] = (dqf[:, n, core] + dqr[:, n]).astype(BF16)
    for r, (dev, other) in enumerate(across):
        send(("dqz", r), dqs.at[other], dqz.at[zh], dev)
    d2, d2o, dd = b["d2"], b["d2o"], b["dd"]
    for h, value in enumerate(own_unit(3)):
        d2[0, 4 * h : 4 * h + 4] = (value[0] * SCALE).astype(BF16)
        d2[1, 4 * h : 4 * h + 4] = value[1].astype(BF16)
    send("d2", d2, d2o, d_core)
    for r, (dev, other) in enumerate(across):
        for t in range(2):
            send(("dz", t, r), d2.at[t, :, other], dd.at[2 * t + zh], dev)

    wown = b["wown"]

    def grad_cols(ref):
        return jnp.concatenate([ref[0].reshape(256, HEAD), ref[1].reshape(256, HEAD)], axis=1)

    def weight_blocks(first):
        cols = grad_cols(d2 if first else d2o)

        def body(i, carry):
            wz = lax.rem(i, 2)
            wy = lax.div(i, 2)
            at = pl.ds(i * 4, 4)
            rows = (xt[at, core] if first else xo[at]).reshape(256, 256)
            part = dot_nn(rows, cols)
            for wx in range(4):
                for h, (wq, wp) in enumerate(((wy, wx), (wx, wy))):
                    block = part[wx * 64 : (wx + 1) * 64, h * HEAD : (h + 1) * HEAD]
                    if first:
                        wown[h, wq, wp, wz] = block
                    else:
                        wown[h, wq, wp, wz] = wown[h, wq, wp, wz] + block
            return carry

        lax.fori_loop(0, 8, body, 0)

    weight_blocks(True)
    arrived("xt", xo)
    arrived("d2", d2o)
    weight_blocks(False)
    w_far, w_near, w_note, w_unit = reducer("w", lambda h, q, p: wown[h, q, p])
    w_far()

    igs, igr, igo, mat = b["igs"], b["igr"], b["igo"], b["mat"]
    for c in own_m:
        c.wait()
    for r, (dev, other) in enumerate(across):
        for t in range(2):
            arrived(("dz", t, r), dd.at[2 * t + other])
    dk_dv = [
        jnp.concatenate([dd[2 * t].reshape(128, HEAD), dd[2 * t + 1].reshape(128, HEAD)], axis=1)
        for t in range(2)
    ]

    def input_block(base, out):
        def body(i, carry):
            rows = pl.ds(pl.multiple_of(base + i * 512, 512), 512)
            part = dot_tt(dk_dv[0], mat[0, rows, :]) + dot_tt(dk_dv[1], mat[1, rows, :])
            out[:, lanes(i * 512, 512)] = part.astype(out.dtype)
            return carry

        lax.fori_loop(0, 4, body, 0)

    input_block(ol * half_feats, igs)
    send("ig", igs, igr, d_tp)
    w_near(0)
    w_near(1)
    w_note()
    input_block(zl * half_feats, igo)
    for r, (dev, other) in enumerate(across):
        arrived(("dqz", r), dqz.at[other])
    dq_out[...] = dqz[...]
    w_unit(0)
    w_unit(1)
    w_unit(2)
    wfin, wz_ref = b["wfin"], b["wz"]
    for h, value in enumerate(w_unit(3)):
        wfin[h] = value.astype(BF16)
    for r, (dev, other) in enumerate(across):
        send(("ws", r), wfin.at[:, other], wz_ref.at[:, zh], dev)
    arrived("ig", igr)
    ig_out[...] = (igo[...] + igr[...].astype(F32)).astype(BF16)
    for r, (dev, other) in enumerate(across):
        arrived(("ws", r), wz_ref.at[:, other])
    w_out[...] = wz_ref[...].astype(F32)

    for copy in pending:
        remote(*copy).wait_send()
    assert len(names) <= NSEM and len(local_names) <= NLOCAL


def finish(dq_in, ig_in, w_in, dq_out, ig_out, kw_out, vw_out):
    for c in range(CHUNKS):
        for kvh in range(2):
            for g in range(GROUP):
                at = (kvh * GROUP + g) * HEAD
                dq_out[c * 16 : (c + 1) * 16, at : at + HEAD] = dq_in[kvh, c, g]
    ig_out[...] = ig_in[...]
    for t, out in enumerate((kw_out, vw_out)):
        for n in range(2):
            out[:, n * HEAD : (n + 1) * HEAD] = w_in[t, n]


def local_step(q, k, v, g, x, mk, mv, placement):
    anywhere = pl.BlockSpec(memory_space=pl.ANY)
    vmem = pl.BlockSpec(memory_space=pltpu.VMEM)
    dq, ig, w = pl.pallas_call(
        kernel,
        out_shape=(
            jax.ShapeDtypeStruct((2, CHUNKS, GROUP, 16, HEAD), BF16),
            jax.ShapeDtypeStruct((128, FEATS // 2), BF16),
            jax.ShapeDtypeStruct((2, 2, 64, HEAD), F32),
        ),
        in_specs=[anywhere] * 7 + [vmem],
        out_specs=(vmem, vmem, vmem),
        scratch_shapes=[pltpu.VMEM(shape, dtype) for shape, dtype in BUFFERS.values()]
        + [
            pltpu.SemaphoreType.DMA((NSEM,)),
            pltpu.SemaphoreType.DMA((NSEM,)),
            pltpu.SemaphoreType.DMA((NLOCAL,)),
        ],
        compiler_params=pltpu.CompilerParams(
            collective_id=0, has_side_effects=True, vmem_limit_bytes=67043328
        ),
    )(
        q.reshape(CHUNKS, 16, -1),
        g.reshape(CHUNKS, 16, -1),
        k.reshape(CHUNKS, 16, -1),
        v.reshape(CHUNKS, 16, -1),
        x.reshape(CHUNKS, 16, -1),
        mk,
        mv,
        placement,
    )
    return pl.pallas_call(
        finish,
        out_shape=(
            jax.ShapeDtypeStruct((128, 2 * GROUP * HEAD), BF16),
            jax.ShapeDtypeStruct((128, FEATS // 2), BF16),
            jax.ShapeDtypeStruct((64, 2 * HEAD), F32),
            jax.ShapeDtypeStruct((64, 2 * HEAD), F32),
        ),
        in_specs=[vmem] * 3,
        out_specs=(vmem,) * 4,
    )(dq, ig, w)


def solution(mesh):
    torus = Mesh(
        mesh.devices.reshape(4, 2, 4, 2, mesh.shape["tp"]), ("seq_0", "seq_1", "seq_2", "seq_3", "tp")
    )
    rows = P(SEQ, "tp")
    return jax.shard_map(
        local_step,
        mesh=torus,
        in_specs=(rows, rows, rows, rows, rows, P(None, "tp"), P(None, "tp"), P()),
        out_specs=(rows, rows, rows, rows),
        check_vma=False,
    )
```

```python
import math

import jax
import jax.numpy as jnp
from jax import lax
from jax.experimental import pallas as pl
from jax.experimental.pallas import tpu as pltpu
from jax.sharding import Mesh
from jax.sharding import PartitionSpec as P

F32 = jnp.float32
BF16 = jnp.bfloat16
Y, ZH, X, CORE, ZL = "seq_0", "seq_1", "seq_2", "seq_3", "tp"
SEQ = (Y, ZH, X, CORE)
MESH = pl.DeviceIdType.MESH

HEAD = 128
GROUP = 4
WINDOW = 4096
CHUNKS = 8
BAND = 4
FEATS = 4096
SCALE = 1.0 / math.sqrt(HEAD)
SCALE2 = SCALE * math.log2(math.e)
MASKED = -1e30
QROWS = 256
KROWS = 128
NSEM = 192
NLOCAL = 24


def key_chunks(cq):
    return list(range(max(0, cq - BAND), cq + 1))


TILE_AT = [KROWS * sum(len(key_chunks(c)) for c in range(cq)) for cq in range(CHUNKS)]
TILE_ROWS = KROWS * sum(len(key_chunks(c)) for c in range(CHUNKS))

UNIT_KV = (2, 4, 2, 16, HEAD)
UNIT_W = (2, 64, HEAD)


def reduce_buffers(name, unit):
    half = unit[1:]
    return {
        name + "_far": ((2, 4) + unit, BF16),
        name + "_rfar": ((2, 2, 4) + half, BF16),
        name + "_near": ((2, 2, 4) + unit, BF16),
        name + "_rnear": ((2, 2, 4) + unit, BF16),
        name + "_far2": ((2,) + unit, BF16),
        name + "_rfar2": ((2,) + unit, BF16),
        name + "_near2": ((2, 2) + unit, BF16),
        name + "_rnear2": ((2, 2) + unit, BF16),
    }


BUFFERS = {
    "kv": ((2, 4, 4) + UNIT_KV, BF16),
    "qg": ((2, CHUNKS, 4, GROUP, 16, HEAD), BF16),
    "kpb": ((32, KROWS, 128), F32),
    "e": ((4, TILE_ROWS, QROWS), F32),
    "dp": ((4, TILE_ROWS, QROWS), F32),
    "st": ((3, 4, BAND + 1, CHUNKS, QROWS), F32),
    "ss": ((3, CHUNKS, QROWS), F32),
    "sr": ((3, CHUNKS, QROWS), F32),
    "fac": ((4, BAND + 1, CHUNKS, QROWS), F32),
    "delta": ((CHUNKS, QROWS), F32),
    "acc": ((2, 4) + UNIT_KV, F32),
    "dqt": ((CHUNKS, HEAD, QROWS), F32),
    "dqf": ((CHUNKS, 2, 2, GROUP, 16, HEAD), F32),
    "dqr": ((CHUNKS, 2, GROUP, 16, HEAD), F32),
    "dqs": ((2, CHUNKS, GROUP, 16, HEAD), BF16),
    "dqz": ((2, CHUNKS, GROUP, 16, HEAD), BF16),
    "kt": ((CHUNKS, HEAD, KROWS), BF16),
    "qp": ((CHUNKS, QROWS), F32),
    "xg": ((CHUNKS, 2, 16, FEATS), BF16),
    "xt": ((32, 2, 64, 256), BF16),
    "xo": ((32, 64, 256), BF16),
    "kst": ((2, CHUNKS, 16, 2 * HEAD), BF16),
    "mat": ((2, 2, FEATS // 2, 2 * HEAD), BF16),
    "d2": ((2, CHUNKS, 2, 16, HEAD), BF16),
    "d2o": ((2, CHUNKS, 2, 16, HEAD), BF16),
    "dd": ((2, 2, 2, CHUNKS, 16, HEAD), BF16),
    "wown": ((2, 4, 4) + UNIT_W, F32),
    "wfin": ((2,) + UNIT_W, BF16),
    "wz": ((2, 2, 64, HEAD), BF16),
    **reduce_buffers("a", UNIT_KV),
    **reduce_buffers("w", UNIT_W),
}


def dot_tt(a, b):
    return lax.dot_general(a, b, (((1,), (1,)), ((), ())), preferred_element_type=F32)


def dot_nn(a, b):
    return lax.dot_general(a, b, (((1,), (0,)), ((), ())), preferred_element_type=F32)


def dot_tn(a, b):
    return lax.dot_general(a, b, (((0,), (0,)), ((), ())), preferred_element_type=F32)


def stack_rows(parts):
    return parts[0] if len(parts) == 1 else jnp.concatenate(parts, axis=0)


def positions(rp_in, kpb, qp, y, x, core):
    slots = rp_in[...].astype(F32).astype(BF16)

    def iota(shape, dim):
        return lax.broadcasted_iota(jnp.int32, shape, dim)

    def bits(a, at, width):
        return jnp.bitwise_and(jnp.right_shift(a, at), (1 << width) - 1)

    row, dev = iota((KROWS, 64), 0), iota((KROWS, 64), 1)
    p, zh, jj = bits(row, 5, 2), bits(row, 4, 1), bits(row, 1, 3)
    wide = iota((KROWS, 128), 0)
    inside = (bits(wide, 1, 3) * 128 + bits(wide, 0, 1)).astype(F32)
    ones = jnp.ones((64, 128), BF16)
    owner = [
        [((q * 2 + zh) * 4 + p) * 2 + core == dev for q in range(4)],
        [((p * 2 + zh) * 4 + q) * 2 + core == dev for q in range(4)],
    ]
    for c in range(CHUNKS):
        block = (dev == jj + 8 * c).astype(F32).astype(BF16)
        rows = dot_nn(block, slots)
        for q in range(4):
            picked = jnp.where(owner[c // 4][q], rows, 0.0).astype(BF16)
            kpb[c // 4 * 16 + q * 4 + c % 4] = (
                dot_nn(picked, ones) * 2.0 + (inside + float(c * 1024))
            )

    dev, lane = iota((64, QROWS), 0), iota((64, QROWS), 1)
    zh, co, jj = bits(lane, 7, 1), bits(lane, 6, 1), bits(lane, 1, 3)
    pick = (((y * 2 + zh) * 4 + x) * 2 + co == dev).astype(F32).astype(BF16)
    slot = dot_nn(slots, pick)
    here = bits(dev, 0, 3) == jj
    pos = jnp.where(here, slot * 2.0 + (dev * 128 + bits(lane, 0, 1)).astype(F32), 0.0)
    qp[...] = jnp.sum(pos.reshape(CHUNKS, 8, QROWS), axis=1)


def kernel(
    q_in, g_in, k_in, v_in, x_in, mk_in, mv_in, rp_in, dq_out, ig_out, w_out, *scratch
):
    ssem, rsem, lsem = scratch[-3:]
    b = dict(zip(BUFFERS, scratch[:-3]))
    y, zh, x, core, zl = (lax.axis_index(a) for a in (Y, ZH, X, CORE, ZL))

    def turn(i, by):
        return lax.rem(i + by, 4)

    z = 2 * zh + zl
    zp, zm = turn(z, 1), turn(z, 3)
    zp_h, zp_l = lax.div(zp, 2), lax.rem(zp, 2)
    zm_h, zm_l = lax.div(zm, 2), lax.rem(zm, 2)
    oh, oc, ol = 1 - zh, 1 - core, 1 - zl
    d_core, d_tp = {CORE: oc}, {ZL: ol}
    across = ((d_tp, zh), ({ZH: oh, ZL: ol}, oh))
    d_zp, d_zm = {ZH: zp_h, ZL: zp_l}, {ZH: zm_h, ZL: zm_l}
    step_of = {a: ({a: turn(i, 1)}, {a: turn(i, 3)}) for a, i in ((X, x), (Y, y))}
    far_of = {X: {X: turn(x, 2)}, Y: {Y: turn(y, 2)}}
    d_zh = {ZH: oh}
    qi, pi = (y, x), (x, y)
    q_to = (step_of[Y], step_of[X])
    p_to = (step_of[X], step_of[Y])
    p_far = (far_of[X], far_of[Y])

    names = {}
    pending = []

    def remote(name, src, dst, dev):
        i = names.setdefault(name, len(names))
        return pltpu.make_async_remote_copy(
            src_ref=src,
            dst_ref=dst,
            send_sem=ssem.at[i],
            recv_sem=rsem.at[i],
            device_id=dev,
            device_id_type=MESH,
        )

    def send(name, src, dst, dev):
        remote(name, src, dst, dev).start()
        pending.append((name, src, dst, dev))

    def arrived(name, dst):
        remote(name, dst, dst, d_core).wait_recv()

    local_names = {}

    def local(name, src, dst):
        i = local_names.setdefault(name, len(local_names))
        return pltpu.make_async_copy(src, dst, lsem.at[i])

    def lanes(start, width=128):
        return pl.ds(pl.multiple_of(start, 128), width)

    kv, qg, xg, mat = b["kv"], b["qg"], b["xg"], b["mat"]
    own_x = local("x", x_in, xg.at[:, zh, :, lanes(zl * (FEATS // 2), FEATS // 2)])
    half_feats = FEATS // 2
    quarter_feats = FEATS // 4
    own_m = [
        local(("m", t), ref.at[pl.ds(pl.multiple_of(zl * half_feats, half_feats), half_feats), :], mat.at[0, t])
        for t, ref in enumerate((mk_in, mv_in))
    ]
    kst = b["kst"]
    stage = [local(("kst", t), ref, kst.at[t]) for t, ref in enumerate((k_in, v_in))]
    for c in stage:
        c.start()

    barrier = pltpu.get_barrier_semaphore()
    peers = [d_core, *step_of[X], *step_of[Y], *far_of.values(), d_zp, d_zm, d_zh]
    for dev in peers:
        pl.semaphore_signal(barrier, inc=1, device_id=dev, device_id_type=MESH)
    pl.semaphore_wait(barrier, len(peers))

    for c in stage:
        c.wait()

    for h in range(2):
        for r, (dev, head) in enumerate(across):
            for t in range(2):
                send(
                    ("zkv", h, t, r),
                    kst.at[t, pl.ds(4 * h, 4), :, lanes(head * HEAD)],
                    kv.at[h, qi[h], pi[h], t, :, zh],
                    dev,
                )
    for t, ref in enumerate((q_in, g_in)):
        for r, (dev, head) in enumerate(across):
            for g in range(GROUP):
                send(
                    ("qz", t, r, g),
                    ref.at[:, :, lanes(head * GROUP * HEAD + g * HEAD)],
                    qg.at[t, :, 2 * zh + core, g],
                    dev,
                )

    unit_offs = (0, 3, 1, 2)

    def unit_piece(h, n, side):
        unit = kv.at[h, qi[h], turn(pi[h], unit_offs[n])]
        return ("q", h, n, side), unit, unit, q_to[h][side]

    def send_unit(h, n):
        for side in range(2):
            send(*unit_piece(h, n, side))

    def near_piece(h, n, side):
        return kv.at[h, turn(qi[h], 3 if side == 0 else 1), turn(pi[h], unit_offs[n])]

    def forward_piece(h, n, side):
        src = near_piece(h, n, side).at[side]
        return ("qf", h, n, side), src, src, q_to[h][side]

    def forward_unit(h, n):
        for side in range(2):
            arrived(("q", h, n, side), near_piece(h, n, side))
            remote(*forward_piece(h, n, side)).start()
            if n == 0:
                pending.append(forward_piece(h, n, side))

    for h in range(2):
        for r, (dev, head) in enumerate(across):
            for t in range(2):
                arrived(("zkv", h, t, r), kv.at[h, qi[h], pi[h], t, :, head])
        unit = kv.at[h, qi[h], pi[h]]
        for side in range(2):
            send(("p", h, side), unit, unit, p_to[h][side])
        send_unit(h, 0)
    own_x.start()
    for c in own_m:
        c.start()
    dqt = b["dqt"]
    dqt[...] = jnp.zeros(dqt.shape, F32)
    b["st"][0] = jnp.full(b["st"].shape[1:], MASKED, F32)
    b["st"][1:] = jnp.zeros((2,) + b["st"].shape[1:], F32)
    positions(rp_in, b["kpb"], b["qp"], y, x, core)
    for h in range(2):
        for side in range(2):
            src = kv.at[h, qi[h], turn(pi[h], 3 if side == 0 else 1)]
            arrived(("p", h, side), src)
            send(("pf", h, side), src.at[side], src.at[side], p_to[h][side])
        for side in range(2):
            send_unit(h, 1 + side)
    for h in range(2):
        forward_unit(h, 0)
    for t in range(2):
        for r, (dev, head) in enumerate(across):
            for g in range(GROUP):
                arrived(("qz", t, r, g), qg.at[t, :, 2 * head + core, g])
            src = qg.at[t, :, 2 * head + core]
            send(("qc", t, r), src, src, d_core)

    def send_matrix(t):
        ref = (mk_in, mv_in)[t]
        for r, (dev, _) in enumerate(across):
            at = (2 * r + core) * 512
            src = ref.at[pl.ds(pl.multiple_of(ol * half_feats + at, 512), 512), :]
            dst = mat.at[1, t, pl.ds(pl.multiple_of(at, 512), 512), :]
            yield ("m", t, r), src, dst, dev

    def matrix_part(t, r, which):
        return mat.at[1, t, pl.ds(pl.multiple_of((2 * r + which) * 512, 512), 512), :]

    mine = xg.at[:, zh, :, lanes(zl * half_feats, half_feats)]
    send("x+", x_in, mine, d_zp)
    send("x-", x_in, mine, d_zm)
    for copy in send_matrix(0):
        send(*copy)
    for h in range(2):
        for side in range(2):
            arrived(("pf", h, side), kv.at[h, qi[h], turn(pi[h], 2), side])
        send_unit(h, 3)
    for t in range(2):
        for r, (dev, head) in enumerate(across):
            arrived(("qc", t, r), qg.at[t, :, 2 * head + oc])

    def queries(t, cq):
        return qg[t, cq].reshape(QROWS, HEAD)

    def keys(t, at, cks):
        return stack_rows(
            [kv[ck // 4, at[ck // 4], :, t, ck % 4].reshape(KROWS, HEAD) for ck in cks]
        )

    st, e_ref, dp_ref = b["st"], b["e"], b["dp"]

    def first_pass(s, carry):
        late = lax.div(s, 2)
        off = (1 - late) * s + late * (5 - s)

        @pl.when(s == 1)
        def _():
            for n in range(1, 4):
                for h in range(2):
                    forward_unit(h, n)

        @pl.when(s == 3)
        def _():
            for n in range(4):
                for h in range(2):
                    for side in range(2):
                        arrived(
                            ("qf", h, n, side),
                            kv.at[h, turn(qi[h], 2), turn(pi[h], unit_offs[n]), side],
                        )

        at = (turn(y, off), turn(x, off))
        for cq in range(CHUNKS):
            cks = key_chunks(cq)
            scores = dot_tt(keys(0, at, cks), queries(0, cq))
            dprobs = dot_tt(keys(1, at, cks), queries(1, cq))
            qpos = b["qp"][cq : cq + 1, :]
            for n, ck in enumerate(cks):
                part = slice(n * KROWS, (n + 1) * KROWS)
                score, dprob = scores[part] * SCALE2, dprobs[part]
                if ck == cq or ck == cq - BAND:
                    kpb = b["kpb"][ck // 4 * 16 + at[ck // 4] * 4 + ck % 4]
                    kpos = jnp.concatenate([kpb, kpb], axis=1)
                    seen = kpos <= qpos if ck == cq else kpos > qpos - WINDOW
                    score = jnp.where(seen, score, MASKED)
                top = jnp.max(score, axis=0, keepdims=True)
                expo = jnp.exp2(score - top)
                rows = pl.ds(TILE_AT[cq] + n * KROWS, KROWS)
                e_ref[off, rows, :] = expo
                dp_ref[off, rows, :] = dprob
                row = slice(cq, cq + 1)
                st[0, off, cq - ck, row, :] = top
                st[1, off, cq - ck, row, :] = jnp.sum(expo, axis=0, keepdims=True)
                st[2, off, cq - ck, row, :] = jnp.sum(expo * dprob, axis=0, keepdims=True)
        return carry

    lax.fori_loop(0, 4, first_pass, 0)
    for h in range(2):
        for n in range(4):
            for side in range(2):
                if n:
                    pending.append(forward_piece(h, n, side))

    ss, sr = b["ss"], b["sr"]
    top_l = jnp.max(st[0], axis=(0, 1))
    fac_l = jnp.exp2(st[0] - top_l[None, None])
    sum_l = jnp.sum(st[1] * fac_l, axis=(0, 1))
    wgt_l = jnp.sum(st[2] * fac_l, axis=(0, 1))
    ss[0] = top_l
    ss[1] = sum_l
    ss[2] = wgt_l
    send("stat", ss, sr, d_core)

    def forward_input(names_only=False):
        for name, src_h, src_l, start, dev in (
            ("x+", zm_h, zm_l, 0, d_zp),
            ("x-", zp_h, zp_l, quarter_feats, d_zm),
        ):
            src = xg.at[:, src_h, :, lanes(src_l * half_feats + start, quarter_feats)]
            if names_only:
                pending.append(("far " + name, src, src, dev))
            else:
                arrived(name, xg.at[:, src_h, :, lanes(src_l * half_feats, half_feats)])
                remote("far " + name, src, src, dev).start()

    arrived("stat", sr)
    top = jnp.maximum(top_l, sr[0])
    mine_f = jnp.exp2(top_l - top)
    other_f = jnp.exp2(sr[0] - top)
    total = sum_l * mine_f + sr[1] * other_f
    b["delta"][...] = (wgt_l * mine_f + sr[2] * other_f) / total
    b["fac"][...] = fac_l * (mine_f / total)[None, None]

    offs = (2, 1, 3, 0)

    def reducer(name, unit_at):
        far, rfar = b[name + "_far"], b[name + "_rfar"]
        near, rnear = b[name + "_near"], b[name + "_rnear"]
        far2, rfar2 = b[name + "_far2"], b[name + "_rfar2"]
        near2, rnear2 = b[name + "_near2"], b[name + "_rnear2"]

        def place(h, n):
            return turn(pi[h], offs[n])

        def far_copy(h, n, side):
            p = place(h, n)
            return (
                (name, "far", h, n, side),
                far.at[h, p, side],
                rfar.at[h, side, p],
                q_to[h][side],
            )

        def near_copy(h, n, side):
            p = place(h, n)
            return (
                (name, "near", h, n, side),
                near.at[h, side, p],
                rnear.at[h, side, p],
                q_to[h][side],
            )

        def start_far():
            for n in range(4):
                for h in range(2):
                    p = place(h, n)
                    far[h, p] = unit_at(h, turn(qi[h], 2), p).astype(BF16)
                    for side in range(2):
                        remote(*far_copy(h, n, side)).start()

        def start_near(side):
            for n in range(4):
                for h in range(2):
                    p = place(h, n)
                    value = unit_at(h, turn(qi[h], 1 if side == 0 else 3), p)
                    arrived((name, "far", h, n, side), rfar.at[h, side, p])
                    near[h, side, p, 1 - side] = value[1 - side].astype(BF16)
                    near[h, side, p, side] = (value[side] + rfar[h, side, p].astype(F32)).astype(
                        BF16
                    )
                    remote(*near_copy(h, n, side)).start()

        def note_sends():
            for h in range(2):
                for n in range(4):
                    for side in range(2):
                        pending.append(far_copy(h, n, side))
                        pending.append(near_copy(h, n, side))

        def own_unit(n):
            out = []
            for h in range(2):
                p = place(h, n)
                for side in range(2):
                    arrived((name, "near", h, n, side), rnear.at[h, side, p])
                value = (
                    unit_at(h, qi[h], p)
                    + rnear[h, 0, p].astype(F32)
                    + rnear[h, 1, p].astype(F32)
                )
                if n == 0:
                    far2[h] = value.astype(BF16)
                    send((name, "far2", h), far2.at[h], rfar2.at[h], p_far[h])
                elif n < 3:
                    side = n - 1
                    near2[h, side] = value.astype(BF16)
                    send(
                        (name, "near2", h, side),
                        near2.at[h, side],
                        rnear2.at[h, side],
                        p_to[h][side],
                    )
                else:
                    for side in range(2):
                        arrived((name, "near2", h, side), rnear2.at[h, side])
                    arrived((name, "far2", h), rfar2.at[h])
                    out.append(
                        (value + rfar2[h].astype(F32))
                        + (rnear2[h, 0].astype(F32) + rnear2[h, 1].astype(F32))
                    )
            return out

        return start_far, start_near, note_sends, own_unit

    acc = b["acc"]
    start_far, start_near, note_sends, own_unit = reducer("a", lambda h, q, p: acc[h, p])

    fac, delta, kt = b["fac"], b["delta"], b["kt"]

    def second_pass(s, carry):
        late = lax.div(s, 2)
        off = (1 - late) * (2 + s) + late * (3 - s)
        at = (turn(y, off), turn(x, off))
        for ck in range(CHUNKS):
            kt[ck] = keys(0, at, [ck]).T
        for cq in range(CHUNKS):
            cks = key_chunks(cq)
            probs, dscores = [], []
            for n, ck in enumerate(cks):
                rows = pl.ds(TILE_AT[cq] + n * KROWS, KROWS)
                prob = e_ref[off, rows, :] * fac[off, cq - ck, cq : cq + 1, :]
                diff = dp_ref[off, rows, :] - delta[cq : cq + 1, :]
                probs.append(prob.astype(BF16))
                dscores.append((prob * diff).astype(BF16))
            prob, dscore = stack_rows(probs), stack_rows(dscores)
            grads = (dot_nn(dscore, queries(0, cq)), dot_nn(prob, queries(1, cq)))
            for t in range(2):
                for n, ck in enumerate(cks):
                    part = grads[t][n * KROWS : (n + 1) * KROWS].reshape(4, 2, 16, HEAD)
                    if ck == cq:
                        acc[ck // 4, :, t, ck % 4] = part
                    else:
                        acc[ck // 4, :, t, ck % 4] = acc[ck // 4, :, t, ck % 4] + part
            flipped = jnp.concatenate([kt[ck] for ck in cks], axis=1)
            dqt[cq] = dqt[cq] + dot_nn(flipped, dscore)

        @pl.when(s == 0)
        def _():
            start_far()
            forward_input()
            for copy in send_matrix(1):
                remote(*copy).start()

        @pl.when(s == 1)
        def _():
            start_near(1)

        @pl.when(s == 2)
        def _():
            start_near(0)

        return carry

    lax.fori_loop(0, 4, second_pass, 0)
    note_sends()
    forward_input(names_only=True)
    pending.extend(send_matrix(1))

    dqf, dqr, dqs, dqz = b["dqf"], b["dqr"], b["dqs"], b["dqz"]
    for cq in range(CHUNKS):
        dqf[cq] = (dqt[cq].T * SCALE).reshape(2, 2, GROUP, 16, HEAD)
    send("dqc", dqf.at[:, :, oc], dqr, d_core)
    own_unit(0)
    own_x.wait()
    far_h = 1 - zh
    arrived("far x+", xg.at[:, far_h, :, lanes(zl * half_feats, quarter_feats)])
    arrived("far x-", xg.at[:, far_h, :, lanes(zl * half_feats + quarter_feats, quarter_feats)])
    xt, xo = b["xt"], b["xo"]

    def flip_input(i, carry):
        for n in range(4):
            at = i * 4 + n
            block = xg[:, :, :, lanes(at * 128)].reshape(256, 128)
            xt[at] = block.T.reshape(2, 64, 256)
        return carry

    lax.fori_loop(0, 8, flip_input, 0)
    send("xt", xt.at[:, oc], xo, d_core)
    own_unit(1)
    own_unit(2)
    arrived("dqc", dqr)
    for n in range(2):
        dqs[n] = (dqf[:, n, core] + dqr[:, n]).astype(BF16)
    for r, (dev, other) in enumerate(across):
        send(("dqz", r), dqs.at[other], dqz.at[zh], dev)
    d2, d2o, dd = b["d2"], b["d2o"], b["dd"]
    for h, value in enumerate(own_unit(3)):
        d2[0, 4 * h : 4 * h + 4] = (value[0] * SCALE).astype(BF16)
        d2[1, 4 * h : 4 * h + 4] = value[1].astype(BF16)
    send("d2", d2, d2o, d_core)
    for r, (dev, other) in enumerate(across):
        for t in range(2):
            send(("dz", t, r), d2.at[t, :, other], dd.at[0, t, zh], dev)
    for t in range(2):
        send(("dy", t), d2.at[t, :, oh], dd.at[1, t, zh], d_zh)
        dd[1, t, zh] = d2[t, :, zh]

    wown = b["wown"]

    def grad_cols(ref):
        return jnp.concatenate([ref[0].reshape(256, HEAD), ref[1].reshape(256, HEAD)], axis=1)

    def weight_blocks(first):
        cols = grad_cols(d2 if first else d2o)

        def body(wy, carry):
            at = pl.ds(wy * 8, 8)
            rows = (xt[at, core] if first else xo[at]).reshape(512, 256)
            part = dot_nn(rows, cols)
            for wz in range(2):
                for wx in range(4):
                    for h, (wq, wp) in enumerate(((wy, wx), (wx, wy))):
                        base = (wz * 4 + wx) * 64
                        block = part[base : base + 64, h * HEAD : (h + 1) * HEAD]
                        if first:
                            wown[h, wq, wp, wz] = block
                        else:
                            wown[h, wq, wp, wz] = wown[h, wq, wp, wz] + block
            return carry

        lax.fori_loop(0, 4, body, 0)

    weight_blocks(True)
    arrived("xt", xo)
    arrived("d2", d2o)
    weight_blocks(False)
    w_far, w_near, w_note, w_unit = reducer("w", lambda h, q, p: wown[h, q, p])
    w_far()

    for c in own_m:
        c.wait()
    for t in range(2):
        for r in range(2):
            arrived(("m", t, r), matrix_part(t, r, core))
            src = matrix_part(t, r, core)
            send(("mc", t, r), src, src, d_core)
    w_near(0)
    w_near(1)
    w_note()
    for t in range(2):
        for r, (dev, other) in enumerate(across):
            arrived(("dz", t, r), dd.at[0, t, other])
            arrived(("mc", t, r), matrix_part(t, r, oc))
        arrived(("dy", t), dd.at[1, t, oh])

    def tokens(which, t):
        return jnp.concatenate(
            [dd[which, t, a].reshape(128, HEAD) for a in range(2)], axis=1
        )

    token_grads = jnp.concatenate([tokens(w, t) for w in range(2) for t in range(2)], axis=1)

    def input_block(i, carry):
        rows = pl.ds(pl.multiple_of(i * 512, 512), 512)
        cols = jnp.concatenate([mat[w, t, rows, :] for w in range(2) for t in range(2)], axis=1)
        ig_out[:, lanes(i * 512, 512)] = dot_tt(token_grads, cols).astype(BF16)
        return carry

    lax.fori_loop(0, 4, input_block, 0)
    for r, (dev, other) in enumerate(across):
        arrived(("dqz", r), dqz.at[other])
    dq_out[...] = dqz[...]
    w_unit(0)
    w_unit(1)
    w_unit(2)
    wfin, wz_ref = b["wfin"], b["wz"]
    for h, value in enumerate(w_unit(3)):
        wfin[h] = value.astype(BF16)
    for r, (dev, other) in enumerate(across):
        send(("ws", r), wfin.at[:, other], wz_ref.at[:, zh], dev)
    for r, (dev, other) in enumerate(across):
        arrived(("ws", r), wz_ref.at[:, other])
    w_out[...] = wz_ref[...].astype(F32)

    for copy in pending:
        remote(*copy).wait_send()
    assert len(names) <= NSEM and len(local_names) <= NLOCAL


def finish(dq_in, ig_in, w_in, dq_out, ig_out, kw_out, vw_out):
    for c in range(CHUNKS):
        for kvh in range(2):
            for g in range(GROUP):
                at = (kvh * GROUP + g) * HEAD
                dq_out[c * 16 : (c + 1) * 16, at : at + HEAD] = dq_in[kvh, c, g]
    ig_out[...] = ig_in[...]
    for t, out in enumerate((kw_out, vw_out)):
        for n in range(2):
            out[:, n * HEAD : (n + 1) * HEAD] = w_in[t, n]


def local_step(q, k, v, g, x, mk, mv, placement):
    anywhere = pl.BlockSpec(memory_space=pl.ANY)
    vmem = pl.BlockSpec(memory_space=pltpu.VMEM)
    dq, ig, w = pl.pallas_call(
        kernel,
        out_shape=(
            jax.ShapeDtypeStruct((2, CHUNKS, GROUP, 16, HEAD), BF16),
            jax.ShapeDtypeStruct((128, FEATS // 2), BF16),
            jax.ShapeDtypeStruct((2, 2, 64, HEAD), F32),
        ),
        in_specs=[anywhere] * 7 + [vmem],
        out_specs=(vmem, vmem, vmem),
        scratch_shapes=[pltpu.VMEM(shape, dtype) for shape, dtype in BUFFERS.values()]
        + [
            pltpu.SemaphoreType.DMA((NSEM,)),
            pltpu.SemaphoreType.DMA((NSEM,)),
            pltpu.SemaphoreType.DMA((NLOCAL,)),
        ],
        compiler_params=pltpu.CompilerParams(
            collective_id=0, has_side_effects=True, vmem_limit_bytes=67043328
        ),
    )(
        q.reshape(CHUNKS, 16, -1),
        g.reshape(CHUNKS, 16, -1),
        k.reshape(CHUNKS, 16, -1),
        v.reshape(CHUNKS, 16, -1),
        x.reshape(CHUNKS, 16, -1),
        mk,
        mv,
        placement,
    )
    return pl.pallas_call(
        finish,
        out_shape=(
            jax.ShapeDtypeStruct((128, 2 * GROUP * HEAD), BF16),
            jax.ShapeDtypeStruct((128, FEATS // 2), BF16),
            jax.ShapeDtypeStruct((64, 2 * HEAD), F32),
            jax.ShapeDtypeStruct((64, 2 * HEAD), F32),
        ),
        in_specs=[vmem] * 3,
        out_specs=(vmem,) * 4,
    )(dq, ig, w)


def solution(mesh):
    torus = Mesh(
        mesh.devices.reshape(4, 2, 4, 2, mesh.shape["tp"]), ("seq_0", "seq_1", "seq_2", "seq_3", "tp")
    )
    rows = P(SEQ, "tp")
    return jax.shard_map(
        local_step,
        mesh=torus,
        in_specs=(rows, rows, rows, rows, rows, P(None, "tp"), P(None, "tp"), P()),
        out_specs=(rows, rows, rows, rows),
        check_vma=False,
    )
```

```python
import math

import jax
import jax.numpy as jnp
from jax import lax
from jax.experimental import pallas as pl
from jax.experimental.pallas import tpu as pltpu
from jax.sharding import Mesh
from jax.sharding import PartitionSpec as P

F32 = jnp.float32
BF16 = jnp.bfloat16
Y, ZH, X, CORE, ZL = "seq_0", "seq_1", "seq_2", "seq_3", "tp"
SEQ = (Y, ZH, X, CORE)
MESH = pl.DeviceIdType.MESH

HEAD = 128
GROUP = 4
WINDOW = 4096
CHUNKS = 8
BAND = 4
FEATS = 4096
SCALE = 1.0 / math.sqrt(HEAD)
SCALE2 = SCALE * math.log2(math.e)
MASKED = -1e30
QROWS = 256
KROWS = 128
NSEM = 192
NLOCAL = 24


def key_chunks(cq):
    return list(range(max(0, cq - BAND), cq + 1))


TILE_AT = [KROWS * sum(len(key_chunks(c)) for c in range(cq)) for cq in range(CHUNKS)]
TILE_ROWS = KROWS * sum(len(key_chunks(c)) for c in range(CHUNKS))

UNIT_KV = (2, 4, 2, 16, HEAD)
UNIT_W = (2, 64, HEAD)


def reduce_buffers(name, unit):
    half = unit[1:]
    return {
        name + "_far": ((2, 4) + unit, BF16),
        name + "_rfar": ((2, 2, 4) + half, BF16),
        name + "_near": ((2, 2, 4) + unit, BF16),
        name + "_rnear": ((2, 2, 4) + unit, BF16),
        name + "_far2": ((2,) + unit, BF16),
        name + "_rfar2": ((2,) + unit, BF16),
        name + "_near2": ((2, 2) + unit, BF16),
        name + "_rnear2": ((2, 2) + unit, BF16),
    }


BUFFERS = {
    "kv": ((2, 4, 4) + UNIT_KV, BF16),
    "qg": ((2, CHUNKS, 4, GROUP, 16, HEAD), BF16),
    "kpb": ((32, KROWS, 128), F32),
    "e": ((4, TILE_ROWS, QROWS), F32),
    "dp": ((4, TILE_ROWS, QROWS), F32),
    "st": ((3, 4, BAND + 1, CHUNKS, QROWS), F32),
    "ss": ((3, CHUNKS, QROWS), F32),
    "sr": ((3, CHUNKS, QROWS), F32),
    "fac": ((4, BAND + 1, CHUNKS, QROWS), F32),
    "delta": ((CHUNKS, QROWS), F32),
    "acc": ((2, 4) + UNIT_KV, F32),
    "dqt": ((CHUNKS, HEAD, QROWS), F32),
    "dqf": ((CHUNKS, 2, 2, GROUP, 16, HEAD), F32),
    "dqr": ((CHUNKS, 2, GROUP, 16, HEAD), F32),
    "dqs": ((2, CHUNKS, GROUP, 16, HEAD), BF16),
    "dqz": ((2, CHUNKS, GROUP, 16, HEAD), BF16),
    "kt": ((CHUNKS, HEAD, KROWS), BF16),
    "qp": ((CHUNKS, QROWS), F32),
    "xg": ((CHUNKS, 2, 16, FEATS), BF16),
    "xt": ((32, 2, 64, 256), BF16),
    "xo": ((32, 64, 256), BF16),
    "kst": ((2, CHUNKS, 16, 2 * HEAD), BF16),
    "mat": ((2, 2, FEATS // 2, 2 * HEAD), BF16),
    "d2": ((2, CHUNKS, 2, 16, HEAD), BF16),
    "d2o": ((2, CHUNKS, 2, 16, HEAD), BF16),
    "dd": ((2, 2, 2, CHUNKS, 16, HEAD), BF16),
    "wown": ((2, 4, 4) + UNIT_W, F32),
    "wmine": ((2,) + UNIT_W, BF16),
    "wz": ((4, 2, 2, 64, HEAD), BF16),
    "wv": ((2, 2, 64, HEAD), F32),
    "igv": ((128, FEATS // 2), BF16),
    **reduce_buffers("a", UNIT_KV),
    **reduce_buffers("w", UNIT_W),
}


def dot_tt(a, b):
    return lax.dot_general(a, b, (((1,), (1,)), ((), ())), preferred_element_type=F32)


def dot_nn(a, b):
    return lax.dot_general(a, b, (((1,), (0,)), ((), ())), preferred_element_type=F32)


def dot_tn(a, b):
    return lax.dot_general(a, b, (((0,), (0,)), ((), ())), preferred_element_type=F32)


def stack_rows(parts):
    return parts[0] if len(parts) == 1 else jnp.concatenate(parts, axis=0)


def positions(rp_in, kpb, qp, y, x, core):
    slots = rp_in[...].astype(F32).astype(BF16)

    def iota(shape, dim):
        return lax.broadcasted_iota(jnp.int32, shape, dim)

    def bits(a, at, width):
        return jnp.bitwise_and(jnp.right_shift(a, at), (1 << width) - 1)

    row, dev = iota((KROWS, 64), 0), iota((KROWS, 64), 1)
    p, zh, jj = bits(row, 5, 2), bits(row, 4, 1), bits(row, 1, 3)
    wide = iota((KROWS, 128), 0)
    inside = (bits(wide, 1, 3) * 128 + bits(wide, 0, 1)).astype(F32)
    ones = jnp.ones((64, 128), BF16)
    owner = [
        [((q * 2 + zh) * 4 + p) * 2 + core == dev for q in range(4)],
        [((p * 2 + zh) * 4 + q) * 2 + core == dev for q in range(4)],
    ]
    for c in range(CHUNKS):
        block = (dev == jj + 8 * c).astype(F32).astype(BF16)
        rows = dot_nn(block, slots)
        for q in range(4):
            picked = jnp.where(owner[c // 4][q], rows, 0.0).astype(BF16)
            kpb[c // 4 * 16 + q * 4 + c % 4] = (
                dot_nn(picked, ones) * 2.0 + (inside + float(c * 1024))
            )

    dev, lane = iota((64, QROWS), 0), iota((64, QROWS), 1)
    zh, co, jj = bits(lane, 7, 1), bits(lane, 6, 1), bits(lane, 1, 3)
    pick = (((y * 2 + zh) * 4 + x) * 2 + co == dev).astype(F32).astype(BF16)
    slot = dot_nn(slots, pick)
    here = bits(dev, 0, 3) == jj
    pos = jnp.where(here, slot * 2.0 + (dev * 128 + bits(lane, 0, 1)).astype(F32), 0.0)
    qp[...] = jnp.sum(pos.reshape(CHUNKS, 8, QROWS), axis=1)


def kernel(
    q_in, g_in, k_in, v_in, x_in, mk_in, mv_in, rp_in, dq_out, ig_out, w_out, *scratch
):
    ssem, rsem, lsem = scratch[-3:]
    b = dict(zip(BUFFERS, scratch[:-3]))
    y, zh, x, core, zl = (lax.axis_index(a) for a in (Y, ZH, X, CORE, ZL))

    def turn(i, by):
        return lax.rem(i + by, 4)

    z = 2 * zh + zl
    zp, zm = turn(z, 1), turn(z, 3)
    zp_h, zp_l = lax.div(zp, 2), lax.rem(zp, 2)
    zm_h, zm_l = lax.div(zm, 2), lax.rem(zm, 2)
    oh, oc, ol = 1 - zh, 1 - core, 1 - zl
    d_core, d_tp = {CORE: oc}, {ZL: ol}
    across = ((d_tp, zh), ({ZH: oh, ZL: ol}, oh))
    d_zp, d_zm = {ZH: zp_h, ZL: zp_l}, {ZH: zm_h, ZL: zm_l}
    step_of = {a: ({a: turn(i, 1)}, {a: turn(i, 3)}) for a, i in ((X, x), (Y, y))}
    far_of = {X: {X: turn(x, 2)}, Y: {Y: turn(y, 2)}}
    d_zh = {ZH: oh}
    qi, pi = (y, x), (x, y)
    q_to = (step_of[Y], step_of[X])
    p_to = (step_of[X], step_of[Y])
    p_far = (far_of[X], far_of[Y])

    names = {}
    pending = []

    def remote(name, src, dst, dev):
        i = names.setdefault(name, len(names))
        return pltpu.make_async_remote_copy(
            src_ref=src,
            dst_ref=dst,
            send_sem=ssem.at[i],
            recv_sem=rsem.at[i],
            device_id=dev,
            device_id_type=MESH,
        )

    def send(name, src, dst, dev):
        remote(name, src, dst, dev).start()
        pending.append((name, src, dst, dev))

    def arrived(name, dst):
        remote(name, dst, dst, d_core).wait_recv()

    local_names = {}

    def local(name, src, dst):
        i = local_names.setdefault(name, len(local_names))
        return pltpu.make_async_copy(src, dst, lsem.at[i])

    def lanes(start, width=128):
        return pl.ds(pl.multiple_of(start, 128), width)

    kv, qg, xg, mat = b["kv"], b["qg"], b["xg"], b["mat"]
    own_x = local("x", x_in, xg.at[:, zh, :, lanes(zl * (FEATS // 2), FEATS // 2)])
    half_feats = FEATS // 2
    quarter_feats = FEATS // 4
    own_m = [
        local(("m", t), ref.at[pl.ds(pl.multiple_of(zl * half_feats, half_feats), half_feats), :], mat.at[0, t])
        for t, ref in enumerate((mk_in, mv_in))
    ]
    kst = b["kst"]
    stage = [local(("kst", t), ref, kst.at[t]) for t, ref in enumerate((k_in, v_in))]
    for c in stage:
        c.start()

    barrier = pltpu.get_barrier_semaphore()
    peers = [d_core, *step_of[X], *step_of[Y], *far_of.values(), d_zp, d_zm, d_zh]
    for dev in peers:
        pl.semaphore_signal(barrier, inc=1, device_id=dev, device_id_type=MESH)
    pl.semaphore_wait(barrier, len(peers))

    for c in stage:
        c.wait()

    for h in range(2):
        for r, (dev, head) in enumerate(across):
            for t in range(2):
                send(
                    ("zkv", h, t, r),
                    kst.at[t, pl.ds(4 * h, 4), :, lanes(head * HEAD)],
                    kv.at[h, qi[h], pi[h], t, :, zh],
                    dev,
                )
    for t, ref in enumerate((q_in, g_in)):
        for r, (dev, head) in enumerate(across):
            for g in range(GROUP):
                send(
                    ("qz", t, r, g),
                    ref.at[:, :, lanes(head * GROUP * HEAD + g * HEAD)],
                    qg.at[t, :, 2 * zh + core, g],
                    dev,
                )

    unit_offs = (0, 3, 1, 2)

    def unit_piece(h, n, side):
        unit = kv.at[h, qi[h], turn(pi[h], unit_offs[n])]
        return ("q", h, n, side), unit, unit, q_to[h][side]

    def send_unit(h, n):
        for side in range(2):
            send(*unit_piece(h, n, side))

    def near_piece(h, n, side):
        return kv.at[h, turn(qi[h], 3 if side == 0 else 1), turn(pi[h], unit_offs[n])]

    def forward_piece(h, n, side):
        src = near_piece(h, n, side).at[side]
        return ("qf", h, n, side), src, src, q_to[h][side]

    def forward_unit(h, n):
        for side in range(2):
            arrived(("q", h, n, side), near_piece(h, n, side))
            remote(*forward_piece(h, n, side)).start()
            if n == 0:
                pending.append(forward_piece(h, n, side))

    for h in range(2):
        for r, (dev, head) in enumerate(across):
            for t in range(2):
                arrived(("zkv", h, t, r), kv.at[h, qi[h], pi[h], t, :, head])
        unit = kv.at[h, qi[h], pi[h]]
        for side in range(2):
            send(("p", h, side), unit, unit, p_to[h][side])
        send(("pf", h), unit, unit, p_far[h])
        send_unit(h, 0)
    own_x.start()
    for c in own_m:
        c.start()
    dqt = b["dqt"]
    dqt[...] = jnp.zeros(dqt.shape, F32)
    b["st"][0] = jnp.full(b["st"].shape[1:], MASKED, F32)
    b["st"][1:] = jnp.zeros((2,) + b["st"].shape[1:], F32)
    positions(rp_in, b["kpb"], b["qp"], y, x, core)
    for h in range(2):
        for side in range(2):
            src = kv.at[h, qi[h], turn(pi[h], 3 if side == 0 else 1)]
            arrived(("p", h, side), src)
        for side in range(2):
            send_unit(h, 1 + side)
    for h in range(2):
        forward_unit(h, 0)
    for t in range(2):
        for r, (dev, head) in enumerate(across):
            for g in range(GROUP):
                arrived(("qz", t, r, g), qg.at[t, :, 2 * head + core, g])
            src = qg.at[t, :, 2 * head + core]
            send(("qc", t, r), src, src, d_core)

    def send_matrix(t):
        ref = (mk_in, mv_in)[t]
        for r, (dev, _) in enumerate(across):
            at = (2 * r + core) * 512
            src = ref.at[pl.ds(pl.multiple_of(ol * half_feats + at, 512), 512), :]
            dst = mat.at[1, t, pl.ds(pl.multiple_of(at, 512), 512), :]
            yield ("m", t, r), src, dst, dev

    def matrix_part(t, r, which):
        return mat.at[1, t, pl.ds(pl.multiple_of((2 * r + which) * 512, 512), 512), :]

    mine = xg.at[:, zh, :, lanes(zl * half_feats, half_feats)]
    send("x+", x_in, mine, d_zp)
    send("x-", x_in, mine, d_zm)
    for copy in send_matrix(0):
        send(*copy)
    for h in range(2):
        arrived(("pf", h), kv.at[h, qi[h], turn(pi[h], 2)])
        send_unit(h, 3)
    for t in range(2):
        for r, (dev, head) in enumerate(across):
            arrived(("qc", t, r), qg.at[t, :, 2 * head + oc])

    def queries(t, cq):
        return qg[t, cq].reshape(QROWS, HEAD)

    def keys(t, at, cks):
        return stack_rows(
            [kv[ck // 4, at[ck // 4], :, t, ck % 4].reshape(KROWS, HEAD) for ck in cks]
        )

    st, e_ref, dp_ref = b["st"], b["e"], b["dp"]

    def first_pass(s, carry):
        late = lax.div(s, 2)
        off = (1 - late) * s + late * (5 - s)

        @pl.when(s == 1)
        def _():
            for n in range(1, 4):
                for h in range(2):
                    forward_unit(h, n)

        @pl.when(s == 3)
        def _():
            for n in range(4):
                for h in range(2):
                    for side in range(2):
                        arrived(
                            ("qf", h, n, side),
                            kv.at[h, turn(qi[h], 2), turn(pi[h], unit_offs[n]), side],
                        )

        at = (turn(y, off), turn(x, off))
        for cq in range(CHUNKS):
            cks = key_chunks(cq)
            scores = dot_tt(keys(0, at, cks), queries(0, cq))
            dprobs = dot_tt(keys(1, at, cks), queries(1, cq))
            qpos = b["qp"][cq : cq + 1, :]
            for n, ck in enumerate(cks):
                part = slice(n * KROWS, (n + 1) * KROWS)
                score, dprob = scores[part] * SCALE2, dprobs[part]
                if ck == cq or ck == cq - BAND:
                    kpb = b["kpb"][ck // 4 * 16 + at[ck // 4] * 4 + ck % 4]
                    kpos = jnp.concatenate([kpb, kpb], axis=1)
                    seen = kpos <= qpos if ck == cq else kpos > qpos - WINDOW
                    score = jnp.where(seen, score, MASKED)
                top = jnp.max(score, axis=0, keepdims=True)
                expo = jnp.exp2(score - top)
                rows = pl.ds(TILE_AT[cq] + n * KROWS, KROWS)
                e_ref[off, rows, :] = expo
                dp_ref[off, rows, :] = dprob
                row = slice(cq, cq + 1)
                st[0, off, cq - ck, row, :] = top
                st[1, off, cq - ck, row, :] = jnp.sum(expo, axis=0, keepdims=True)
                st[2, off, cq - ck, row, :] = jnp.sum(expo * dprob, axis=0, keepdims=True)
        return carry

    lax.fori_loop(0, 4, first_pass, 0)
    for h in range(2):
        for n in range(4):
            for side in range(2):
                if n:
                    pending.append(forward_piece(h, n, side))

    ss, sr = b["ss"], b["sr"]
    top_l = jnp.max(st[0], axis=(0, 1))
    fac_l = jnp.exp2(st[0] - top_l[None, None])
    sum_l = jnp.sum(st[1] * fac_l, axis=(0, 1))
    wgt_l = jnp.sum(st[2] * fac_l, axis=(0, 1))
    ss[0] = top_l
    ss[1] = sum_l
    ss[2] = wgt_l
    send("stat", ss, sr, d_core)

    def forward_input(names_only=False):
        for name, src_h, src_l, start, dev in (
            ("x+", zm_h, zm_l, 0, d_zp),
            ("x-", zp_h, zp_l, quarter_feats, d_zm),
        ):
            src = xg.at[:, src_h, :, lanes(src_l * half_feats + start, quarter_feats)]
            if names_only:
                pending.append(("far " + name, src, src, dev))
            else:
                arrived(name, xg.at[:, src_h, :, lanes(src_l * half_feats, half_feats)])
                remote("far " + name, src, src, dev).start()

    arrived("stat", sr)
    top = jnp.maximum(top_l, sr[0])
    mine_f = jnp.exp2(top_l - top)
    other_f = jnp.exp2(sr[0] - top)
    total = sum_l * mine_f + sr[1] * other_f
    b["delta"][...] = (wgt_l * mine_f + sr[2] * other_f) / total
    b["fac"][...] = fac_l * (mine_f / total)[None, None]

    offs = (2, 1, 3, 0)

    def reducer(name, unit_at, deliver=None):
        far, rfar = b[name + "_far"], b[name + "_rfar"]
        near, rnear = b[name + "_near"], b[name + "_rnear"]
        far2, rfar2 = b[name + "_far2"], b[name + "_rfar2"]
        near2, rnear2 = b[name + "_near2"], b[name + "_rnear2"]

        def place(h, n):
            return turn(pi[h], offs[n])

        def far_copy(h, n, side):
            p = place(h, n)
            return (
                (name, "far", h, n, side),
                far.at[h, p, side],
                rfar.at[h, side, p],
                q_to[h][side],
            )

        def near_copy(h, n, side):
            p = place(h, n)
            return (
                (name, "near", h, n, side),
                near.at[h, side, p],
                rnear.at[h, side, p],
                q_to[h][side],
            )

        def start_far():
            for n in range(4):
                for h in range(2):
                    p = place(h, n)
                    far[h, p] = unit_at(h, turn(qi[h], 2), p).astype(BF16)
                    for side in range(2):
                        remote(*far_copy(h, n, side)).start()

        def start_near(side):
            for n in range(4):
                for h in range(2):
                    p = place(h, n)
                    value = unit_at(h, turn(qi[h], 1 if side == 0 else 3), p)
                    arrived((name, "far", h, n, side), rfar.at[h, side, p])
                    near[h, side, p, 1 - side] = value[1 - side].astype(BF16)
                    near[h, side, p, side] = (value[side] + rfar[h, side, p].astype(F32)).astype(
                        BF16
                    )
                    remote(*near_copy(h, n, side)).start()

        def note_sends():
            for h in range(2):
                for n in range(4):
                    for side in range(2):
                        pending.append(far_copy(h, n, side))
                        pending.append(near_copy(h, n, side))

        def own_unit(n):
            out = []
            for h in range(2):
                p = place(h, n)
                for side in range(2):
                    arrived((name, "near", h, n, side), rnear.at[h, side, p])
                value = (
                    unit_at(h, qi[h], p)
                    + rnear[h, 0, p].astype(F32)
                    + rnear[h, 1, p].astype(F32)
                )
                if deliver:
                    deliver(h, n, value.astype(BF16))
                elif n == 0:
                    far2[h] = value.astype(BF16)
                    send((name, "far2", h), far2.at[h], rfar2.at[h], p_far[h])
                elif n < 3:
                    side = n - 1
                    near2[h, side] = value.astype(BF16)
                    send(
                        (name, "near2", h, side),
                        near2.at[h, side],
                        rnear2.at[h, side],
                        p_to[h][side],
                    )
                else:
                    for side in range(2):
                        arrived((name, "near2", h, side), rnear2.at[h, side])
                    arrived((name, "far2", h), rfar2.at[h])
                    out.append(
                        (value + rfar2[h].astype(F32))
                        + (rnear2[h, 0].astype(F32) + rnear2[h, 1].astype(F32))
                    )
            return out

        return start_far, start_near, note_sends, own_unit

    acc = b["acc"]
    start_far, start_near, note_sends, own_unit = reducer("a", lambda h, q, p: acc[h, p])

    fac, delta, kt = b["fac"], b["delta"], b["kt"]

    def second_pass(s, carry):
        late = lax.div(s, 2)
        off = (1 - late) * (2 + s) + late * (3 - s)
        at = (turn(y, off), turn(x, off))
        for ck in range(CHUNKS):
            kt[ck] = keys(0, at, [ck]).T
        for cq in range(CHUNKS):
            cks = key_chunks(cq)
            probs, dscores = [], []
            for n, ck in enumerate(cks):
                rows = pl.ds(TILE_AT[cq] + n * KROWS, KROWS)
                prob = e_ref[off, rows, :] * fac[off, cq - ck, cq : cq + 1, :]
                diff = dp_ref[off, rows, :] - delta[cq : cq + 1, :]
                probs.append(prob.astype(BF16))
                dscores.append((prob * diff).astype(BF16))
            prob, dscore = stack_rows(probs), stack_rows(dscores)
            grads = (dot_nn(dscore, queries(0, cq)), dot_nn(prob, queries(1, cq)))
            for t in range(2):
                for n, ck in enumerate(cks):
                    part = grads[t][n * KROWS : (n + 1) * KROWS].reshape(4, 2, 16, HEAD)
                    if ck == cq:
                        acc[ck // 4, :, t, ck % 4] = part
                    else:
                        acc[ck // 4, :, t, ck % 4] = acc[ck // 4, :, t, ck % 4] + part
            flipped = jnp.concatenate([kt[ck] for ck in cks], axis=1)
            dqt[cq] = dqt[cq] + dot_nn(flipped, dscore)

        @pl.when(s == 0)
        def _():
            start_far()
            forward_input()
            for copy in send_matrix(1):
                remote(*copy).start()

        @pl.when(s == 1)
        def _():
            start_near(1)

        @pl.when(s == 2)
        def _():
            start_near(0)

        return carry

    lax.fori_loop(0, 4, second_pass, 0)
    note_sends()
    forward_input(names_only=True)
    pending.extend(send_matrix(1))

    dqf, dqr, dqs, dqz = b["dqf"], b["dqr"], b["dqs"], b["dqz"]
    for cq in range(CHUNKS):
        dqf[cq] = (dqt[cq].T * SCALE).reshape(2, 2, GROUP, 16, HEAD)
    send("dqc", dqf.at[:, :, oc], dqr, d_core)
    own_unit(0)
    own_x.wait()
    far_h = 1 - zh
    arrived("far x+", xg.at[:, far_h, :, lanes(zl * half_feats, quarter_feats)])
    arrived("far x-", xg.at[:, far_h, :, lanes(zl * half_feats + quarter_feats, quarter_feats)])
    xt, xo = b["xt"], b["xo"]

    def flip_input(i, carry):
        for n in range(4):
            at = i * 4 + n
            block = xg[:, :, :, lanes(at * 128)].reshape(256, 128)
            xt[at] = block.T.reshape(2, 64, 256)
        return carry

    lax.fori_loop(0, 8, flip_input, 0)
    send("xt", xt.at[:, oc], xo, d_core)
    own_unit(1)
    own_unit(2)
    arrived("dqc", dqr)
    for n in range(2):
        dqs[n] = (dqf[:, n, core] + dqr[:, n]).astype(BF16)
    for r, (dev, other) in enumerate(across):
        send(("dqz", r), dqs.at[other], dqz.at[zh], dev)
    d2, d2o, dd = b["d2"], b["d2o"], b["dd"]
    for h, value in enumerate(own_unit(3)):
        d2[0, 4 * h : 4 * h + 4] = (value[0] * SCALE).astype(BF16)
        d2[1, 4 * h : 4 * h + 4] = value[1].astype(BF16)
    send("d2", d2, d2o, d_core)
    for r, (dev, other) in enumerate(across):
        for t in range(2):
            send(("dz", t, r), d2.at[t, :, other], dd.at[0, t, zh], dev)
    for t in range(2):
        send(("dy", t), d2.at[t, :, oh], dd.at[1, t, zh], d_zh)
        dd[1, t, zh] = d2[t, :, zh]

    wown = b["wown"]

    def grad_cols(ref):
        return jnp.concatenate([ref[0].reshape(256, HEAD), ref[1].reshape(256, HEAD)], axis=1)

    def weight_blocks(first):
        cols = grad_cols(d2 if first else d2o)

        def body(i, carry):
            for wy in (2 * i, 2 * i + 1):
                rows = (xt[pl.ds(wy * 8, 8), core] if first else xo[pl.ds(wy * 8, 8)]).reshape(512, 256)
                part = dot_nn(rows, cols)
                for wz in range(2):
                    for wx in range(4):
                        for h, (wq, wp) in enumerate(((wy, wx), (wx, wy))):
                            base = (wz * 4 + wx) * 64
                            block = part[base : base + 64, h * HEAD : (h + 1) * HEAD]
                            if first:
                                wown[h, wq, wp, wz] = block
                            else:
                                wown[h, wq, wp, wz] = wown[h, wq, wp, wz] + block
            return carry

        lax.fori_loop(0, 2, body, 0)

    weight_blocks(True)
    arrived("xt", xo)
    arrived("d2", d2o)
    weight_blocks(False)
    wz_ref = b["wz"]

    def deliver(h, n, value):
        kind, ref, hop = (
            (3, b["w_far2"].at[h], p_far[h]),
            (1, b["w_near2"].at[h, 0], p_to[h][0]),
            (2, b["w_near2"].at[h, 1], p_to[h][1]),
            (0, b["wmine"].at[h], {}),
        )[n]
        ref[...] = value
        for r, (dev, other) in enumerate(across):
            send(("ws", kind, h, r), ref.at[other], wz_ref.at[kind, h, zh], {**hop, **dev})

    w_far, w_near, w_note, w_unit = reducer("w", lambda h, q, p: wown[h, q, p], deliver)
    w_far()

    for c in own_m:
        c.wait()
    for t in range(2):
        for r in range(2):
            arrived(("m", t, r), matrix_part(t, r, core))
            src = matrix_part(t, r, core)
            send(("mc", t, r), src, src, d_core)
    w_near(0)
    w_near(1)
    w_note()
    for t in range(2):
        for r, (dev, other) in enumerate(across):
            arrived(("dz", t, r), dd.at[0, t, other])
            arrived(("mc", t, r), matrix_part(t, r, oc))
        arrived(("dy", t), dd.at[1, t, oh])

    def tokens(which, t):
        return jnp.concatenate(
            [dd[which, t, a].reshape(128, HEAD) for a in range(2)], axis=1
        )

    token_grads = jnp.concatenate([tokens(w, t) for w in range(2) for t in range(2)], axis=1)

    def input_block(i, carry):
        rows = pl.ds(pl.multiple_of(i * 512, 512), 512)
        cols = jnp.concatenate([mat[w, t, rows, :] for w in range(2) for t in range(2)], axis=1)
        igv[:, lanes(i * 512, 512)] = dot_tt(token_grads, cols).astype(BF16)
        return carry

    igv = b["igv"]
    lax.fori_loop(0, 4, input_block, 0)
    ig_copy = local("ig out", igv, ig_out)
    ig_copy.start()
    for r, (dev, other) in enumerate(across):
        arrived(("dqz", r), dqz.at[other])
    outs = [local("dq out", dqz, dq_out)]
    outs[0].start()
    for n in range(4):
        w_unit(n)
    for kind in (3, 1, 2, 0):
        for h in range(2):
            for r, (dev, other) in enumerate(across):
                arrived(("ws", kind, h, r), wz_ref.at[kind, h, other])
    total_w = wz_ref[0].astype(F32)
    for kind in range(1, 4):
        total_w = total_w + wz_ref[kind].astype(F32)
    b["wv"][...] = total_w
    outs.append(local("w out", b["wv"], w_out))
    outs[-1].start()
    outs.append(ig_copy)
    for c in outs:
        c.wait()

    for copy in pending:
        remote(*copy).wait_send()
    assert len(names) <= NSEM and len(local_names) <= NLOCAL


def finish(dq_in, ig_in, w_in, dq_out, ig_out, kw_out, vw_out):
    for c in range(CHUNKS):
        for kvh in range(2):
            for g in range(GROUP):
                at = (kvh * GROUP + g) * HEAD
                dq_out[c * 16 : (c + 1) * 16, at : at + HEAD] = dq_in[kvh, c, g]
    ig_out[...] = ig_in[...]
    for t, out in enumerate((kw_out, vw_out)):
        for n in range(2):
            out[:, n * HEAD : (n + 1) * HEAD] = w_in[t, n]


def local_step(q, k, v, g, x, mk, mv, placement):
    anywhere = pl.BlockSpec(memory_space=pl.ANY)
    vmem = pl.BlockSpec(memory_space=pltpu.VMEM)
    dq, ig, w = pl.pallas_call(
        kernel,
        out_shape=(
            jax.ShapeDtypeStruct((2, CHUNKS, GROUP, 16, HEAD), BF16),
            jax.ShapeDtypeStruct((128, FEATS // 2), BF16),
            jax.ShapeDtypeStruct((2, 2, 64, HEAD), F32),
        ),
        in_specs=[anywhere] * 7 + [vmem],
        out_specs=(anywhere,) * 3,
        scratch_shapes=[pltpu.VMEM(shape, dtype) for shape, dtype in BUFFERS.values()]
        + [
            pltpu.SemaphoreType.DMA((NSEM,)),
            pltpu.SemaphoreType.DMA((NSEM,)),
            pltpu.SemaphoreType.DMA((NLOCAL,)),
        ],
        compiler_params=pltpu.CompilerParams(
            collective_id=0, has_side_effects=True, vmem_limit_bytes=67043328
        ),
    )(
        q.reshape(CHUNKS, 16, -1),
        g.reshape(CHUNKS, 16, -1),
        k.reshape(CHUNKS, 16, -1),
        v.reshape(CHUNKS, 16, -1),
        x.reshape(CHUNKS, 16, -1),
        mk,
        mv,
        placement,
    )
    return pl.pallas_call(
        finish,
        out_shape=(
            jax.ShapeDtypeStruct((128, 2 * GROUP * HEAD), BF16),
            jax.ShapeDtypeStruct((128, FEATS // 2), BF16),
            jax.ShapeDtypeStruct((64, 2 * HEAD), F32),
            jax.ShapeDtypeStruct((64, 2 * HEAD), F32),
        ),
        in_specs=[vmem] * 3,
        out_specs=(vmem,) * 4,
    )(dq, ig, w)


def solution(mesh):
    torus = Mesh(
        mesh.devices.reshape(4, 2, 4, 2, mesh.shape["tp"]), ("seq_0", "seq_1", "seq_2", "seq_3", "tp")
    )
    rows = P(SEQ, "tp")
    return jax.shard_map(
        local_step,
        mesh=torus,
        in_specs=(rows, rows, rows, rows, rows, P(None, "tp"), P(None, "tp"), P()),
        out_specs=(rows, rows, rows, rows),
        check_vma=False,
    )
```

```python
import math

import jax
import jax.numpy as jnp
from jax import lax
from jax.experimental import pallas as pl
from jax.experimental.pallas import tpu as pltpu
from jax.sharding import Mesh
from jax.sharding import PartitionSpec as P

F32 = jnp.float32
BF16 = jnp.bfloat16
Y, ZH, X, CORE, ZL = "seq_0", "seq_1", "seq_2", "seq_3", "tp"
SEQ = (Y, ZH, X, CORE)
MESH = pl.DeviceIdType.MESH

HEAD = 128
GROUP = 4
WINDOW = 4096
CHUNKS = 8
BAND = 4
FEATS = 4096
SCALE = 1.0 / math.sqrt(HEAD)
SCALE2 = SCALE * math.log2(math.e)
MASKED = -1e30
QROWS = 256
KROWS = 128
NSEM = 69
NSEND = 5
NLOCAL = 8


def key_chunks(cq):
    return list(range(max(0, cq - BAND), cq + 1))


TILE_AT = [KROWS * sum(len(key_chunks(c)) for c in range(cq)) for cq in range(CHUNKS)]
TILE_ROWS = KROWS * sum(len(key_chunks(c)) for c in range(CHUNKS))

UNIT_KV = (2, 4, 2, 16, HEAD)
UNIT_W = (2, 64, HEAD)


def reduce_buffers(name, unit):
    half = unit[1:]
    return {
        name + "_far": ((2, 4) + unit, BF16),
        name + "_rfar": ((2, 2, 4) + half, BF16),
        name + "_near": ((2, 2, 4) + unit, BF16),
        name + "_rnear": ((2, 2, 4) + unit, BF16),
        name + "_far2": ((2,) + unit, BF16),
        name + "_rfar2": ((2,) + unit, BF16),
        name + "_near2": ((2, 2) + unit, BF16),
        name + "_rnear2": ((2, 2) + unit, BF16),
    }


BUFFERS = {
    "kv": ((2, 4, 4) + UNIT_KV, BF16),
    "qg": ((2, CHUNKS, 4, GROUP, 16, HEAD), BF16),
    "kpb": ((32, KROWS, 128), F32),
    "e": ((4, TILE_ROWS, QROWS), F32),
    "dp": ((4, TILE_ROWS, QROWS), F32),
    "st": ((3, 4, BAND + 1, CHUNKS, QROWS), F32),
    "ss": ((3, CHUNKS, QROWS), F32),
    "sr": ((3, CHUNKS, QROWS), F32),
    "fac": ((4, BAND + 1, CHUNKS, QROWS), F32),
    "delta": ((CHUNKS, QROWS), F32),
    "acc": ((2, 4) + UNIT_KV, F32),
    "dqt": ((CHUNKS, HEAD, QROWS), F32),
    "dqf": ((CHUNKS, 2, 2, GROUP, 16, HEAD), F32),
    "dqr": ((CHUNKS, 2, GROUP, 16, HEAD), F32),
    "dqs": ((2, CHUNKS, GROUP, 16, HEAD), BF16),
    "dqz": ((2, CHUNKS, GROUP, 16, HEAD), BF16),
    "kt": ((CHUNKS, HEAD, KROWS), BF16),
    "qp": ((CHUNKS, QROWS), F32),
    "xg": ((CHUNKS, 2, 16, FEATS), BF16),
    "xt": ((32, 2, 64, 256), BF16),
    "xo": ((32, 64, 256), BF16),
    "kst": ((2, CHUNKS, 16, 2 * HEAD), BF16),
    "mat": ((2, 2, FEATS // 2, 2 * HEAD), BF16),
    "d2": ((2, CHUNKS, 2, 16, HEAD), BF16),
    "d2o": ((2, CHUNKS, 2, 16, HEAD), BF16),
    "dd": ((2, 2, 2, CHUNKS, 16, HEAD), BF16),
    "wown": ((2, 4, 4) + UNIT_W, F32),
    "wmine": ((2,) + UNIT_W, BF16),
    "wz": ((4, 2, 2, 64, HEAD), BF16),
    "wv": ((2, 2, 64, HEAD), F32),
    "igv": ((128, FEATS // 2), BF16),
    **reduce_buffers("a", UNIT_KV),
    **reduce_buffers("w", UNIT_W),
}


def dot_tt(a, b):
    return lax.dot_general(a, b, (((1,), (1,)), ((), ())), preferred_element_type=F32)


def dot_nn(a, b):
    return lax.dot_general(a, b, (((1,), (0,)), ((), ())), preferred_element_type=F32)


def dot_tn(a, b):
    return lax.dot_general(a, b, (((0,), (0,)), ((), ())), preferred_element_type=F32)


def stack_rows(parts):
    return parts[0] if len(parts) == 1 else jnp.concatenate(parts, axis=0)


def positions(rp_in, kpb, qp, y, x, core):
    slots = rp_in[...].astype(F32).astype(BF16)

    def iota(shape, dim):
        return lax.broadcasted_iota(jnp.int32, shape, dim)

    def bits(a, at, width):
        return jnp.bitwise_and(jnp.right_shift(a, at), (1 << width) - 1)

    row, dev = iota((KROWS, 64), 0), iota((KROWS, 64), 1)
    p, zh, jj = bits(row, 5, 2), bits(row, 4, 1), bits(row, 1, 3)
    wide = iota((KROWS, 128), 0)
    inside = (bits(wide, 1, 3) * 128 + bits(wide, 0, 1)).astype(F32)
    ones = jnp.ones((64, 128), BF16)
    owner = [
        [((q * 2 + zh) * 4 + p) * 2 + core == dev for q in range(4)],
        [((p * 2 + zh) * 4 + q) * 2 + core == dev for q in range(4)],
    ]
    for c in range(CHUNKS):
        block = (dev == jj + 8 * c).astype(F32).astype(BF16)
        rows = dot_nn(block, slots)
        for q in range(4):
            picked = jnp.where(owner[c // 4][q], rows, 0.0).astype(BF16)
            kpb[c // 4 * 16 + q * 4 + c % 4] = (
                dot_nn(picked, ones) * 2.0 + (inside + float(c * 1024))
            )

    dev, lane = iota((64, QROWS), 0), iota((64, QROWS), 1)
    zh, co, jj = bits(lane, 7, 1), bits(lane, 6, 1), bits(lane, 1, 3)
    pick = (((y * 2 + zh) * 4 + x) * 2 + co == dev).astype(F32).astype(BF16)
    slot = dot_nn(slots, pick)
    here = bits(dev, 0, 3) == jj
    pos = jnp.where(here, slot * 2.0 + (dev * 128 + bits(lane, 0, 1)).astype(F32), 0.0)
    qp[...] = jnp.sum(pos.reshape(CHUNKS, 8, QROWS), axis=1)


def kernel(
    q_in, g_in, k_in, v_in, x_in, mk_in, mv_in, rp_in, dq_out, ig_out, w_out, *scratch
):
    ssem, rsem, lsem = scratch[-3:]
    b = dict(zip(BUFFERS, scratch[:-3]))
    y, zh, x, core, zl = (lax.axis_index(a) for a in (Y, ZH, X, CORE, ZL))

    def turn(i, by):
        return lax.rem(i + by, 4)

    z = 2 * zh + zl
    zp, zm = turn(z, 1), turn(z, 3)
    zp_h, zp_l = lax.div(zp, 2), lax.rem(zp, 2)
    zm_h, zm_l = lax.div(zm, 2), lax.rem(zm, 2)
    oh, oc, ol = 1 - zh, 1 - core, 1 - zl
    d_core, d_tp = {CORE: oc}, {ZL: ol}
    across = ((d_tp, zh), ({ZH: oh, ZL: ol}, oh))
    d_zp, d_zm = {ZH: zp_h, ZL: zp_l}, {ZH: zm_h, ZL: zm_l}
    step_of = {a: ({a: turn(i, 1)}, {a: turn(i, 3)}) for a, i in ((X, x), (Y, y))}
    far_of = {X: {X: turn(x, 2)}, Y: {Y: turn(y, 2)}}
    d_zh = {ZH: oh}
    qi, pi = (y, x), (x, y)
    q_to = (step_of[Y], step_of[X])
    p_to = (step_of[X], step_of[Y])
    p_far = (far_of[X], far_of[Y])

    names = {}
    sent = {}
    filled = [0] * NSEND

    def remote(name, src, dst, dev, group=0):
        i = names.setdefault(name, len(names))
        return pltpu.make_async_remote_copy(
            src_ref=src,
            dst_ref=dst,
            send_sem=ssem.at[group],
            recv_sem=rsem.at[i],
            device_id=dev,
            device_id_type=MESH,
        )

    def send(name, part, src, dst, dev):
        kib = math.prod(src.shape) * src.dtype.itemsize // 1024
        if (name, part) not in sent:
            group = min(range(NSEND), key=lambda n: filled[n])
            filled[group] += kib
            sent[name, part] = group
        remote(name, src, dst, dev, sent[name, part]).start()

    def arrived(name, size_of):
        remote(name, size_of, size_of, d_core).wait_recv()

    local_names = {}

    def local(name, src, dst):
        i = local_names.setdefault(name, len(local_names))
        return pltpu.make_async_copy(src, dst, lsem.at[i])

    def lanes(start, width=128):
        return pl.ds(pl.multiple_of(start, 128), width)

    kv, qg, xg, mat = b["kv"], b["qg"], b["xg"], b["mat"]
    own_x = local("x", x_in, xg.at[:, zh, :, lanes(zl * (FEATS // 2), FEATS // 2)])
    half_feats = FEATS // 2
    quarter_feats = FEATS // 4
    own_m = [
        local(("m", t), ref.at[pl.ds(pl.multiple_of(zl * half_feats, half_feats), half_feats), :], mat.at[0, t])
        for t, ref in enumerate((mk_in, mv_in))
    ]
    kst = b["kst"]
    stage = [local(("kst", t), ref, kst.at[t]) for t, ref in enumerate((k_in, v_in))]
    for c in stage:
        c.start()

    barrier = pltpu.get_barrier_semaphore()
    peers = [d_core, *step_of[X], *step_of[Y], *far_of.values(), d_zp, d_zm, d_zh]
    for dev in peers:
        pl.semaphore_signal(barrier, inc=1, device_id=dev, device_id_type=MESH)
    pl.semaphore_wait(barrier, len(peers))

    for c in stage:
        c.wait()

    for h in range(2):
        for r, (dev, head) in enumerate(across):
            for t in range(2):
                send(
                    ("zkv", h),
                    (t, r),
                    kst.at[t, pl.ds(4 * h, 4), :, lanes(head * HEAD)],
                    kv.at[h, qi[h], pi[h], t, :, zh],
                    dev,
                )
    for t, ref in enumerate((q_in, g_in)):
        for r, (dev, head) in enumerate(across):
            for g in range(GROUP):
                send(
                    ("qz", t, r),
                    g,
                    ref.at[:, :, lanes(head * GROUP * HEAD + g * HEAD)],
                    qg.at[t, :, 2 * zh + core, g],
                    dev,
                )

    unit_offs = (0, 3, 1, 2)

    def unit_piece(h, n, side):
        unit = kv.at[h, qi[h], turn(pi[h], unit_offs[n])]
        return ("q", h, n), side, unit, unit, q_to[h][side]

    def send_unit(h, n):
        for side in range(2):
            send(*unit_piece(h, n, side))

    def near_piece(h, n, side):
        return kv.at[h, turn(qi[h], 3 if side == 0 else 1), turn(pi[h], unit_offs[n])]

    def forward_piece(h, n, side):
        src = near_piece(h, n, side).at[side]
        return ("qf", h, side), n, src, src, q_to[h][side]

    def forward_unit(h, n):
        arrived(("q", h, n), kv.at[h, 0, pl.ds(0, 2)])
        for side in range(2):
            send(*forward_piece(h, n, side))

    for h in range(2):
        arrived(("zkv", h), kv.at[h, qi[h], pi[h]])
        unit = kv.at[h, qi[h], pi[h]]
        for side in range(2):
            send(("p", h, side), 0, unit, unit, p_to[h][side])
        send(("pf", h), 0, unit, unit, p_far[h])
        send_unit(h, 0)
    own_x.start()
    for c in own_m:
        c.start()
    dqt = b["dqt"]
    dqt[...] = jnp.zeros(dqt.shape, F32)
    b["st"][0] = jnp.full(b["st"].shape[1:], MASKED, F32)
    b["st"][1:] = jnp.zeros((2,) + b["st"].shape[1:], F32)
    positions(rp_in, b["kpb"], b["qp"], y, x, core)
    for h in range(2):
        for side in range(2):
            src = kv.at[h, qi[h], turn(pi[h], 3 if side == 0 else 1)]
            arrived(("p", h, side), src)
        for side in range(2):
            send_unit(h, 1 + side)
    for h in range(2):
        forward_unit(h, 0)
    for t in range(2):
        for r, (dev, head) in enumerate(across):
            src = qg.at[t, :, 2 * head + core]
            arrived(("qz", t, r), src)
            send(("qc", t), r, src, src, d_core)

    def send_matrix(t):
        ref = (mk_in, mv_in)[t]
        for r, (dev, _) in enumerate(across):
            at = (2 * r + core) * 512
            src = ref.at[pl.ds(pl.multiple_of(ol * half_feats + at, 512), 512), :]
            dst = mat.at[1, t, pl.ds(pl.multiple_of(at, 512), 512), :]
            yield ("m", t, r), 0, src, dst, dev

    def matrix_part(t, r, which):
        return mat.at[1, t, pl.ds(pl.multiple_of((2 * r + which) * 512, 512), 512), :]

    mine = xg.at[:, zh, :, lanes(zl * half_feats, half_feats)]
    send("x+", 0, x_in, mine, d_zp)
    send("x-", 0, x_in, mine, d_zm)
    for copy in send_matrix(0):
        send(*copy)
    for h in range(2):
        arrived(("pf", h), kv.at[h, qi[h], turn(pi[h], 2)])
        send_unit(h, 3)
    for t in range(2):
        arrived(("qc", t), qg.at[t, pl.ds(0, CHUNKS // 2)])

    def queries(t, cq):
        return qg[t, cq].reshape(QROWS, HEAD)

    def keys(t, at, cks):
        return stack_rows(
            [kv[ck // 4, at[ck // 4], :, t, ck % 4].reshape(KROWS, HEAD) for ck in cks]
        )

    st, e_ref, dp_ref = b["st"], b["e"], b["dp"]

    def first_pass(s, carry):
        late = lax.div(s, 2)
        off = (1 - late) * s + late * (5 - s)

        @pl.when(s == 1)
        def _():
            for n in range(1, 4):
                for h in range(2):
                    forward_unit(h, n)

        @pl.when(s == 3)
        def _():
            for h in range(2):
                for side in range(2):
                    arrived(("qf", h, side), kv.at[h, turn(qi[h], 2), :, side])

        at = (turn(y, off), turn(x, off))
        for cq in range(CHUNKS):
            cks = key_chunks(cq)
            scores = dot_tt(keys(0, at, cks), queries(0, cq))
            dprobs = dot_tt(keys(1, at, cks), queries(1, cq))
            qpos = b["qp"][cq : cq + 1, :]
            for n, ck in enumerate(cks):
                part = slice(n * KROWS, (n + 1) * KROWS)
                score, dprob = scores[part] * SCALE2, dprobs[part]
                if ck == cq or ck == cq - BAND:
                    kpb = b["kpb"][ck // 4 * 16 + at[ck // 4] * 4 + ck % 4]
                    kpos = jnp.concatenate([kpb, kpb], axis=1)
                    seen = kpos <= qpos if ck == cq else kpos > qpos - WINDOW
                    score = jnp.where(seen, score, MASKED)
                top = jnp.max(score, axis=0, keepdims=True)
                expo = jnp.exp2(score - top)
                rows = pl.ds(TILE_AT[cq] + n * KROWS, KROWS)
                e_ref[off, rows, :] = expo
                dp_ref[off, rows, :] = dprob
                row = slice(cq, cq + 1)
                st[0, off, cq - ck, row, :] = top
                st[1, off, cq - ck, row, :] = jnp.sum(expo, axis=0, keepdims=True)
                st[2, off, cq - ck, row, :] = jnp.sum(expo * dprob, axis=0, keepdims=True)
        return carry

    lax.fori_loop(0, 4, first_pass, 0)
    ss, sr = b["ss"], b["sr"]
    top_l = jnp.max(st[0], axis=(0, 1))
    fac_l = jnp.exp2(st[0] - top_l[None, None])
    sum_l = jnp.sum(st[1] * fac_l, axis=(0, 1))
    wgt_l = jnp.sum(st[2] * fac_l, axis=(0, 1))
    ss[0] = top_l
    ss[1] = sum_l
    ss[2] = wgt_l
    send("stat", 0, ss, sr, d_core)

    def forward_input():
        for name, src_h, src_l, start, dev in (
            ("x+", zm_h, zm_l, 0, d_zp),
            ("x-", zp_h, zp_l, quarter_feats, d_zm),
        ):
            src = xg.at[:, src_h, :, lanes(src_l * half_feats + start, quarter_feats)]
            arrived(name, xg.at[:, src_h, :, lanes(src_l * half_feats, half_feats)])
            send("far " + name, 0, src, src, dev)

    arrived("stat", sr)
    top = jnp.maximum(top_l, sr[0])
    mine_f = jnp.exp2(top_l - top)
    other_f = jnp.exp2(sr[0] - top)
    total = sum_l * mine_f + sr[1] * other_f
    b["delta"][...] = (wgt_l * mine_f + sr[2] * other_f) / total
    b["fac"][...] = fac_l * (mine_f / total)[None, None]

    offs = (2, 1, 3, 0)

    def reducer(name, unit_at, deliver=None):
        far, rfar = b[name + "_far"], b[name + "_rfar"]
        near, rnear = b[name + "_near"], b[name + "_rnear"]
        far2, rfar2 = b[name + "_far2"], b[name + "_rfar2"]
        near2, rnear2 = b[name + "_near2"], b[name + "_rnear2"]

        def place(h, n):
            return turn(pi[h], offs[n])

        def far_copy(h, n, side):
            p = place(h, n)
            return (
                (name, "far", n, side),
                h,
                far.at[h, p, side],
                rfar.at[h, side, p],
                q_to[h][side],
            )

        def near_copy(h, n, side):
            p = place(h, n)
            return (
                (name, "near", n),
                (h, side),
                near.at[h, side, p],
                rnear.at[h, side, p],
                q_to[h][side],
            )

        def start_far():
            for n in range(4):
                for h in range(2):
                    p = place(h, n)
                    far[h, p] = unit_at(h, turn(qi[h], 2), p).astype(BF16)
                    for side in range(2):
                        send(*far_copy(h, n, side))

        def start_near(side):
            for n in range(4):
                arrived((name, "far", n, side), rfar.at[0, side, pl.ds(0, 2)])
                for h in range(2):
                    p = place(h, n)
                    value = unit_at(h, turn(qi[h], 1 if side == 0 else 3), p)
                    near[h, side, p, 1 - side] = value[1 - side].astype(BF16)
                    near[h, side, p, side] = (value[side] + rfar[h, side, p].astype(F32)).astype(
                        BF16
                    )
                    send(*near_copy(h, n, side))

        def own_unit(n):
            out = []
            arrived((name, "near", n), rnear.at[0, 0])
            for h in range(2):
                p = place(h, n)
                value = (
                    unit_at(h, qi[h], p)
                    + rnear[h, 0, p].astype(F32)
                    + rnear[h, 1, p].astype(F32)
                )
                if deliver:
                    deliver(h, n, value.astype(BF16))
                elif n == 0:
                    far2[h] = value.astype(BF16)
                    send((name, "p", h), 2, far2.at[h], rfar2.at[h], p_far[h])
                elif n < 3:
                    side = n - 1
                    near2[h, side] = value.astype(BF16)
                    send(
                        (name, "p", h),
                        side,
                        near2.at[h, side],
                        rnear2.at[h, side],
                        p_to[h][side],
                    )
                else:
                    arrived((name, "p", h), rnear.at[0, 0, pl.ds(0, 3)])
                    out.append(
                        (value + rfar2[h].astype(F32))
                        + (rnear2[h, 0].astype(F32) + rnear2[h, 1].astype(F32))
                    )
            return out

        return start_far, start_near, own_unit

    acc = b["acc"]
    start_far, start_near, own_unit = reducer("a", lambda h, q, p: acc[h, p])

    fac, delta, kt = b["fac"], b["delta"], b["kt"]

    def second_pass(s, carry):
        late = lax.div(s, 2)
        off = (1 - late) * (2 + s) + late * (3 - s)
        at = (turn(y, off), turn(x, off))
        for ck in range(CHUNKS):
            kt[ck] = keys(0, at, [ck]).T
        for cq in range(CHUNKS):
            cks = key_chunks(cq)
            probs, dscores = [], []
            for n, ck in enumerate(cks):
                rows = pl.ds(TILE_AT[cq] + n * KROWS, KROWS)
                prob = e_ref[off, rows, :] * fac[off, cq - ck, cq : cq + 1, :]
                diff = dp_ref[off, rows, :] - delta[cq : cq + 1, :]
                probs.append(prob.astype(BF16))
                dscores.append((prob * diff).astype(BF16))
            prob, dscore = stack_rows(probs), stack_rows(dscores)
            grads = (dot_nn(dscore, queries(0, cq)), dot_nn(prob, queries(1, cq)))
            for t in range(2):
                for n, ck in enumerate(cks):
                    part = grads[t][n * KROWS : (n + 1) * KROWS].reshape(4, 2, 16, HEAD)
                    if ck == cq:
                        acc[ck // 4, :, t, ck % 4] = part
                    else:
                        acc[ck // 4, :, t, ck % 4] = acc[ck // 4, :, t, ck % 4] + part
            flipped = jnp.concatenate([kt[ck] for ck in cks], axis=1)
            dqt[cq] = dqt[cq] + dot_nn(flipped, dscore)

        @pl.when(s == 0)
        def _():
            start_far()
            forward_input()
            for copy in send_matrix(1):
                send(*copy)

        @pl.when(s == 1)
        def _():
            start_near(1)

        @pl.when(s == 2)
        def _():
            start_near(0)

        return carry

    lax.fori_loop(0, 4, second_pass, 0)
    dqf, dqr, dqs, dqz = b["dqf"], b["dqr"], b["dqs"], b["dqz"]
    for cq in range(CHUNKS):
        dqf[cq] = (dqt[cq].T * SCALE).reshape(2, 2, GROUP, 16, HEAD)
    send("dqc", 0, dqf.at[:, :, oc], dqr, d_core)
    own_unit(0)
    own_x.wait()
    far_h = 1 - zh
    arrived("far x+", xg.at[:, far_h, :, lanes(zl * half_feats, quarter_feats)])
    arrived("far x-", xg.at[:, far_h, :, lanes(zl * half_feats + quarter_feats, quarter_feats)])
    xt, xo = b["xt"], b["xo"]

    def flip_input(i, carry):
        for n in range(4):
            at = i * 4 + n
            block = xg[:, :, :, lanes(at * 128)].reshape(256, 128)
            xt[at] = block.T.reshape(2, 64, 256)
        return carry

    lax.fori_loop(0, 8, flip_input, 0)
    send("xt", 0, xt.at[:, oc], xo, d_core)
    own_unit(1)
    own_unit(2)
    arrived("dqc", dqr)
    for n in range(2):
        dqs[n] = (dqf[:, n, core] + dqr[:, n]).astype(BF16)
    for r, (dev, other) in enumerate(across):
        send("dqz", r, dqs.at[other], dqz.at[zh], dev)
    d2, d2o, dd = b["d2"], b["d2o"], b["dd"]
    for h, value in enumerate(own_unit(3)):
        d2[0, 4 * h : 4 * h + 4] = (value[0] * SCALE).astype(BF16)
        d2[1, 4 * h : 4 * h + 4] = value[1].astype(BF16)
    send("d2", 0, d2, d2o, d_core)
    for r, (dev, other) in enumerate(across):
        for t in range(2):
            send("dz", (t, r), d2.at[t, :, other], dd.at[0, t, zh], dev)
    for t in range(2):
        send("dy", t, d2.at[t, :, oh], dd.at[1, t, zh], d_zh)
        dd[1, t, zh] = d2[t, :, zh]

    wown = b["wown"]

    def grad_cols(ref):
        return jnp.concatenate([ref[0].reshape(256, HEAD), ref[1].reshape(256, HEAD)], axis=1)

    def weight_blocks(first):
        cols = grad_cols(d2 if first else d2o)

        def body(i, carry):
            for wy in (2 * i, 2 * i + 1):
                rows = (xt[pl.ds(wy * 8, 8), core] if first else xo[pl.ds(wy * 8, 8)]).reshape(512, 256)
                part = dot_nn(rows, cols)
                for wz in range(2):
                    for wx in range(4):
                        for h, (wq, wp) in enumerate(((wy, wx), (wx, wy))):
                            base = (wz * 4 + wx) * 64
                            block = part[base : base + 64, h * HEAD : (h + 1) * HEAD]
                            if first:
                                wown[h, wq, wp, wz] = block
                            else:
                                wown[h, wq, wp, wz] = wown[h, wq, wp, wz] + block
            return carry

        lax.fori_loop(0, 2, body, 0)

    weight_blocks(True)
    arrived("xt", xo)
    arrived("d2", d2o)
    weight_blocks(False)
    wz_ref = b["wz"]

    def deliver(h, n, value):
        kind, ref, hop = (
            (3, b["w_far2"].at[h], p_far[h]),
            (1, b["w_near2"].at[h, 0], p_to[h][0]),
            (2, b["w_near2"].at[h, 1], p_to[h][1]),
            (0, b["wmine"].at[h], {}),
        )[n]
        ref[...] = value
        for r, (dev, other) in enumerate(across):
            send("ws", (kind, h, r), ref.at[other], wz_ref.at[kind, h, zh], {**hop, **dev})

    w_far, w_near, w_unit = reducer("w", lambda h, q, p: wown[h, q, p], deliver)
    w_far()

    for c in own_m:
        c.wait()
    for t in range(2):
        for r in range(2):
            arrived(("m", t, r), matrix_part(t, r, core))
            src = matrix_part(t, r, core)
            send("mc", (t, r), src, src, d_core)
    w_near(0)
    w_near(1)
    arrived("dz", dd.at[0])
    arrived("dy", dd.at[1, :, oh])
    arrived("mc", mat.at[1, 0])

    def tokens(which, t):
        return jnp.concatenate(
            [dd[which, t, a].reshape(128, HEAD) for a in range(2)], axis=1
        )

    token_grads = jnp.concatenate([tokens(w, t) for w in range(2) for t in range(2)], axis=1)

    def input_block(i, carry):
        rows = pl.ds(pl.multiple_of(i * 512, 512), 512)
        cols = jnp.concatenate([mat[w, t, rows, :] for w in range(2) for t in range(2)], axis=1)
        igv[:, lanes(i * 512, 512)] = dot_tt(token_grads, cols).astype(BF16)
        return carry

    igv = b["igv"]
    lax.fori_loop(0, 4, input_block, 0)
    ig_copy = local("ig out", igv, ig_out)
    ig_copy.start()
    arrived("dqz", dqz)
    outs = [local("dq out", dqz, dq_out)]
    outs[0].start()
    for n in range(4):
        w_unit(n)
    arrived("ws", wz_ref)
    total_w = wz_ref[0].astype(F32)
    for kind in range(1, 4):
        total_w = total_w + wz_ref[kind].astype(F32)
    b["wv"][...] = total_w
    outs.append(local("w out", b["wv"], w_out))
    outs[-1].start()
    outs.append(ig_copy)
    for c in outs:
        c.wait()

    for group, kib in enumerate(filled):
        size_of = e_ref.at[0, pl.ds(0, kib), :]
        pltpu.make_async_copy(size_of, size_of, ssem.at[group]).wait()
    assert len(names) <= NSEM and len(local_names) <= NLOCAL


def finish(dq_in, ig_in, w_in, dq_out, ig_out, kw_out, vw_out):
    for c in range(CHUNKS):
        for kvh in range(2):
            for g in range(GROUP):
                at = (kvh * GROUP + g) * HEAD
                dq_out[c * 16 : (c + 1) * 16, at : at + HEAD] = dq_in[kvh, c, g]
    ig_out[...] = ig_in[...]
    for t, out in enumerate((kw_out, vw_out)):
        for n in range(2):
            out[:, n * HEAD : (n + 1) * HEAD] = w_in[t, n]


def local_step(q, k, v, g, x, mk, mv, placement):
    anywhere = pl.BlockSpec(memory_space=pl.ANY)
    vmem = pl.BlockSpec(memory_space=pltpu.VMEM)
    dq, ig, w = pl.pallas_call(
        kernel,
        out_shape=(
            jax.ShapeDtypeStruct((2, CHUNKS, GROUP, 16, HEAD), BF16),
            jax.ShapeDtypeStruct((128, FEATS // 2), BF16),
            jax.ShapeDtypeStruct((2, 2, 64, HEAD), F32),
        ),
        in_specs=[anywhere] * 7 + [vmem],
        out_specs=(anywhere,) * 3,
        scratch_shapes=[pltpu.VMEM(shape, dtype) for shape, dtype in BUFFERS.values()]
        + [
            pltpu.SemaphoreType.DMA((NSEND,)),
            pltpu.SemaphoreType.DMA((NSEM,)),
            pltpu.SemaphoreType.DMA((NLOCAL,)),
        ],
        compiler_params=pltpu.CompilerParams(
            collective_id=0, has_side_effects=True, vmem_limit_bytes=67043328
        ),
    )(
        q.reshape(CHUNKS, 16, -1),
        g.reshape(CHUNKS, 16, -1),
        k.reshape(CHUNKS, 16, -1),
        v.reshape(CHUNKS, 16, -1),
        x.reshape(CHUNKS, 16, -1),
        mk,
        mv,
        placement,
    )
    return pl.pallas_call(
        finish,
        out_shape=(
            jax.ShapeDtypeStruct((128, 2 * GROUP * HEAD), BF16),
            jax.ShapeDtypeStruct((128, FEATS // 2), BF16),
            jax.ShapeDtypeStruct((64, 2 * HEAD), F32),
            jax.ShapeDtypeStruct((64, 2 * HEAD), F32),
        ),
        in_specs=[vmem] * 3,
        out_specs=(vmem,) * 4,
    )(dq, ig, w)


def solution(mesh):
    torus = Mesh(
        mesh.devices.reshape(4, 2, 4, 2, mesh.shape["tp"]), ("seq_0", "seq_1", "seq_2", "seq_3", "tp")
    )
    rows = P(SEQ, "tp")
    return jax.shard_map(
        local_step,
        mesh=torus,
        in_specs=(rows, rows, rows, rows, rows, P(None, "tp"), P(None, "tp"), P()),
        out_specs=(rows, rows, rows, rows),
        check_vma=False,
    )
```

```python
import math

import jax
import jax.numpy as jnp
from jax import lax
from jax.experimental import pallas as pl
from jax.experimental.pallas import tpu as pltpu
from jax.sharding import Mesh
from jax.sharding import PartitionSpec as P

F32 = jnp.float32
BF16 = jnp.bfloat16
Y, ZH, X, CORE, ZL = "seq_0", "seq_1", "seq_2", "seq_3", "tp"
SEQ = (Y, ZH, X, CORE)
MESH = pl.DeviceIdType.MESH

HEAD = 128
GROUP = 4
WINDOW = 4096
CHUNKS = 8
BAND = 4
FEATS = 4096
SCALE = 1.0 / math.sqrt(HEAD)
SCALE2 = SCALE * math.log2(math.e)
MASKED = -1e30
QROWS = 256
KROWS = 128
NSEM = 71
NSEND = 5
NLOCAL = 8


def key_chunks(cq):
    return list(range(max(0, cq - BAND), cq + 1))


TILE_AT = [KROWS * sum(len(key_chunks(c)) for c in range(cq)) for cq in range(CHUNKS)]
TILE_ROWS = KROWS * sum(len(key_chunks(c)) for c in range(CHUNKS))

UNIT_KV = (2, 4, 2, 16, HEAD)
UNIT_W = (2, 64, HEAD)


def reduce_buffers(name, unit):
    half = unit[1:]
    return {
        name + "_far": ((2, 4) + unit, BF16),
        name + "_rfar": ((2, 2, 4) + half, BF16),
        name + "_near": ((2, 2, 4) + unit, BF16),
        name + "_rnear": ((2, 2, 4) + unit, BF16),
        name + "_far2": ((2,) + unit, BF16),
        name + "_rfar2": ((2,) + unit, BF16),
        name + "_near2": ((2, 2) + unit, BF16),
        name + "_rnear2": ((2, 2) + unit, BF16),
    }


BUFFERS = {
    "kv": ((2, 4, 4) + UNIT_KV, BF16),
    "qg": ((2, CHUNKS, 4, GROUP, 16, HEAD), BF16),
    "kpb": ((32, KROWS, 128), F32),
    "e": ((4, TILE_ROWS, QROWS), F32),
    "dp": ((4, TILE_ROWS, QROWS), F32),
    "st": ((3, 4, BAND + 1, CHUNKS, QROWS), F32),
    "ss": ((3, CHUNKS, QROWS), F32),
    "sr": ((3, CHUNKS, QROWS), F32),
    "fac": ((4, BAND + 1, CHUNKS, QROWS), F32),
    "delta": ((CHUNKS, QROWS), F32),
    "acc": ((2, 2, 4) + UNIT_KV, F32),
    "dqf": ((CHUNKS, 2, 2, GROUP, 16, HEAD), F32),
    "dqr": ((CHUNKS, 2, GROUP, 16, HEAD), F32),
    "dqs": ((2, CHUNKS, GROUP, 16, HEAD), BF16),
    "dqz": ((2, CHUNKS, GROUP, 16, HEAD), BF16),
    "kt": ((4, CHUNKS, HEAD, KROWS), BF16),
    "qp": ((CHUNKS, QROWS), F32),
    "xg": ((CHUNKS, 2, 16, FEATS), BF16),
    "xt": ((32, 2, 64, 256), BF16),
    "xo": ((32, 64, 256), BF16),
    "kst": ((2, CHUNKS, 16, 2 * HEAD), BF16),
    "mat": ((2, 2, FEATS // 2, 2 * HEAD), BF16),
    "d2": ((2, CHUNKS, 2, 16, HEAD), BF16),
    "d2o": ((2, CHUNKS, 2, 16, HEAD), BF16),
    "dd": ((2, 2, 2, CHUNKS, 16, HEAD), BF16),
    "wown": ((2, 4, 4) + UNIT_W, F32),
    "wmine": ((2,) + UNIT_W, BF16),
    "igv": ((128, FEATS // 2), BF16),
    **reduce_buffers("a", UNIT_KV),
    **reduce_buffers("w", UNIT_W),
}


def dot_tt(a, b):
    return lax.dot_general(a, b, (((1,), (1,)), ((), ())), preferred_element_type=F32)


def dot_nn(a, b):
    return lax.dot_general(a, b, (((1,), (0,)), ((), ())), preferred_element_type=F32)


def dot_tn(a, b):
    return lax.dot_general(a, b, (((0,), (0,)), ((), ())), preferred_element_type=F32)


def stack_rows(parts):
    return parts[0] if len(parts) == 1 else jnp.concatenate(parts, axis=0)


def positions(rp_in, kpb, qp, y, x, core):
    slots = rp_in[...].astype(F32).astype(BF16)

    def iota(shape, dim):
        return lax.broadcasted_iota(jnp.int32, shape, dim)

    def bits(a, at, width):
        return jnp.bitwise_and(jnp.right_shift(a, at), (1 << width) - 1)

    row, dev = iota((KROWS, 64), 0), iota((KROWS, 64), 1)
    p, zh, jj = bits(row, 5, 2), bits(row, 4, 1), bits(row, 1, 3)
    wide = iota((KROWS, 128), 0)
    inside = (bits(wide, 1, 3) * 128 + bits(wide, 0, 1)).astype(F32)
    ones = jnp.ones((64, 128), BF16)
    owner = [
        [((q * 2 + zh) * 4 + p) * 2 + core == dev for q in range(4)],
        [((p * 2 + zh) * 4 + q) * 2 + core == dev for q in range(4)],
    ]
    for c in range(CHUNKS):
        block = (dev == jj + 8 * c).astype(F32).astype(BF16)
        rows = dot_nn(block, slots)
        for q in range(4):
            picked = jnp.where(owner[c // 4][q], rows, 0.0).astype(BF16)
            kpb[c // 4 * 16 + q * 4 + c % 4] = (
                dot_nn(picked, ones) * 2.0 + (inside + float(c * 1024))
            )

    dev, lane = iota((64, QROWS), 0), iota((64, QROWS), 1)
    zh, co, jj = bits(lane, 7, 1), bits(lane, 6, 1), bits(lane, 1, 3)
    pick = (((y * 2 + zh) * 4 + x) * 2 + co == dev).astype(F32).astype(BF16)
    slot = dot_nn(slots, pick)
    here = bits(dev, 0, 3) == jj
    pos = jnp.where(here, slot * 2.0 + (dev * 128 + bits(lane, 0, 1)).astype(F32), 0.0)
    qp[...] = jnp.sum(pos.reshape(CHUNKS, 8, QROWS), axis=1)


def kernel(
    q_in, g_in, k_in, v_in, x_in, mk_in, mv_in, rp_in, dq_out, ig_out, w_out, *scratch
):
    ssem, rsem, lsem = scratch[-3:]
    b = dict(zip(BUFFERS, scratch[:-3]))
    y, zh, x, core, zl = (lax.axis_index(a) for a in (Y, ZH, X, CORE, ZL))

    def turn(i, by):
        return lax.rem(i + by, 4)

    z = 2 * zh + zl
    zp, zm = turn(z, 1), turn(z, 3)
    zp_h, zp_l = lax.div(zp, 2), lax.rem(zp, 2)
    zm_h, zm_l = lax.div(zm, 2), lax.rem(zm, 2)
    oh, oc, ol = 1 - zh, 1 - core, 1 - zl
    d_core, d_tp = {CORE: oc}, {ZL: ol}
    across = ((d_tp, zh), ({ZH: oh, ZL: ol}, oh))
    d_zp, d_zm = {ZH: zp_h, ZL: zp_l}, {ZH: zm_h, ZL: zm_l}
    step_of = {a: ({a: turn(i, 1)}, {a: turn(i, 3)}) for a, i in ((X, x), (Y, y))}
    far_of = {X: {X: turn(x, 2)}, Y: {Y: turn(y, 2)}}
    d_zh = {ZH: oh}
    qi, pi = (y, x), (x, y)
    q_to = (step_of[Y], step_of[X])
    p_to = (step_of[X], step_of[Y])
    p_far = (far_of[X], far_of[Y])

    names = {}
    sent = {}
    filled = [0] * NSEND

    def remote(name, src, dst, dev, group=0):
        i = names.setdefault(name, len(names))
        return pltpu.make_async_remote_copy(
            src_ref=src,
            dst_ref=dst,
            send_sem=ssem.at[group],
            recv_sem=rsem.at[i],
            device_id=dev,
            device_id_type=MESH,
        )

    def send(name, part, src, dst, dev):
        kib = math.prod(src.shape) * src.dtype.itemsize // 1024
        if (name, part) not in sent:
            group = min(range(NSEND), key=lambda n: filled[n])
            filled[group] += kib
            sent[name, part] = group
        remote(name, src, dst, dev, sent[name, part]).start()

    def arrived(name, size_of):
        remote(name, size_of, size_of, d_core).wait_recv()

    local_names = {}

    def local(name, src, dst):
        i = local_names.setdefault(name, len(local_names))
        return pltpu.make_async_copy(src, dst, lsem.at[i])

    def lanes(start, width=128):
        return pl.ds(pl.multiple_of(start, 128), width)

    kv, qg, xg, mat = b["kv"], b["qg"], b["xg"], b["mat"]
    own_x = local("x", x_in, xg.at[:, zh, :, lanes(zl * (FEATS // 2), FEATS // 2)])
    half_feats = FEATS // 2
    quarter_feats = FEATS // 4
    own_m = [
        local(("m", t), ref.at[pl.ds(pl.multiple_of(zl * half_feats, half_feats), half_feats), :], mat.at[0, t])
        for t, ref in enumerate((mk_in, mv_in))
    ]
    kst = b["kst"]
    stage = [local(("kst", t), ref, kst.at[t]) for t, ref in enumerate((k_in, v_in))]
    for c in stage:
        c.start()

    barrier = pltpu.get_barrier_semaphore()
    peers = [d_core, *step_of[X], *step_of[Y], *far_of.values(), d_zp, d_zm, d_zh]
    for dev in peers:
        pl.semaphore_signal(barrier, inc=1, device_id=dev, device_id_type=MESH)
    pl.semaphore_wait(barrier, len(peers))

    for c in stage:
        c.wait()

    for h in range(2):
        for r, (dev, head) in enumerate(across):
            for t in range(2):
                send(
                    ("zkv", h),
                    (t, r),
                    kst.at[t, pl.ds(4 * h, 4), :, lanes(head * HEAD)],
                    kv.at[h, qi[h], pi[h], t, :, zh],
                    dev,
                )
    for t, ref in enumerate((q_in, g_in)):
        for r, (dev, head) in enumerate(across):
            for g in range(GROUP):
                send(
                    ("qz", t, r),
                    g,
                    ref.at[:, :, lanes(head * GROUP * HEAD + g * HEAD)],
                    qg.at[t, :, 2 * zh + core, g],
                    dev,
                )

    unit_offs = (0, 3, 1, 2)

    def unit_piece(h, n, side):
        unit = kv.at[h, qi[h], turn(pi[h], unit_offs[n])]
        return ("q", h, n), side, unit, unit, q_to[h][side]

    def send_unit(h, n):
        for side in range(2):
            send(*unit_piece(h, n, side))

    def near_piece(h, n, side):
        return kv.at[h, turn(qi[h], 3 if side == 0 else 1), turn(pi[h], unit_offs[n])]

    def forward_piece(h, n, side):
        src = near_piece(h, n, side).at[side]
        return ("qf", h, side), n, src, src, q_to[h][side]

    def forward_unit(h, n):
        arrived(("q", h, n), kv.at[h, 0, pl.ds(0, 2)])
        for side in range(2):
            send(*forward_piece(h, n, side))

    for h in range(2):
        arrived(("zkv", h), kv.at[h, qi[h], pi[h]])
        unit = kv.at[h, qi[h], pi[h]]
        for side in range(2):
            send(("p", h, side), 0, unit, unit, p_to[h][side])
        send(("pf", h), 0, unit, unit, p_far[h])
        send_unit(h, 0)
    own_x.start()
    for c in own_m:
        c.start()
    b["st"][0] = jnp.full(b["st"].shape[1:], MASKED, F32)
    b["st"][1:] = jnp.zeros((2,) + b["st"].shape[1:], F32)
    positions(rp_in, b["kpb"], b["qp"], y, x, core)
    for h in range(2):
        for side in range(2):
            src = kv.at[h, qi[h], turn(pi[h], 3 if side == 0 else 1)]
            arrived(("p", h, side), src)
        for side in range(2):
            send_unit(h, 1 + side)
    for h in range(2):
        forward_unit(h, 0)
    for t in range(2):
        for r, (dev, head) in enumerate(across):
            src = qg.at[t, :, 2 * head + core]
            arrived(("qz", t, r), src)
            send(("qc", t), r, src, src, d_core)

    def send_matrix(t):
        ref = (mk_in, mv_in)[t]
        for r, (dev, _) in enumerate(across):
            at = (2 * r + core) * 512
            src = ref.at[pl.ds(pl.multiple_of(ol * half_feats + at, 512), 512), :]
            dst = mat.at[1, t, pl.ds(pl.multiple_of(at, 512), 512), :]
            yield ("m", t, r), 0, src, dst, dev

    def matrix_part(t, r, which):
        return mat.at[1, t, pl.ds(pl.multiple_of((2 * r + which) * 512, 512), 512), :]

    ring = (
        ("x+", d_zp, zm_h, zm_l, 0),
        ("x-", d_zm, zp_h, zp_l, quarter_feats),
    )
    for second in range(2):
        for name, dev, _, _, first in ring:
            at = quarter_feats - first if second else first
            send(
                (name, second),
                0,
                x_in.at[:, :, pl.ds(at, quarter_feats)],
                xg.at[:, zh, :, lanes(zl * half_feats + at, quarter_feats)],
                dev,
            )

    def ring_part(src_h, src_l, at):
        return xg.at[:, src_h, :, lanes(src_l * half_feats + at, quarter_feats)]

    def forward_input():
        for name, dev, src_h, src_l, first in ring:
            src = ring_part(src_h, src_l, first)
            arrived((name, 0), src)
            send((name, 2), 0, src, src, dev)

    def wait_input():
        own_x.wait()
        for name, _, src_h, src_l, first in ring:
            arrived((name, 1), ring_part(src_h, src_l, quarter_feats - first))
            arrived((name, 2), ring_part(oh, zl, first))

    for h in range(2):
        arrived(("pf", h), kv.at[h, qi[h], turn(pi[h], 2)])
        send_unit(h, 3)
    for t in range(2):
        arrived(("qc", t), qg.at[t, pl.ds(0, CHUNKS // 2)])

    def tile_rows(cq, ck):
        return pl.ds(TILE_AT[cq] + (ck - key_chunks(cq)[0]) * KROWS, KROWS)

    def queries(t, cq):
        return qg[t, cq].reshape(QROWS, HEAD)

    def keys(t, at, cks):
        return stack_rows(
            [kv[ck // 4, at[ck // 4], :, t, ck % 4].reshape(KROWS, HEAD) for ck in cks]
        )

    st, e_ref, dp_ref = b["st"], b["e"], b["dp"]

    def first_pass(s, carry):
        late = lax.div(s, 2)
        off = (1 - late) * s + late * (5 - s)

        @pl.when(s == 1)
        def _():
            for n in range(1, 4):
                for h in range(2):
                    forward_unit(h, n)

        @pl.when(s == 3)
        def _():
            for h in range(2):
                for side in range(2):
                    arrived(("qf", h, side), kv.at[h, turn(qi[h], 2), :, side])
            forward_input()
            for t in range(2):
                for copy in send_matrix(t):
                    send(*copy)

        at = (turn(y, off), turn(x, off))
        for cq in range(CHUNKS):
            cks = key_chunks(cq)
            scores = dot_tt(keys(0, at, cks), queries(0, cq))
            dprobs = dot_tt(keys(1, at, cks), queries(1, cq))
            qpos = b["qp"][cq : cq + 1, :]
            for n, ck in enumerate(cks):
                part = slice(n * KROWS, (n + 1) * KROWS)
                score, dprob = scores[part] * SCALE2, dprobs[part]
                if ck == cq or ck == cq - BAND:
                    kpb = b["kpb"][ck // 4 * 16 + at[ck // 4] * 4 + ck % 4]
                    kpos = jnp.concatenate([kpb, kpb], axis=1)
                    seen = kpos <= qpos if ck == cq else kpos > qpos - WINDOW
                    score = jnp.where(seen, score, MASKED)
                top = jnp.max(score, axis=0, keepdims=True)
                expo = jnp.exp2(score - top)
                rows = tile_rows(cq, ck)
                e_ref[off, rows, :] = expo
                dp_ref[off, rows, :] = dprob
                row = slice(cq, cq + 1)
                st[0, off, cq - ck, row, :] = top
                st[1, off, cq - ck, row, :] = jnp.sum(expo, axis=0, keepdims=True)
                st[2, off, cq - ck, row, :] = jnp.sum(expo * dprob, axis=0, keepdims=True)
        return carry

    lax.fori_loop(0, 4, first_pass, 0)
    ss, sr = b["ss"], b["sr"]
    top_l = jnp.max(st[0], axis=(0, 1))
    fac_l = jnp.exp2(st[0] - top_l[None, None])
    sum_l = jnp.sum(st[1] * fac_l, axis=(0, 1))
    wgt_l = jnp.sum(st[2] * fac_l, axis=(0, 1))
    ss[0] = top_l
    ss[1] = sum_l
    ss[2] = wgt_l
    send("stat", 0, ss, sr, d_core)

    arrived("stat", sr)
    top = jnp.maximum(top_l, sr[0])
    mine_f = jnp.exp2(top_l - top)
    other_f = jnp.exp2(sr[0] - top)
    total = sum_l * mine_f + sr[1] * other_f
    b["delta"][...] = (wgt_l * mine_f + sr[2] * other_f) / total
    b["fac"][...] = fac_l * (mine_f / total)[None, None]

    offs = (2, 1, 3, 0)

    def reducer(name, unit_at, deliver=None):
        far, rfar = b[name + "_far"], b[name + "_rfar"]
        near, rnear = b[name + "_near"], b[name + "_rnear"]
        far2, rfar2 = b[name + "_far2"], b[name + "_rfar2"]
        near2, rnear2 = b[name + "_near2"], b[name + "_rnear2"]

        def place(h, n):
            return turn(pi[h], offs[n])

        def far_copy(h, n, side):
            p = place(h, n)
            return (
                (name, "far", n, side),
                h,
                far.at[h, p, side],
                rfar.at[h, side, p],
                q_to[h][side],
            )

        def near_copy(h, n, side):
            p = place(h, n)
            return (
                (name, "near", n),
                (h, side),
                near.at[h, side, p],
                rnear.at[h, side, p],
                q_to[h][side],
            )

        def start_far():
            for n in range(4):
                for h in range(2):
                    p = place(h, n)
                    far[h, p] = unit_at(h, turn(qi[h], 2), p, 0).astype(BF16)
                    for side in range(2):
                        send(*far_copy(h, n, side))

        def start_near(n):
            for side in (1, 0):
                arrived((name, "far", n, side), rfar.at[0, side, pl.ds(0, 2)])
                for h in range(2):
                    p = place(h, n)
                    value = unit_at(h, turn(qi[h], 1 if side == 0 else 3), p, 1 - side)
                    near[h, side, p, 1 - side] = value[1 - side].astype(BF16)
                    near[h, side, p, side] = (value[side] + rfar[h, side, p].astype(F32)).astype(
                        BF16
                    )
                    send(*near_copy(h, n, side))

        def own_unit(n):
            out = []
            arrived((name, "near", n), rnear.at[0, 0])
            for h in range(2):
                p = place(h, n)
                value = (
                    unit_at(h, qi[h], p, 0)
                    + rnear[h, 0, p].astype(F32)
                    + rnear[h, 1, p].astype(F32)
                )
                if deliver:
                    deliver(h, n, value.astype(BF16))
                elif n == 0:
                    far2[h] = value.astype(BF16)
                    send((name, "p", h), 2, far2.at[h], rfar2.at[h], p_far[h])
                elif n < 3:
                    side = n - 1
                    near2[h, side] = value.astype(BF16)
                    send(
                        (name, "p", h),
                        side,
                        near2.at[h, side],
                        rnear2.at[h, side],
                        p_to[h][side],
                    )
                else:
                    arrived((name, "p", h), rnear.at[0, 0, pl.ds(0, 3)])
                    out.append(
                        (value + rfar2[h].astype(F32))
                        + (rnear2[h, 0].astype(F32) + rnear2[h, 1].astype(F32))
                    )
            return out

        return start_far, start_near, own_unit

    acc = b["acc"]
    start_far, start_near, own_unit = reducer(
        "a", lambda h, q, p, slot: acc[slot, h, p]
    )

    fac, delta, kt = b["fac"], b["delta"], b["kt"]

    def second_pass(s, carry):
        late = lax.div(s, 2)
        off = (1 - late) * (2 + s) + late * (3 - s)
        slot = late * (3 - s)
        for ck in range(CHUNKS):
            probs, dscores = [], []
            cqs = [cq for cq in range(CHUNKS) if ck in key_chunks(cq)]
            for cq in cqs:
                rows = tile_rows(cq, ck)
                prob = e_ref[off, rows, :] * fac[off, cq - ck, cq : cq + 1, :]
                dscore = prob * (dp_ref[off, rows, :] - delta[cq : cq + 1, :])
                e_ref[off, rows, :] = dscore
                probs.append(prob.astype(BF16))
                dscores.append(dscore.astype(BF16))
            for t, parts in enumerate((dscores, probs)):
                depth = qg[t, ck : ck + len(cqs)].reshape(len(cqs) * QROWS, HEAD)
                grad = dot_nn(jnp.concatenate(parts, axis=1), depth)
                acc[slot, ck // 4, :, t, ck % 4] = grad.reshape(4, 2, 16, HEAD)

        @pl.when(s == 0)
        def _():
            start_far()

        @pl.when(s == 2)
        def _():
            for n in range(4):
                start_near(n)

        return carry

    lax.fori_loop(0, 4, second_pass, 0)
    dqf, dqr, dqs, dqz = b["dqf"], b["dqr"], b["dqs"], b["dqz"]
    own_unit(0)
    wait_input()
    xt, xo = b["xt"], b["xo"]

    def flip_input(i, carry):
        for n in range(4):
            at = i * 4 + n
            block = xg[:, :, :, lanes(at * 128)].reshape(256, 128)
            xt[at] = block.T.reshape(2, 64, 256)
        return carry

    lax.fori_loop(0, 8, flip_input, 0)
    send("xt", 0, xt.at[:, oc], xo, d_core)
    own_unit(1)
    own_unit(2)
    for off in range(4):
        at = (turn(y, off), turn(x, off))
        for ck in range(CHUNKS):
            kt[off, ck] = keys(0, at, [ck]).T
    for cq in range(CHUNKS):
        cks = key_chunks(cq)
        rows = pl.ds(TILE_AT[cq], KROWS * len(cks))
        flipped = jnp.concatenate([kt[off, ck] for off in range(4) for ck in cks], axis=1)
        dscore = jnp.concatenate([e_ref[off, rows, :].astype(BF16) for off in range(4)], axis=0)
        dqf[cq] = (dot_nn(flipped, dscore).T * SCALE).reshape(2, 2, GROUP, 16, HEAD)
    send("dqc", 0, dqf.at[:, :, oc], dqr, d_core)
    d2, d2o, dd = b["d2"], b["d2o"], b["dd"]
    for h, value in enumerate(own_unit(3)):
        d2[0, 4 * h : 4 * h + 4] = (value[0] * SCALE).astype(BF16)
        d2[1, 4 * h : 4 * h + 4] = value[1].astype(BF16)
    send("d2", 0, d2, d2o, d_core)
    for r, (dev, other) in enumerate(across):
        for t in range(2):
            send("dz", (t, r), d2.at[t, :, other], dd.at[0, t, zh], dev)
    for t in range(2):
        send("dy", t, d2.at[t, :, oh], dd.at[1, t, zh], d_zh)
        dd[1, t, zh] = d2[t, :, zh]

    wown = b["wown"]

    def grad_cols(ref):
        return jnp.concatenate([ref[0].reshape(256, HEAD), ref[1].reshape(256, HEAD)], axis=1)

    def weight_blocks(first):
        cols = grad_cols(d2 if first else d2o)

        def body(i, carry):
            for wy in (2 * i, 2 * i + 1):
                rows = (xt[pl.ds(wy * 8, 8), core] if first else xo[pl.ds(wy * 8, 8)]).reshape(512, 256)
                part = dot_nn(rows, cols)
                for wz in range(2):
                    for wx in range(4):
                        for h, (wq, wp) in enumerate(((wy, wx), (wx, wy))):
                            base = (wz * 4 + wx) * 64
                            block = part[base : base + 64, h * HEAD : (h + 1) * HEAD]
                            if first:
                                wown[h, wq, wp, wz] = block
                            else:
                                wown[h, wq, wp, wz] = wown[h, wq, wp, wz] + block
            return carry

        lax.fori_loop(0, 2, body, 0)

    weight_blocks(True)
    arrived("dqc", dqr)
    for n in range(2):
        dqs[n] = (dqf[:, n, core] + dqr[:, n]).astype(BF16)
    for r, (dev, other) in enumerate(across):
        send("dqz", r, dqs.at[other], dqz.at[zh], dev)
    arrived("xt", xo)
    arrived("d2", d2o)
    weight_blocks(False)
    def deliver(h, n, value):
        kind, ref, hop = (
            (3, b["w_far2"].at[h], p_far[h]),
            (1, b["w_near2"].at[h, 0], p_to[h][0]),
            (2, b["w_near2"].at[h, 1], p_to[h][1]),
            (0, b["wmine"].at[h], {}),
        )[n]
        ref[...] = value
        for r, (dev, other) in enumerate(across):
            send("ws", (kind, h, r), ref.at[other], w_out.at[kind, h, zh], {**hop, **dev})

    w_far, w_near, w_unit = reducer("w", lambda h, q, p, slot: wown[h, q, p], deliver)
    w_far()

    for n in range(4):
        w_near(n)
    for c in own_m:
        c.wait()
    for t in range(2):
        for r in range(2):
            src = matrix_part(t, r, core)
            arrived(("m", t, r), src)
            send("mc", (t, r), src, src, d_core)
    for n in range(4):
        w_unit(n)
    arrived("dz", dd.at[0])
    arrived("dy", dd.at[1, :, oh])
    arrived("mc", mat.at[1, 0])

    def tokens(which, t):
        return jnp.concatenate(
            [dd[which, t, a].reshape(128, HEAD) for a in range(2)], axis=1
        )

    token_grads = jnp.concatenate([tokens(w, t) for w in range(2) for t in range(2)], axis=1)

    def input_block(i, carry):
        rows = pl.ds(pl.multiple_of(i * 512, 512), 512)
        cols = jnp.concatenate([mat[w, t, rows, :] for w in range(2) for t in range(2)], axis=1)
        igv[:, lanes(i * 512, 512)] = dot_tt(token_grads, cols).astype(BF16)
        return carry

    igv = b["igv"]
    lax.fori_loop(0, 4, input_block, 0)
    ig_copy = local("ig out", igv, ig_out)
    ig_copy.start()
    arrived("dqz", dqz)
    outs = [local("dq out", dqz, dq_out)]
    outs[0].start()
    arrived("ws", w_out)
    outs.append(ig_copy)
    for c in outs:
        c.wait()

    for group, kib in enumerate(filled):
        size_of = e_ref.at[0, pl.ds(0, kib), :]
        pltpu.make_async_copy(size_of, size_of, ssem.at[group]).wait()
    assert len(names) <= NSEM and len(local_names) <= NLOCAL


def finish(dq_in, ig_in, w_in, dq_out, ig_out, kw_out, vw_out):
    for c in range(CHUNKS):
        for kvh in range(2):
            for g in range(GROUP):
                at = (kvh * GROUP + g) * HEAD
                dq_out[c * 16 : (c + 1) * 16, at : at + HEAD] = dq_in[kvh, c, g]
    ig_out[...] = ig_in[...]
    for t, out in enumerate((kw_out, vw_out)):
        for n in range(2):
            parts = [w_in[kind, t, n].astype(F32) for kind in range(4)]
            out[:, n * HEAD : (n + 1) * HEAD] = (parts[0] + parts[1]) + (parts[2] + parts[3])


def local_step(q, k, v, g, x, mk, mv, placement):
    anywhere = pl.BlockSpec(memory_space=pl.ANY)
    vmem = pl.BlockSpec(memory_space=pltpu.VMEM)
    dq, ig, w = pl.pallas_call(
        kernel,
        out_shape=(
            jax.ShapeDtypeStruct((2, CHUNKS, GROUP, 16, HEAD), BF16),
            jax.ShapeDtypeStruct((128, FEATS // 2), BF16),
            jax.ShapeDtypeStruct((4, 2, 2, 64, HEAD), BF16),
        ),
        in_specs=[anywhere] * 7 + [vmem],
        out_specs=(anywhere,) * 3,
        scratch_shapes=[pltpu.VMEM(shape, dtype) for shape, dtype in BUFFERS.values()]
        + [
            pltpu.SemaphoreType.DMA((NSEND,)),
            pltpu.SemaphoreType.DMA((NSEM,)),
            pltpu.SemaphoreType.DMA((NLOCAL,)),
        ],
        compiler_params=pltpu.CompilerParams(
            collective_id=0, has_side_effects=True, vmem_limit_bytes=67043328
        ),
    )(
        q.reshape(CHUNKS, 16, -1),
        g.reshape(CHUNKS, 16, -1),
        k.reshape(CHUNKS, 16, -1),
        v.reshape(CHUNKS, 16, -1),
        x.reshape(CHUNKS, 16, -1),
        mk,
        mv,
        placement,
    )
    return pl.pallas_call(
        finish,
        out_shape=(
            jax.ShapeDtypeStruct((128, 2 * GROUP * HEAD), BF16),
            jax.ShapeDtypeStruct((128, FEATS // 2), BF16),
            jax.ShapeDtypeStruct((64, 2 * HEAD), F32),
            jax.ShapeDtypeStruct((64, 2 * HEAD), F32),
        ),
        in_specs=[vmem] * 3,
        out_specs=(vmem,) * 4,
    )(dq, ig, w)


def solution(mesh):
    torus = Mesh(
        mesh.devices.reshape(4, 2, 4, 2, mesh.shape["tp"]), ("seq_0", "seq_1", "seq_2", "seq_3", "tp")
    )
    rows = P(SEQ, "tp")
    return jax.shard_map(
        local_step,
        mesh=torus,
        in_specs=(rows, rows, rows, rows, rows, P(None, "tp"), P(None, "tp"), P()),
        out_specs=(rows, rows, rows, rows),
        check_vma=False,
    )
```

```python
import math

import jax
import jax.numpy as jnp
from jax import lax
from jax.experimental import pallas as pl
from jax.experimental.pallas import tpu as pltpu
from jax.sharding import Mesh
from jax.sharding import PartitionSpec as P

F32 = jnp.float32
BF16 = jnp.bfloat16
Y, ZH, X, CORE, ZL = "seq_0", "seq_1", "seq_2", "seq_3", "tp"
SEQ = (Y, ZH, X, CORE)
MESH = pl.DeviceIdType.MESH

HEAD = 128
GROUP = 4
WINDOW = 4096
CHUNKS = 8
BAND = 4
FEATS = 4096
SCALE = 1.0 / math.sqrt(HEAD)
SCALE2 = SCALE * math.log2(math.e)
MASKED = -1e30
QROWS = 256
KROWS = 128
NSEM = 71
NSEND = 5
NLOCAL = 9


def key_chunks(cq):
    return list(range(max(0, cq - BAND), cq + 1))


TILE_AT = [KROWS * sum(len(key_chunks(c)) for c in range(cq)) for cq in range(CHUNKS)]
TILE_ROWS = KROWS * sum(len(key_chunks(c)) for c in range(CHUNKS))

UNIT_KV = (2, 4, 2, 16, HEAD)
UNIT_W = (2, 64, HEAD)


def reduce_buffers(name, unit):
    half = unit[1:]
    return {
        name + "_far": ((2, 4) + unit, BF16),
        name + "_rfar": ((2, 2, 4) + half, BF16),
        name + "_near": ((2, 2, 4) + unit, BF16),
        name + "_rnear": ((2, 2, 4) + unit, BF16),
        name + "_far2": ((2,) + unit, BF16),
        name + "_rfar2": ((2,) + unit, BF16),
        name + "_near2": ((2, 2) + unit, BF16),
        name + "_rnear2": ((2, 2) + unit, BF16),
    }


BUFFERS = {
    "kv": ((2, 4, 4) + UNIT_KV, BF16),
    "qg": ((2, CHUNKS, 4, GROUP, 16, HEAD), BF16),
    "kpb": ((32, KROWS, 128), F32),
    "e": ((4, TILE_ROWS, QROWS), F32),
    "dp": ((4, TILE_ROWS, QROWS), F32),
    "st": ((3, 4, BAND + 1, CHUNKS, QROWS), F32),
    "ss": ((3, CHUNKS, QROWS), F32),
    "sr": ((3, CHUNKS, QROWS), F32),
    "fac": ((4, BAND + 1, CHUNKS, QROWS), F32),
    "delta": ((CHUNKS, QROWS), F32),
    "acc": ((2, 2, 4) + UNIT_KV, F32),
    "dqf": ((CHUNKS, 2, 2, GROUP, 16, HEAD), F32),
    "dqr": ((CHUNKS, 2, GROUP, 16, HEAD), F32),
    "dqs": ((2, CHUNKS, GROUP, 16, HEAD), BF16),
    "dqz": ((2, CHUNKS, GROUP, 16, HEAD), BF16),
    "kt": ((4, CHUNKS, HEAD, KROWS), BF16),
    "qp": ((CHUNKS, QROWS), F32),
    "xg": ((CHUNKS, 2, 16, FEATS), BF16),
    "xt": ((32, 2, 64, 256), BF16),
    "xo": ((32, 64, 256), BF16),
    "kst": ((2, CHUNKS, 16, 2 * HEAD), BF16),
    "mat": ((2, 2, FEATS // 2, 2 * HEAD), BF16),
    "d2": ((2, CHUNKS, 2, 16, HEAD), BF16),
    "d2o": ((2, CHUNKS, 2, 16, HEAD), BF16),
    "dd": ((2, 2, 2, CHUNKS, 16, HEAD), BF16),
    "wown": ((2, 4, 4) + UNIT_W, F32),
    "wmine": ((2,) + UNIT_W, BF16),
    "igv": ((128, FEATS // 2), BF16),
    "rp": ((64, 64), jnp.int32),
    **reduce_buffers("a", UNIT_KV),
    **reduce_buffers("w", UNIT_W),
}


def dot_tt(a, b):
    return lax.dot_general(a, b, (((1,), (1,)), ((), ())), preferred_element_type=F32)


def dot_nn(a, b):
    return lax.dot_general(a, b, (((1,), (0,)), ((), ())), preferred_element_type=F32)


def dot_tn(a, b):
    return lax.dot_general(a, b, (((0,), (0,)), ((), ())), preferred_element_type=F32)


def stack_rows(parts):
    return parts[0] if len(parts) == 1 else jnp.concatenate(parts, axis=0)


def positions(rp_in, kpb, qp, y, x, core):
    slots = rp_in[...].astype(F32).astype(BF16)

    def iota(shape, dim):
        return lax.broadcasted_iota(jnp.int32, shape, dim)

    def bits(a, at, width):
        return jnp.bitwise_and(jnp.right_shift(a, at), (1 << width) - 1)

    row, dev = iota((KROWS, 64), 0), iota((KROWS, 64), 1)
    p, zh, jj = bits(row, 5, 2), bits(row, 4, 1), bits(row, 1, 3)
    wide = iota((KROWS, 128), 0)
    inside = (bits(wide, 1, 3) * 128 + bits(wide, 0, 1)).astype(F32)
    ones = jnp.ones((64, 128), BF16)
    owner = [
        [((q * 2 + zh) * 4 + p) * 2 + core == dev for q in range(4)],
        [((p * 2 + zh) * 4 + q) * 2 + core == dev for q in range(4)],
    ]
    for c in range(CHUNKS):
        block = (dev == jj + 8 * c).astype(F32).astype(BF16)
        rows = dot_nn(block, slots)
        for q in range(4):
            picked = jnp.where(owner[c // 4][q], rows, 0.0).astype(BF16)
            kpb[c // 4 * 16 + q * 4 + c % 4] = (
                dot_nn(picked, ones) * 2.0 + (inside + float(c * 1024))
            )

    dev, lane = iota((64, QROWS), 0), iota((64, QROWS), 1)
    zh, co, jj = bits(lane, 7, 1), bits(lane, 6, 1), bits(lane, 1, 3)
    pick = (((y * 2 + zh) * 4 + x) * 2 + co == dev).astype(F32).astype(BF16)
    slot = dot_nn(slots, pick)
    here = bits(dev, 0, 3) == jj
    pos = jnp.where(here, slot * 2.0 + (dev * 128 + bits(lane, 0, 1)).astype(F32), 0.0)
    qp[...] = jnp.sum(pos.reshape(CHUNKS, 8, QROWS), axis=1)


def kernel(
    q_in, g_in, k_in, v_in, x_in, mk_in, mv_in, rp_in, dq_out, ig_out, w_out, *scratch
):
    ssem, rsem, lsem, relay = scratch[-4:]
    b = dict(zip(BUFFERS, scratch[:-4]))
    y, zh, x, core, zl = (lax.axis_index(a) for a in (Y, ZH, X, CORE, ZL))

    def turn(i, by):
        return lax.rem(i + by, 4)

    z = 2 * zh + zl
    zp, zm = turn(z, 1), turn(z, 3)
    zp_h, zp_l = lax.div(zp, 2), lax.rem(zp, 2)
    zm_h, zm_l = lax.div(zm, 2), lax.rem(zm, 2)
    oh, oc, ol = 1 - zh, 1 - core, 1 - zl
    d_core, d_tp = {CORE: oc}, {ZL: ol}
    across = ((d_tp, zh), ({ZH: oh, ZL: ol}, oh))
    d_zp, d_zm = {ZH: zp_h, ZL: zp_l}, {ZH: zm_h, ZL: zm_l}
    step_of = {a: ({a: turn(i, 1)}, {a: turn(i, 3)}) for a, i in ((X, x), (Y, y))}
    far_of = {X: {X: turn(x, 2)}, Y: {Y: turn(y, 2)}}
    d_zh = {ZH: oh}
    qi, pi = (y, x), (x, y)
    q_to = (step_of[Y], step_of[X])
    p_to = (step_of[X], step_of[Y])
    p_far = (far_of[X], far_of[Y])

    names = {}
    sent = {}
    filled = [0] * NSEND

    def remote(name, src, dst, dev, group=0):
        i = names.setdefault(name, len(names))
        return pltpu.make_async_remote_copy(
            src_ref=src,
            dst_ref=dst,
            send_sem=ssem.at[group],
            recv_sem=rsem.at[i],
            device_id=dev,
            device_id_type=MESH,
        )

    def send(name, part, src, dst, dev):
        kib = math.prod(src.shape) * src.dtype.itemsize // 1024
        if (name, part) not in sent:
            group = min(range(NSEND), key=lambda n: filled[n])
            filled[group] += kib
            sent[name, part] = group
        remote(name, src, dst, dev, sent[name, part]).start()

    def arrived(name, size_of):
        remote(name, size_of, size_of, d_core).wait_recv()

    local_names = {}

    def local(name, src, dst):
        i = local_names.setdefault(name, len(local_names))
        return pltpu.make_async_copy(src, dst, lsem.at[i])

    def lanes(start, width=128):
        return pl.ds(pl.multiple_of(start, 128), width)

    kv, qg, xg, mat = b["kv"], b["qg"], b["xg"], b["mat"]
    own_x = local("x", x_in, xg.at[:, zh, :, lanes(zl * (FEATS // 2), FEATS // 2)])
    half_feats = FEATS // 2
    quarter_feats = FEATS // 4
    own_m = [
        local(("m", t), ref.at[pl.ds(pl.multiple_of(zl * half_feats, half_feats), half_feats), :], mat.at[0, t])
        for t, ref in enumerate((mk_in, mv_in))
    ]
    kst = b["kst"]
    stage = [local(("kst", t), ref, kst.at[t]) for t, ref in enumerate((k_in, v_in))]
    stage_rp = local("rp", rp_in, b["rp"])
    for c in stage + [stage_rp]:
        c.start()

    barrier = pltpu.get_barrier_semaphore()
    peers = [d_core, *step_of[X], *step_of[Y], d_zp, d_zm]
    for dev in peers:
        pl.semaphore_signal(barrier, inc=1, device_id=dev, device_id_type=MESH)
    pl.semaphore_wait(barrier, len(peers))
    for a in (X, Y):
        pl.semaphore_signal(relay, inc=1, device_id=step_of[a][0], device_id_type=MESH)

    for c in stage:
        c.wait()

    for h in range(2):
        for r, (dev, head) in enumerate(across):
            for t in range(2):
                send(
                    ("zkv", h),
                    (t, r),
                    kst.at[t, pl.ds(4 * h, 4), :, lanes(head * HEAD)],
                    kv.at[h, qi[h], pi[h], t, :, zh],
                    dev,
                )
    for t, ref in enumerate((q_in, g_in)):
        for r, (dev, head) in enumerate(across):
            for g in range(GROUP):
                send(
                    ("qz", t, r),
                    g,
                    ref.at[:, :, lanes(head * GROUP * HEAD + g * HEAD)],
                    qg.at[t, :, 2 * zh + core, g],
                    dev,
                )

    unit_offs = (0, 3, 1, 2)

    def unit_piece(h, n, side):
        unit = kv.at[h, qi[h], turn(pi[h], unit_offs[n])]
        return ("q", h, n), side, unit, unit, q_to[h][side]

    def send_unit(h, n):
        for side in range(2):
            send(*unit_piece(h, n, side))

    def near_piece(h, n, side):
        return kv.at[h, turn(qi[h], 3 if side == 0 else 1), turn(pi[h], unit_offs[n])]

    def forward_piece(h, n, side):
        src = near_piece(h, n, side).at[side]
        return ("qf", h, side), n, src, src, q_to[h][side]

    def forward_unit(h, n):
        arrived(("q", h, n), kv.at[h, 0, pl.ds(0, 2)])
        for side in range(2):
            send(*forward_piece(h, n, side))

    pl.semaphore_wait(relay, 2)
    for h in range(2):
        arrived(("zkv", h), kv.at[h, qi[h], pi[h]])
        unit = kv.at[h, qi[h], pi[h]]
        for side in range(2):
            send(("p", h, side), 0, unit, unit, p_to[h][side])
    for h in range(2):
        unit = kv.at[h, qi[h], pi[h]]
        send(("pf", h), 0, unit, unit, p_far[h])

    for h in range(2):
        send_unit(h, 0)

    own_x.start()
    for c in own_m:
        c.start()
    b["st"][0] = jnp.full(b["st"].shape[1:], MASKED, F32)
    b["st"][1:] = jnp.zeros((2,) + b["st"].shape[1:], F32)
    stage_rp.wait()
    positions(b["rp"], b["kpb"], b["qp"], y, x, core)
    for h in range(2):
        for side in range(2):
            src = kv.at[h, qi[h], turn(pi[h], 3 if side == 0 else 1)]
            arrived(("p", h, side), src)
        for side in range(2):
            send_unit(h, 1 + side)
    for t in range(2):
        for r, (dev, head) in enumerate(across):
            src = qg.at[t, :, 2 * head + core]
            arrived(("qz", t, r), src)
            send(("qc", t), r, src, src, d_core)

    def send_matrix(t):
        ref = (mk_in, mv_in)[t]
        for r, (dev, _) in enumerate(across):
            at = (2 * r + core) * 512
            src = ref.at[pl.ds(pl.multiple_of(ol * half_feats + at, 512), 512), :]
            dst = mat.at[1, t, pl.ds(pl.multiple_of(at, 512), 512), :]
            yield ("m", t, r), 0, src, dst, dev

    def matrix_part(t, r, which):
        return mat.at[1, t, pl.ds(pl.multiple_of((2 * r + which) * 512, 512), 512), :]

    ring = (
        ("x+", d_zp, zm_h, zm_l, 0),
        ("x-", d_zm, zp_h, zp_l, quarter_feats),
    )
    for second in range(2):
        for name, dev, _, _, first in ring:
            at = quarter_feats - first if second else first
            send(
                (name, second),
                0,
                x_in.at[:, :, pl.ds(at, quarter_feats)],
                xg.at[:, zh, :, lanes(zl * half_feats + at, quarter_feats)],
                dev,
            )

    def ring_part(src_h, src_l, at):
        return xg.at[:, src_h, :, lanes(src_l * half_feats + at, quarter_feats)]

    def forward_input():
        for name, dev, src_h, src_l, first in ring:
            src = ring_part(src_h, src_l, first)
            arrived((name, 0), src)
            send((name, 2), 0, src, src, dev)

    def wait_input():
        own_x.wait()
        for name, _, src_h, src_l, first in ring:
            arrived((name, 1), ring_part(src_h, src_l, quarter_feats - first))
            arrived((name, 2), ring_part(oh, zl, first))

    for h in range(2):
        arrived(("pf", h), kv.at[h, qi[h], turn(pi[h], 2)])
        send_unit(h, 3)
    for t in range(2):
        arrived(("qc", t), qg.at[t, pl.ds(0, CHUNKS // 2)])

    def tile_rows(cq, ck):
        return pl.ds(TILE_AT[cq] + (ck - key_chunks(cq)[0]) * KROWS, KROWS)

    def queries(t, cq):
        return qg[t, cq].reshape(QROWS, HEAD)

    def keys(t, at, cks):
        return stack_rows(
            [kv[ck // 4, at[ck // 4], :, t, ck % 4].reshape(KROWS, HEAD) for ck in cks]
        )

    st, e_ref, dp_ref = b["st"], b["e"], b["dp"]

    def first_pass(s, carry):
        late = lax.div(s, 2)
        off = (1 - late) * s + late * (5 - s)

        @pl.when(s == 1)
        def _():
            for n in range(4):
                for h in range(2):
                    forward_unit(h, n)

        @pl.when(s == 3)
        def _():
            for h in range(2):
                for side in range(2):
                    arrived(("qf", h, side), kv.at[h, turn(qi[h], 2), :, side])
            forward_input()
            for t in range(2):
                for copy in send_matrix(t):
                    send(*copy)

        at = (turn(y, off), turn(x, off))
        for cq in range(CHUNKS):
            cks = key_chunks(cq)
            scores = dot_tt(keys(0, at, cks), queries(0, cq))
            dprobs = dot_tt(keys(1, at, cks), queries(1, cq))
            qpos = b["qp"][cq : cq + 1, :]
            for n, ck in enumerate(cks):
                part = slice(n * KROWS, (n + 1) * KROWS)
                score, dprob = scores[part] * SCALE2, dprobs[part]
                if ck == cq or ck == cq - BAND:
                    kpb = b["kpb"][ck // 4 * 16 + at[ck // 4] * 4 + ck % 4]
                    kpos = jnp.concatenate([kpb, kpb], axis=1)
                    seen = kpos <= qpos if ck == cq else kpos > qpos - WINDOW
                    score = jnp.where(seen, score, MASKED)
                top = jnp.max(score, axis=0, keepdims=True)
                expo = jnp.exp2(score - top)
                rows = tile_rows(cq, ck)
                e_ref[off, rows, :] = expo
                dp_ref[off, rows, :] = dprob
                row = slice(cq, cq + 1)
                st[0, off, cq - ck, row, :] = top
                st[1, off, cq - ck, row, :] = jnp.sum(expo, axis=0, keepdims=True)
                st[2, off, cq - ck, row, :] = jnp.sum(expo * dprob, axis=0, keepdims=True)
        return carry

    lax.fori_loop(0, 4, first_pass, 0)
    ss, sr = b["ss"], b["sr"]
    top_l = jnp.max(st[0], axis=(0, 1))
    fac_l = jnp.exp2(st[0] - top_l[None, None])
    sum_l = jnp.sum(st[1] * fac_l, axis=(0, 1))
    wgt_l = jnp.sum(st[2] * fac_l, axis=(0, 1))
    ss[0] = top_l
    ss[1] = sum_l
    ss[2] = wgt_l
    send("stat", 0, ss, sr, d_core)

    arrived("stat", sr)
    top = jnp.maximum(top_l, sr[0])
    mine_f = jnp.exp2(top_l - top)
    other_f = jnp.exp2(sr[0] - top)
    total = sum_l * mine_f + sr[1] * other_f
    b["delta"][...] = (wgt_l * mine_f + sr[2] * other_f) / total
    b["fac"][...] = fac_l * (mine_f / total)[None, None]

    offs = (2, 1, 3, 0)

    def reducer(name, unit_at, deliver=None):
        far, rfar = b[name + "_far"], b[name + "_rfar"]
        near, rnear = b[name + "_near"], b[name + "_rnear"]
        far2, rfar2 = b[name + "_far2"], b[name + "_rfar2"]
        near2, rnear2 = b[name + "_near2"], b[name + "_rnear2"]

        def place(h, n):
            return turn(pi[h], offs[n])

        def far_copy(h, n, side):
            p = place(h, n)
            return (
                (name, "far", n, side),
                h,
                far.at[h, p, side],
                rfar.at[h, side, p],
                q_to[h][side],
            )

        def near_copy(h, n, side):
            p = place(h, n)
            return (
                (name, "near", n),
                (h, side),
                near.at[h, side, p],
                rnear.at[h, side, p],
                q_to[h][side],
            )

        def start_far():
            for n in range(4):
                for h in range(2):
                    p = place(h, n)
                    far[h, p] = unit_at(h, turn(qi[h], 2), p, 0).astype(BF16)
                    for side in range(2):
                        send(*far_copy(h, n, side))

        def start_near(n):
            for side in (1, 0):
                arrived((name, "far", n, side), rfar.at[0, side, pl.ds(0, 2)])
                for h in range(2):
                    p = place(h, n)
                    value = unit_at(h, turn(qi[h], 1 if side == 0 else 3), p, 1 - side)
                    near[h, side, p, 1 - side] = value[1 - side].astype(BF16)
                    near[h, side, p, side] = (value[side] + rfar[h, side, p].astype(F32)).astype(
                        BF16
                    )
                    send(*near_copy(h, n, side))

        def own_unit(n):
            out = []
            arrived((name, "near", n), rnear.at[0, 0])
            for h in range(2):
                p = place(h, n)
                value = (
                    unit_at(h, qi[h], p, 0)
                    + rnear[h, 0, p].astype(F32)
                    + rnear[h, 1, p].astype(F32)
                )
                if deliver:
                    deliver(h, n, value.astype(BF16))
                elif n == 0:
                    far2[h] = value.astype(BF16)
                    send((name, "p", h), 2, far2.at[h], rfar2.at[h], p_far[h])
                elif n < 3:
                    side = n - 1
                    near2[h, side] = value.astype(BF16)
                    send(
                        (name, "p", h),
                        side,
                        near2.at[h, side],
                        rnear2.at[h, side],
                        p_to[h][side],
                    )
                else:
                    arrived((name, "p", h), rnear.at[0, 0, pl.ds(0, 3)])
                    out.append(
                        (value + rfar2[h].astype(F32))
                        + (rnear2[h, 0].astype(F32) + rnear2[h, 1].astype(F32))
                    )
            return out

        return start_far, start_near, own_unit

    acc = b["acc"]
    start_far, start_near, own_unit = reducer(
        "a", lambda h, q, p, slot: acc[slot, h, p]
    )

    fac, delta, kt = b["fac"], b["delta"], b["kt"]

    def second_pass(s, carry):
        late = lax.div(s, 2)
        off = (1 - late) * (2 + s) + late * (3 - s)
        slot = late * (3 - s)
        for ck in range(CHUNKS):
            probs, dscores = [], []
            cqs = [cq for cq in range(CHUNKS) if ck in key_chunks(cq)]
            for cq in cqs:
                rows = tile_rows(cq, ck)
                prob = e_ref[off, rows, :] * fac[off, cq - ck, cq : cq + 1, :]
                dscore = prob * (dp_ref[off, rows, :] - delta[cq : cq + 1, :])
                e_ref[off, rows, :] = dscore
                probs.append(prob.astype(BF16))
                dscores.append(dscore.astype(BF16))
            for t, parts in enumerate((dscores, probs)):
                depth = qg[t, ck : ck + len(cqs)].reshape(len(cqs) * QROWS, HEAD)
                grad = dot_nn(jnp.concatenate(parts, axis=1), depth)
                acc[slot, ck // 4, :, t, ck % 4] = grad.reshape(4, 2, 16, HEAD)

        @pl.when(s == 0)
        def _():
            start_far()

        @pl.when(s == 2)
        def _():
            for n in range(4):
                start_near(n)

        return carry

    lax.fori_loop(0, 4, second_pass, 0)
    dqf, dqr, dqs, dqz = b["dqf"], b["dqr"], b["dqs"], b["dqz"]
    own_unit(0)
    wait_input()
    xt, xo = b["xt"], b["xo"]

    def flip_input(i, carry):
        for n in range(4):
            at = i * 4 + n
            block = xg[:, :, :, lanes(at * 128)].reshape(256, 128)
            xt[at] = block.T.reshape(2, 64, 256)
        return carry

    lax.fori_loop(0, 8, flip_input, 0)
    send("xt", 0, xt.at[:, oc], xo, d_core)
    own_unit(1)
    own_unit(2)
    for off in range(4):
        at = (turn(y, off), turn(x, off))
        for ck in range(CHUNKS):
            kt[off, ck] = keys(0, at, [ck]).T
    for cq in range(CHUNKS):
        cks = key_chunks(cq)
        rows = pl.ds(TILE_AT[cq], KROWS * len(cks))
        flipped = jnp.concatenate([kt[off, ck] for off in range(4) for ck in cks], axis=1)
        dscore = jnp.concatenate([e_ref[off, rows, :].astype(BF16) for off in range(4)], axis=0)
        dqf[cq] = (dot_nn(flipped, dscore).T * SCALE).reshape(2, 2, GROUP, 16, HEAD)
    send("dqc", 0, dqf.at[:, :, oc], dqr, d_core)
    d2, d2o, dd = b["d2"], b["d2o"], b["dd"]
    for h, value in enumerate(own_unit(3)):
        d2[0, 4 * h : 4 * h + 4] = (value[0] * SCALE).astype(BF16)
        d2[1, 4 * h : 4 * h + 4] = value[1].astype(BF16)
    send("d2", 0, d2, d2o, d_core)
    for r, (dev, other) in enumerate(across):
        for t in range(2):
            send("dz", (t, r), d2.at[t, :, other], dd.at[0, t, zh], dev)
    for t in range(2):
        send("dy", t, d2.at[t, :, oh], dd.at[1, t, zh], d_zh)
        dd[1, t, zh] = d2[t, :, zh]

    wown = b["wown"]

    def grad_cols(ref):
        return jnp.concatenate([ref[0].reshape(256, HEAD), ref[1].reshape(256, HEAD)], axis=1)

    def weight_blocks(first):
        cols = grad_cols(d2 if first else d2o)

        def body(i, carry):
            for wy in (2 * i, 2 * i + 1):
                rows = (xt[pl.ds(wy * 8, 8), core] if first else xo[pl.ds(wy * 8, 8)]).reshape(512, 256)
                part = dot_nn(rows, cols)
                for wz in range(2):
                    for wx in range(4):
                        for h, (wq, wp) in enumerate(((wy, wx), (wx, wy))):
                            base = (wz * 4 + wx) * 64
                            block = part[base : base + 64, h * HEAD : (h + 1) * HEAD]
                            if first:
                                wown[h, wq, wp, wz] = block
                            else:
                                wown[h, wq, wp, wz] = wown[h, wq, wp, wz] + block
            return carry

        lax.fori_loop(0, 2, body, 0)

    weight_blocks(True)
    arrived("dqc", dqr)
    for n in range(2):
        dqs[n] = (dqf[:, n, core] + dqr[:, n]).astype(BF16)
    for r, (dev, other) in enumerate(across):
        send("dqz", r, dqs.at[other], dqz.at[zh], dev)
    arrived("xt", xo)
    arrived("d2", d2o)
    weight_blocks(False)
    def deliver(h, n, value):
        kind, ref, hop = (
            (3, b["w_far2"].at[h], p_far[h]),
            (1, b["w_near2"].at[h, 0], p_to[h][0]),
            (2, b["w_near2"].at[h, 1], p_to[h][1]),
            (0, b["wmine"].at[h], {}),
        )[n]
        ref[...] = value
        for r, (dev, other) in enumerate(across):
            send("ws", (kind, h, r), ref.at[other], w_out.at[kind, h, zh], {**hop, **dev})

    w_far, w_near, w_unit = reducer("w", lambda h, q, p, slot: wown[h, q, p], deliver)
    w_far()

    for n in range(4):
        w_near(n)
    for c in own_m:
        c.wait()
    for t in range(2):
        for r in range(2):
            src = matrix_part(t, r, core)
            arrived(("m", t, r), src)
            send("mc", (t, r), src, src, d_core)
    for n in range(4):
        w_unit(n)
    arrived("dz", dd.at[0])
    arrived("dy", dd.at[1, :, oh])
    arrived("mc", mat.at[1, 0])

    def tokens(which, t):
        return jnp.concatenate(
            [dd[which, t, a].reshape(128, HEAD) for a in range(2)], axis=1
        )

    token_grads = jnp.concatenate([tokens(w, t) for w in range(2) for t in range(2)], axis=1)

    def input_block(i, carry):
        rows = pl.ds(pl.multiple_of(i * 512, 512), 512)
        cols = jnp.concatenate([mat[w, t, rows, :] for w in range(2) for t in range(2)], axis=1)
        igv[:, lanes(i * 512, 512)] = dot_tt(token_grads, cols).astype(BF16)
        return carry

    igv = b["igv"]
    lax.fori_loop(0, 4, input_block, 0)
    ig_copy = local("ig out", igv, ig_out)
    ig_copy.start()
    arrived("dqz", dqz)
    outs = [local("dq out", dqz, dq_out)]
    outs[0].start()
    arrived("ws", w_out)
    outs.append(ig_copy)
    for c in outs:
        c.wait()

    for group, kib in enumerate(filled):
        size_of = e_ref.at[0, pl.ds(0, kib), :]
        pltpu.make_async_copy(size_of, size_of, ssem.at[group]).wait()
    assert len(names) <= NSEM and len(local_names) <= NLOCAL


def finish(dq_in, ig_in, w_in, dq_out, ig_out, kw_out, vw_out, dq, ig, w, kv_w, sems):
    copies = [pltpu.make_async_copy(w_in, w, sems.at[0])]
    for kvh in range(2):
        for g in range(GROUP):
            at = (kvh * GROUP + g) * HEAD
            copies.append(
                pltpu.make_async_copy(dq_in.at[kvh, :, g], dq.at[:, :, at : at + HEAD], sems.at[1])
            )
    copies.append(pltpu.make_async_copy(ig_in, ig, sems.at[2]))
    for c in copies:
        c.start()
    whole = [
        pltpu.make_async_copy(dq, dq_out, sems.at[1]),
        pltpu.make_async_copy(ig, ig_out, sems.at[2]),
        pltpu.make_async_copy(kv_w.at[0], kw_out, sems.at[3]),
        pltpu.make_async_copy(kv_w.at[1], vw_out, sems.at[4]),
    ]
    copies[0].wait()
    for t in range(2):
        for n in range(2):
            parts = [w[kind, t, n].astype(F32) for kind in range(4)]
            kv_w[t, :, n * HEAD : (n + 1) * HEAD] = (parts[0] + parts[1]) + (parts[2] + parts[3])
    whole[2].start()
    whole[3].start()
    whole[0].wait()
    whole[0].start()
    copies[-1].wait()
    whole[1].start()
    for c in whole:
        c.wait()


def local_step(q, k, v, g, x, mk, mv, placement):
    anywhere = pl.BlockSpec(memory_space=pl.ANY)
    dq, ig, w = pl.pallas_call(
        kernel,
        out_shape=(
            jax.ShapeDtypeStruct((2, CHUNKS, GROUP, 16, HEAD), BF16),
            jax.ShapeDtypeStruct((128, FEATS // 2), BF16),
            jax.ShapeDtypeStruct((4, 2, 2, 64, HEAD), BF16),
        ),
        in_specs=[anywhere] * 8,
        out_specs=(anywhere,) * 3,
        scratch_shapes=[pltpu.VMEM(shape, dtype) for shape, dtype in BUFFERS.values()]
        + [
            pltpu.SemaphoreType.DMA((NSEND,)),
            pltpu.SemaphoreType.DMA((NSEM,)),
            pltpu.SemaphoreType.DMA((NLOCAL,)),
            pltpu.SemaphoreType.REGULAR,
        ],
        compiler_params=pltpu.CompilerParams(
            collective_id=0, has_side_effects=True, vmem_limit_bytes=67043328
        ),
    )(
        q.reshape(CHUNKS, 16, -1),
        g.reshape(CHUNKS, 16, -1),
        k.reshape(CHUNKS, 16, -1),
        v.reshape(CHUNKS, 16, -1),
        x.reshape(CHUNKS, 16, -1),
        mk,
        mv,
        placement,
    )
    query_grad, *rest = pl.pallas_call(
        finish,
        out_shape=(
            jax.ShapeDtypeStruct((CHUNKS, 16, 2 * GROUP * HEAD), BF16),
            jax.ShapeDtypeStruct((128, FEATS // 2), BF16),
            jax.ShapeDtypeStruct((64, 2 * HEAD), F32),
            jax.ShapeDtypeStruct((64, 2 * HEAD), F32),
        ),
        in_specs=[anywhere] * 3,
        out_specs=(anywhere,) * 4,
        scratch_shapes=[
            pltpu.VMEM((CHUNKS, 16, 2 * GROUP * HEAD), BF16),
            pltpu.VMEM((128, FEATS // 2), BF16),
            pltpu.VMEM((4, 2, 2, 64, HEAD), BF16),
            pltpu.VMEM((2, 64, 2 * HEAD), F32),
            pltpu.SemaphoreType.DMA((5,)),
        ],
    )(dq, ig, w)
    return (query_grad.reshape(128, -1), *rest)


def solution(mesh):
    torus = Mesh(
        mesh.devices.reshape(4, 2, 4, 2, mesh.shape["tp"]), ("seq_0", "seq_1", "seq_2", "seq_3", "tp")
    )
    rows = P(SEQ, "tp")
    return jax.shard_map(
        local_step,
        mesh=torus,
        in_specs=(rows, rows, rows, rows, rows, P(None, "tp"), P(None, "tp"), P()),
        out_specs=(rows, rows, rows, rows),
        check_vma=False,
    )
```

```python
import math

import jax
import jax.numpy as jnp
from jax import lax
from jax.experimental import pallas as pl
from jax.experimental.pallas import tpu as pltpu
from jax.sharding import Mesh
from jax.sharding import PartitionSpec as P

F32 = jnp.float32
BF16 = jnp.bfloat16
Y, ZH, X, CORE, ZL = "seq_0", "seq_1", "seq_2", "seq_3", "tp"
SEQ = (Y, ZH, X, CORE)
MESH = pl.DeviceIdType.MESH

HEAD = 128
GROUP = 4
WINDOW = 4096
CHUNKS = 8
BAND = 4
FEATS = 4096
SCALE = 1.0 / math.sqrt(HEAD)
SCALE2 = SCALE * math.log2(math.e)
MASKED = -1e30
QROWS = 256
KROWS = 128
NSEM = 71
NSEND = 5
NLOCAL = 9


def key_chunks(cq):
    return list(range(max(0, cq - BAND), cq + 1))


TILE_AT = [KROWS * sum(len(key_chunks(c)) for c in range(cq)) for cq in range(CHUNKS)]
TILE_ROWS = KROWS * sum(len(key_chunks(c)) for c in range(CHUNKS))

UNIT_KV = (2, 4, 2, 16, HEAD)
UNIT_W = (2, 64, HEAD)


def reduce_buffers(name, unit):
    half = unit[1:]
    return {
        name + "_far": ((2, 4) + unit, BF16),
        name + "_rfar": ((2, 2, 4) + half, BF16),
        name + "_near": ((2, 2, 4) + unit, BF16),
        name + "_rnear": ((2, 2, 4) + unit, BF16),
        name + "_far2": ((2,) + unit, BF16),
        name + "_rfar2": ((2,) + unit, BF16),
        name + "_near2": ((2, 2) + unit, BF16),
        name + "_rnear2": ((2, 2) + unit, BF16),
    }


BUFFERS = {
    "kv": ((2, 4, 4) + UNIT_KV, BF16),
    "qg": ((2, CHUNKS, 4, GROUP, 16, HEAD), BF16),
    "kpb": ((32, KROWS, 128), F32),
    "e": ((4, TILE_ROWS, QROWS), F32),
    "dp": ((4, TILE_ROWS, QROWS), F32),
    "st": ((3, 4, BAND + 1, CHUNKS, QROWS), F32),
    "ss": ((3, CHUNKS, QROWS), F32),
    "sr": ((3, CHUNKS, QROWS), F32),
    "fac": ((4, BAND + 1, CHUNKS, QROWS), F32),
    "delta": ((CHUNKS, QROWS), F32),
    "acc": ((2, 2, 4) + UNIT_KV, F32),
    "dqf": ((CHUNKS, 2, 2, GROUP, 16, HEAD), F32),
    "dqr": ((CHUNKS, 2, GROUP, 16, HEAD), F32),
    "dqs": ((2, CHUNKS, GROUP, 16, HEAD), BF16),
    "kt": ((4, CHUNKS, HEAD, KROWS), BF16),
    "qp": ((CHUNKS, QROWS), F32),
    "xg": ((CHUNKS, 2, 16, FEATS), BF16),
    "xt": ((32, 2, 64, 256), BF16),
    "xo": ((32, 64, 256), BF16),
    "kst": ((2, CHUNKS, 16, 2 * HEAD), BF16),
    "mat": ((2, 2, FEATS // 2, 2 * HEAD), BF16),
    "d2": ((2, CHUNKS, 2, 16, HEAD), BF16),
    "d2o": ((2, CHUNKS, 2, 16, HEAD), BF16),
    "dd": ((2, 2, 2, CHUNKS, 16, HEAD), BF16),
    "wown": ((2, 4, 4) + UNIT_W, F32),
    "wmine": ((2,) + UNIT_W, BF16),
    "rp": ((64, 64), jnp.int32),
    **reduce_buffers("a", UNIT_KV),
    **reduce_buffers("w", UNIT_W),
}


def dot_tt(a, b):
    return lax.dot_general(a, b, (((1,), (1,)), ((), ())), preferred_element_type=F32)


def dot_nn(a, b):
    return lax.dot_general(a, b, (((1,), (0,)), ((), ())), preferred_element_type=F32)


def dot_tn(a, b):
    return lax.dot_general(a, b, (((0,), (0,)), ((), ())), preferred_element_type=F32)


def stack_rows(parts):
    return parts[0] if len(parts) == 1 else jnp.concatenate(parts, axis=0)


def positions(rp_in, kpb, qp, y, x, core):
    slots = rp_in[...].astype(F32).astype(BF16)

    def iota(shape, dim):
        return lax.broadcasted_iota(jnp.int32, shape, dim)

    def bits(a, at, width):
        return jnp.bitwise_and(jnp.right_shift(a, at), (1 << width) - 1)

    row, dev = iota((KROWS, 64), 0), iota((KROWS, 64), 1)
    p, zh, jj = bits(row, 5, 2), bits(row, 4, 1), bits(row, 1, 3)
    wide = iota((KROWS, 128), 0)
    inside = (bits(wide, 1, 3) * 128 + bits(wide, 0, 1)).astype(F32)
    ones = jnp.ones((64, 128), BF16)
    owner = [
        [((q * 2 + zh) * 4 + p) * 2 + core == dev for q in range(4)],
        [((p * 2 + zh) * 4 + q) * 2 + core == dev for q in range(4)],
    ]
    for c in range(CHUNKS):
        block = (dev == jj + 8 * c).astype(F32).astype(BF16)
        rows = dot_nn(block, slots)
        for q in range(4):
            picked = jnp.where(owner[c // 4][q], rows, 0.0).astype(BF16)
            kpb[c // 4 * 16 + q * 4 + c % 4] = (
                dot_nn(picked, ones) * 2.0 + (inside + float(c * 1024))
            )

    dev, lane = iota((64, QROWS), 0), iota((64, QROWS), 1)
    zh, co, jj = bits(lane, 7, 1), bits(lane, 6, 1), bits(lane, 1, 3)
    pick = (((y * 2 + zh) * 4 + x) * 2 + co == dev).astype(F32).astype(BF16)
    slot = dot_nn(slots, pick)
    here = bits(dev, 0, 3) == jj
    pos = jnp.where(here, slot * 2.0 + (dev * 128 + bits(lane, 0, 1)).astype(F32), 0.0)
    qp[...] = jnp.sum(pos.reshape(CHUNKS, 8, QROWS), axis=1)


def kernel(
    q_in, g_in, k_in, v_in, x_in, mk_in, mv_in, rp_in, dq_out, ig_out, w_out, *scratch
):
    ssem, rsem, lsem, relay = scratch[-4:]
    b = dict(zip(BUFFERS, scratch[:-4]))
    y, zh, x, core, zl = (lax.axis_index(a) for a in (Y, ZH, X, CORE, ZL))

    def turn(i, by):
        return lax.rem(i + by, 4)

    z = 2 * zh + zl
    zp, zm = turn(z, 1), turn(z, 3)
    zp_h, zp_l = lax.div(zp, 2), lax.rem(zp, 2)
    zm_h, zm_l = lax.div(zm, 2), lax.rem(zm, 2)
    oh, oc, ol = 1 - zh, 1 - core, 1 - zl
    d_core, d_tp = {CORE: oc}, {ZL: ol}
    across = ((d_tp, zh), ({ZH: oh, ZL: ol}, oh))
    d_zp, d_zm = {ZH: zp_h, ZL: zp_l}, {ZH: zm_h, ZL: zm_l}
    step_of = {a: ({a: turn(i, 1)}, {a: turn(i, 3)}) for a, i in ((X, x), (Y, y))}
    far_of = {X: {X: turn(x, 2)}, Y: {Y: turn(y, 2)}}
    d_zh = {ZH: oh}
    qi, pi = (y, x), (x, y)
    q_to = (step_of[Y], step_of[X])
    p_to = (step_of[X], step_of[Y])
    p_far = (far_of[X], far_of[Y])

    names = {}
    sent = {}
    filled = [0] * NSEND

    def remote(name, src, dst, dev, group=0):
        i = names.setdefault(name, len(names))
        return pltpu.make_async_remote_copy(
            src_ref=src,
            dst_ref=dst,
            send_sem=ssem.at[group],
            recv_sem=rsem.at[i],
            device_id=dev,
            device_id_type=MESH,
        )

    def send(name, part, src, dst, dev):
        kib = math.prod(src.shape) * src.dtype.itemsize // 1024
        if (name, part) not in sent:
            group = min(range(NSEND), key=lambda n: filled[n])
            filled[group] += kib
            sent[name, part] = group
        remote(name, src, dst, dev, sent[name, part]).start()

    def arrived(name, size_of):
        remote(name, size_of, size_of, d_core).wait_recv()

    local_names = {}

    def local(name, src, dst):
        i = local_names.setdefault(name, len(local_names))
        return pltpu.make_async_copy(src, dst, lsem.at[i])

    def lanes(start, width=128):
        return pl.ds(pl.multiple_of(start, 128), width)

    kv, qg, xg, mat = b["kv"], b["qg"], b["xg"], b["mat"]
    own_x = local("x", x_in, xg.at[:, zh, :, lanes(zl * (FEATS // 2), FEATS // 2)])
    half_feats = FEATS // 2
    quarter_feats = FEATS // 4
    own_m = [
        local(("m", t), ref.at[pl.ds(pl.multiple_of(zl * half_feats, half_feats), half_feats), :], mat.at[0, t])
        for t, ref in enumerate((mk_in, mv_in))
    ]
    kst = b["kst"]
    stage = [local(("kst", t), ref, kst.at[t]) for t, ref in enumerate((k_in, v_in))]
    stage_rp = local("rp", rp_in, b["rp"])
    for c in stage + [stage_rp]:
        c.start()

    barrier = pltpu.get_barrier_semaphore()
    peers = [d_core, *step_of[X], *step_of[Y], d_zp, d_zm]
    for dev in peers:
        pl.semaphore_signal(barrier, inc=1, device_id=dev, device_id_type=MESH)
    pl.semaphore_wait(barrier, len(peers))
    for a in (X, Y):
        pl.semaphore_signal(relay, inc=1, device_id=step_of[a][0], device_id_type=MESH)

    for c in stage:
        c.wait()

    for h in range(2):
        for r, (dev, head) in enumerate(across):
            for t in range(2):
                send(
                    ("zkv", h),
                    (t, r),
                    kst.at[t, pl.ds(4 * h, 4), :, lanes(head * HEAD)],
                    kv.at[h, qi[h], pi[h], t, :, zh],
                    dev,
                )
    for t, ref in enumerate((q_in, g_in)):
        for r, (dev, head) in enumerate(across):
            for g in range(GROUP):
                send(
                    ("qz", t, r),
                    g,
                    ref.at[:, :, lanes(head * GROUP * HEAD + g * HEAD)],
                    qg.at[t, :, 2 * zh + core, g],
                    dev,
                )

    unit_offs = (0, 3, 1, 2)

    def unit_piece(h, n, side):
        unit = kv.at[h, qi[h], turn(pi[h], unit_offs[n])]
        return ("q", h, n), side, unit, unit, q_to[h][side]

    def send_unit(h, n):
        for side in range(2):
            send(*unit_piece(h, n, side))

    def near_piece(h, n, side):
        return kv.at[h, turn(qi[h], 3 if side == 0 else 1), turn(pi[h], unit_offs[n])]

    def forward_piece(h, n, side):
        src = near_piece(h, n, side).at[side]
        return ("qf", h, side), n, src, src, q_to[h][side]

    def forward_unit(h, n):
        arrived(("q", h, n), kv.at[h, 0, pl.ds(0, 2)])
        for side in range(2):
            send(*forward_piece(h, n, side))

    pl.semaphore_wait(relay, 2)
    for h in range(2):
        arrived(("zkv", h), kv.at[h, qi[h], pi[h]])
        unit = kv.at[h, qi[h], pi[h]]
        for side in range(2):
            send(("p", h, side), 0, unit, unit, p_to[h][side])
    for h in range(2):
        unit = kv.at[h, qi[h], pi[h]]
        send(("pf", h), 0, unit, unit, p_far[h])

    for h in range(2):
        send_unit(h, 0)

    own_x.start()
    for c in own_m:
        c.start()
    b["st"][0] = jnp.full(b["st"].shape[1:], MASKED, F32)
    b["st"][1:] = jnp.zeros((2,) + b["st"].shape[1:], F32)
    stage_rp.wait()
    positions(b["rp"], b["kpb"], b["qp"], y, x, core)
    for h in range(2):
        for side in range(2):
            src = kv.at[h, qi[h], turn(pi[h], 3 if side == 0 else 1)]
            arrived(("p", h, side), src)
        for side in range(2):
            send_unit(h, 1 + side)
    for t in range(2):
        for r, (dev, head) in enumerate(across):
            src = qg.at[t, :, 2 * head + core]
            arrived(("qz", t, r), src)
            send(("qc", t), r, src, src, d_core)

    def send_matrix(t):
        ref = (mk_in, mv_in)[t]
        for r, (dev, _) in enumerate(across):
            at = (2 * r + core) * 512
            src = ref.at[pl.ds(pl.multiple_of(ol * half_feats + at, 512), 512), :]
            dst = mat.at[1, t, pl.ds(pl.multiple_of(at, 512), 512), :]
            yield ("m", t, r), 0, src, dst, dev

    def matrix_part(t, r, which):
        return mat.at[1, t, pl.ds(pl.multiple_of((2 * r + which) * 512, 512), 512), :]

    ring = (
        ("x+", d_zp, zm_h, zm_l, 0),
        ("x-", d_zm, zp_h, zp_l, quarter_feats),
    )
    for second in range(2):
        for name, dev, _, _, first in ring:
            at = quarter_feats - first if second else first
            send(
                (name, second),
                0,
                x_in.at[:, :, pl.ds(at, quarter_feats)],
                xg.at[:, zh, :, lanes(zl * half_feats + at, quarter_feats)],
                dev,
            )

    def ring_part(src_h, src_l, at):
        return xg.at[:, src_h, :, lanes(src_l * half_feats + at, quarter_feats)]

    def forward_input():
        for name, dev, src_h, src_l, first in ring:
            src = ring_part(src_h, src_l, first)
            arrived((name, 0), src)
            send((name, 2), 0, src, src, dev)

    def wait_input():
        own_x.wait()
        for name, _, src_h, src_l, first in ring:
            arrived((name, 1), ring_part(src_h, src_l, quarter_feats - first))
            arrived((name, 2), ring_part(oh, zl, first))

    for h in range(2):
        arrived(("pf", h), kv.at[h, qi[h], turn(pi[h], 2)])
        send_unit(h, 3)
    for t in range(2):
        arrived(("qc", t), qg.at[t, pl.ds(0, CHUNKS // 2)])

    def tile_rows(cq, ck):
        return pl.ds(TILE_AT[cq] + (ck - key_chunks(cq)[0]) * KROWS, KROWS)

    def queries(t, cq):
        return qg[t, cq].reshape(QROWS, HEAD)

    def keys(t, at, cks):
        return stack_rows(
            [kv[ck // 4, at[ck // 4], :, t, ck % 4].reshape(KROWS, HEAD) for ck in cks]
        )

    st, e_ref, dp_ref = b["st"], b["e"], b["dp"]

    def first_pass(s, carry):
        late = lax.div(s, 2)
        off = (1 - late) * s + late * (5 - s)

        @pl.when(s == 1)
        def _():
            for n in range(4):
                for h in range(2):
                    forward_unit(h, n)

        @pl.when(s == 3)
        def _():
            for h in range(2):
                for side in range(2):
                    arrived(("qf", h, side), kv.at[h, turn(qi[h], 2), :, side])
            forward_input()
            for t in range(2):
                for copy in send_matrix(t):
                    send(*copy)

        at = (turn(y, off), turn(x, off))
        for cq in range(CHUNKS):
            cks = key_chunks(cq)
            scores = dot_tt(keys(0, at, cks), queries(0, cq))
            dprobs = dot_tt(keys(1, at, cks), queries(1, cq))
            qpos = b["qp"][cq : cq + 1, :]
            for n, ck in enumerate(cks):
                part = slice(n * KROWS, (n + 1) * KROWS)
                score, dprob = scores[part] * SCALE2, dprobs[part]
                if ck == cq or ck == cq - BAND:
                    kpb = b["kpb"][ck // 4 * 16 + at[ck // 4] * 4 + ck % 4]
                    kpos = jnp.concatenate([kpb, kpb], axis=1)
                    seen = kpos <= qpos if ck == cq else kpos > qpos - WINDOW
                    score = jnp.where(seen, score, MASKED)
                top = jnp.max(score, axis=0, keepdims=True)
                expo = jnp.exp2(score - top)
                rows = tile_rows(cq, ck)
                e_ref[off, rows, :] = expo
                dp_ref[off, rows, :] = dprob
                row = slice(cq, cq + 1)
                st[0, off, cq - ck, row, :] = top
                st[1, off, cq - ck, row, :] = jnp.sum(expo, axis=0, keepdims=True)
                st[2, off, cq - ck, row, :] = jnp.sum(expo * dprob, axis=0, keepdims=True)
        return carry

    lax.fori_loop(0, 4, first_pass, 0)
    ss, sr = b["ss"], b["sr"]
    top_l = jnp.max(st[0], axis=(0, 1))
    fac_l = jnp.exp2(st[0] - top_l[None, None])
    sum_l = jnp.sum(st[1] * fac_l, axis=(0, 1))
    wgt_l = jnp.sum(st[2] * fac_l, axis=(0, 1))
    ss[0] = top_l
    ss[1] = sum_l
    ss[2] = wgt_l
    send("stat", 0, ss, sr, d_core)

    arrived("stat", sr)
    top = jnp.maximum(top_l, sr[0])
    mine_f = jnp.exp2(top_l - top)
    other_f = jnp.exp2(sr[0] - top)
    total = sum_l * mine_f + sr[1] * other_f
    b["delta"][...] = (wgt_l * mine_f + sr[2] * other_f) / total
    b["fac"][...] = fac_l * (mine_f / total)[None, None]

    offs = (2, 1, 3, 0)

    def reducer(name, unit_at, deliver=None):
        far, rfar = b[name + "_far"], b[name + "_rfar"]
        near, rnear = b[name + "_near"], b[name + "_rnear"]
        far2, rfar2 = b[name + "_far2"], b[name + "_rfar2"]
        near2, rnear2 = b[name + "_near2"], b[name + "_rnear2"]

        def place(h, n):
            return turn(pi[h], offs[n])

        def far_copy(h, n, side):
            p = place(h, n)
            return (
                (name, "far", n, side),
                h,
                far.at[h, p, side],
                rfar.at[h, side, p],
                q_to[h][side],
            )

        def near_copy(h, n, side):
            p = place(h, n)
            return (
                (name, "near", n),
                (h, side),
                near.at[h, side, p],
                rnear.at[h, side, p],
                q_to[h][side],
            )

        def start_far():
            for n in range(4):
                for h in range(2):
                    p = place(h, n)
                    far[h, p] = unit_at(h, turn(qi[h], 2), p, 0).astype(BF16)
                    for side in range(2):
                        send(*far_copy(h, n, side))

        def start_near(n):
            for side in (1, 0):
                arrived((name, "far", n, side), rfar.at[0, side, pl.ds(0, 2)])
                for h in range(2):
                    p = place(h, n)
                    value = unit_at(h, turn(qi[h], 1 if side == 0 else 3), p, 1 - side)
                    near[h, side, p, 1 - side] = value[1 - side].astype(BF16)
                    near[h, side, p, side] = (value[side] + rfar[h, side, p].astype(F32)).astype(
                        BF16
                    )
                    send(*near_copy(h, n, side))

        def own_unit(n):
            out = []
            arrived((name, "near", n), rnear.at[0, 0])
            for h in range(2):
                p = place(h, n)
                value = (
                    unit_at(h, qi[h], p, 0)
                    + rnear[h, 0, p].astype(F32)
                    + rnear[h, 1, p].astype(F32)
                )
                if deliver:
                    deliver(h, n, value.astype(BF16))
                elif n == 0:
                    far2[h] = value.astype(BF16)
                    send((name, "p", h), 2, far2.at[h], rfar2.at[h], p_far[h])
                elif n < 3:
                    side = n - 1
                    near2[h, side] = value.astype(BF16)
                    send(
                        (name, "p", h),
                        side,
                        near2.at[h, side],
                        rnear2.at[h, side],
                        p_to[h][side],
                    )
                else:
                    arrived((name, "p", h), rnear.at[0, 0, pl.ds(0, 3)])
                    out.append(
                        (value + rfar2[h].astype(F32))
                        + (rnear2[h, 0].astype(F32) + rnear2[h, 1].astype(F32))
                    )
            return out

        return start_far, start_near, own_unit

    acc = b["acc"]
    start_far, start_near, own_unit = reducer(
        "a", lambda h, q, p, slot: acc[slot, h, p]
    )

    fac, delta, kt = b["fac"], b["delta"], b["kt"]

    def second_pass(s, carry):
        late = lax.div(s, 2)
        off = (1 - late) * (2 + s) + late * (3 - s)
        slot = late * (3 - s)
        for ck in range(CHUNKS):
            probs, dscores = [], []
            cqs = [cq for cq in range(CHUNKS) if ck in key_chunks(cq)]
            for cq in cqs:
                rows = tile_rows(cq, ck)
                prob = e_ref[off, rows, :] * fac[off, cq - ck, cq : cq + 1, :]
                dscore = prob * (dp_ref[off, rows, :] - delta[cq : cq + 1, :])
                e_ref[off, rows, :] = dscore
                probs.append(prob.astype(BF16))
                dscores.append(dscore.astype(BF16))
            for t, parts in enumerate((dscores, probs)):
                depth = qg[t, ck : ck + len(cqs)].reshape(len(cqs) * QROWS, HEAD)
                grad = dot_nn(jnp.concatenate(parts, axis=1), depth)
                acc[slot, ck // 4, :, t, ck % 4] = grad.reshape(4, 2, 16, HEAD)

        @pl.when(s == 0)
        def _():
            start_far()

        @pl.when(s == 2)
        def _():
            for n in range(4):
                start_near(n)

        return carry

    lax.fori_loop(0, 4, second_pass, 0)
    dqf, dqr, dqs = b["dqf"], b["dqr"], b["dqs"]
    own_unit(0)
    wait_input()
    xt, xo = b["xt"], b["xo"]

    def flip_input(i, carry):
        for n in range(4):
            at = i * 4 + n
            block = xg[:, :, :, lanes(at * 128)].reshape(256, 128)
            xt[at] = block.T.reshape(2, 64, 256)
        return carry

    lax.fori_loop(0, 8, flip_input, 0)
    send("xt", 0, xt.at[:, oc], xo, d_core)
    own_unit(1)
    own_unit(2)
    for off in range(4):
        at = (turn(y, off), turn(x, off))
        for ck in range(CHUNKS):
            kt[off, ck] = keys(0, at, [ck]).T
    for cq in range(CHUNKS):
        cks = key_chunks(cq)
        rows = pl.ds(TILE_AT[cq], KROWS * len(cks))
        flipped = jnp.concatenate([kt[off, ck] for off in range(4) for ck in cks], axis=1)
        dscore = jnp.concatenate([e_ref[off, rows, :].astype(BF16) for off in range(4)], axis=0)
        dqf[cq] = (dot_nn(flipped, dscore).T * SCALE).reshape(2, 2, GROUP, 16, HEAD)
    send("dqc", 0, dqf.at[:, :, oc], dqr, d_core)
    d2, d2o, dd = b["d2"], b["d2o"], b["dd"]
    for h, value in enumerate(own_unit(3)):
        d2[0, 4 * h : 4 * h + 4] = (value[0] * SCALE).astype(BF16)
        d2[1, 4 * h : 4 * h + 4] = value[1].astype(BF16)
    send("d2", 0, d2, d2o, d_core)
    for r, (dev, other) in enumerate(across):
        for t in range(2):
            send("dz", (t, r), d2.at[t, :, other], dd.at[0, t, zh], dev)
    for t in range(2):
        send("dy", t, d2.at[t, :, oh], dd.at[1, t, zh], d_zh)
        dd[1, t, zh] = d2[t, :, zh]

    wown = b["wown"]

    def grad_cols(ref):
        return jnp.concatenate([ref[0].reshape(256, HEAD), ref[1].reshape(256, HEAD)], axis=1)

    def weight_blocks(first):
        cols = grad_cols(d2 if first else d2o)

        def body(i, carry):
            for wy in (2 * i, 2 * i + 1):
                rows = (xt[pl.ds(wy * 8, 8), core] if first else xo[pl.ds(wy * 8, 8)]).reshape(512, 256)
                part = dot_nn(rows, cols)
                for wz in range(2):
                    for wx in range(4):
                        for h, (wq, wp) in enumerate(((wy, wx), (wx, wy))):
                            base = (wz * 4 + wx) * 64
                            block = part[base : base + 64, h * HEAD : (h + 1) * HEAD]
                            if first:
                                wown[h, wq, wp, wz] = block
                            else:
                                wown[h, wq, wp, wz] = wown[h, wq, wp, wz] + block
            return carry

        lax.fori_loop(0, 2, body, 0)

    weight_blocks(True)
    arrived("dqc", dqr)
    for n in range(2):
        dqs[n] = (dqf[:, n, core] + dqr[:, n]).astype(BF16)
    for r, (dev, other) in enumerate(across):
        send("dqz", r, dqs.at[other], dq_out.at[zh], dev)
    arrived("xt", xo)
    arrived("d2", d2o)
    weight_blocks(False)
    def deliver(h, n, value):
        kind, ref, hop = (
            (3, b["w_far2"].at[h], p_far[h]),
            (1, b["w_near2"].at[h, 0], p_to[h][0]),
            (2, b["w_near2"].at[h, 1], p_to[h][1]),
            (0, b["wmine"].at[h], {}),
        )[n]
        ref[...] = value
        for r, (dev, other) in enumerate(across):
            send("ws", (kind, h, r), ref.at[other], w_out.at[kind, h, zh], {**hop, **dev})

    w_far, w_near, w_unit = reducer("w", lambda h, q, p, slot: wown[h, q, p], deliver)
    w_far()

    for n in range(4):
        w_near(n)
    for c in own_m:
        c.wait()
    for t in range(2):
        for r in range(2):
            src = matrix_part(t, r, core)
            arrived(("m", t, r), src)
            send("mc", (t, r), src, src, d_core)
    for n in range(4):
        w_unit(n)
    arrived("dz", dd.at[0])
    arrived("dy", dd.at[1, :, oh])
    arrived("mc", mat.at[1, 0])

    def tokens(which, t):
        return jnp.concatenate(
            [dd[which, t, a].reshape(128, HEAD) for a in range(2)], axis=1
        )

    token_grads = jnp.concatenate([tokens(w, t) for w in range(2) for t in range(2)], axis=1)

    def input_block(i, carry):
        rows = pl.ds(pl.multiple_of(i * 512, 512), 512)
        cols = jnp.concatenate([mat[w, t, rows, :] for w in range(2) for t in range(2)], axis=1)
        ig_out[:, lanes(i * 512, 512)] = dot_tt(token_grads, cols).astype(BF16)
        return carry

    lax.fori_loop(0, 4, input_block, 0)
    arrived("dqz", dq_out)
    arrived("ws", w_out)

    for group, kib in enumerate(filled):
        size_of = e_ref.at[0, pl.ds(0, kib), :]
        pltpu.make_async_copy(size_of, size_of, ssem.at[group]).wait()
    assert len(names) <= NSEM and len(local_names) <= NLOCAL


def finish(dq_in, ig_in, w_in, dq_out, ig_out, kw_out, vw_out, dq, kv_w, sems):
    whole = [
        pltpu.make_async_copy(ig_in, ig_out, sems.at[0]),
        pltpu.make_async_copy(dq, dq_out, sems.at[1]),
        pltpu.make_async_copy(kv_w.at[0], kw_out, sems.at[2]),
        pltpu.make_async_copy(kv_w.at[1], vw_out, sems.at[3]),
    ]
    whole[0].start()
    for kvh in range(2):
        for g in range(GROUP):
            at = (kvh * GROUP + g) * HEAD
            dq[:, :, at : at + HEAD] = dq_in[kvh, :, g]
    whole[1].start()
    for t in range(2):
        for n in range(2):
            parts = [w_in[kind, t, n].astype(F32) for kind in range(4)]
            kv_w[t, :, n * HEAD : (n + 1) * HEAD] = (parts[0] + parts[1]) + (parts[2] + parts[3])
        whole[2 + t].start()
    for c in whole:
        c.wait()


def local_step(q, k, v, g, x, mk, mv, placement):
    anywhere = pl.BlockSpec(memory_space=pl.ANY)
    vmem = pl.BlockSpec(memory_space=pltpu.VMEM)
    dq, ig, w = pl.pallas_call(
        kernel,
        out_shape=(
            pltpu.VMEM((2, CHUNKS, GROUP, 16, HEAD), BF16),
            pltpu.VMEM((128, FEATS // 2), BF16),
            pltpu.VMEM((4, 2, 2, 64, HEAD), BF16),
        ),
        in_specs=[anywhere] * 8,
        out_specs=(vmem,) * 3,
        scratch_shapes=[pltpu.VMEM(shape, dtype) for shape, dtype in BUFFERS.values()]
        + [
            pltpu.SemaphoreType.DMA((NSEND,)),
            pltpu.SemaphoreType.DMA((NSEM,)),
            pltpu.SemaphoreType.DMA((NLOCAL,)),
            pltpu.SemaphoreType.REGULAR,
        ],
        compiler_params=pltpu.CompilerParams(
            collective_id=0, has_side_effects=True, vmem_limit_bytes=65 * 1000 * 1000
        ),
    )(
        q.reshape(CHUNKS, 16, -1),
        g.reshape(CHUNKS, 16, -1),
        k.reshape(CHUNKS, 16, -1),
        v.reshape(CHUNKS, 16, -1),
        x.reshape(CHUNKS, 16, -1),
        mk,
        mv,
        placement,
    )
    query_grad, *rest = pl.pallas_call(
        finish,
        out_shape=(
            jax.ShapeDtypeStruct((CHUNKS, 16, 2 * GROUP * HEAD), BF16),
            jax.ShapeDtypeStruct((128, FEATS // 2), BF16),
            jax.ShapeDtypeStruct((64, 2 * HEAD), F32),
            jax.ShapeDtypeStruct((64, 2 * HEAD), F32),
        ),
        in_specs=[vmem] * 3,
        out_specs=(anywhere,) * 4,
        scratch_shapes=[
            pltpu.VMEM((CHUNKS, 16, 2 * GROUP * HEAD), BF16),
            pltpu.VMEM((2, 64, 2 * HEAD), F32),
            pltpu.SemaphoreType.DMA((4,)),
        ],
    )(*[pltpu.with_memory_space_constraint(a, pltpu.VMEM) for a in (dq, ig, w)])
    return (query_grad.reshape(128, -1), *rest)


def solution(mesh):
    torus = Mesh(
        mesh.devices.reshape(4, 2, 4, 2, mesh.shape["tp"]), ("seq_0", "seq_1", "seq_2", "seq_3", "tp")
    )
    rows = P(SEQ, "tp")
    return jax.shard_map(
        local_step,
        mesh=torus,
        in_specs=(rows, rows, rows, rows, rows, P(None, "tp"), P(None, "tp"), P()),
        out_specs=(rows, rows, rows, rows),
        check_vma=False,
    )
```

```python
import math

import jax
import jax.numpy as jnp
from jax import lax
from jax.experimental import pallas as pl
from jax.experimental.pallas import tpu as pltpu
from jax.sharding import Mesh
from jax.sharding import PartitionSpec as P

F32 = jnp.float32
BF16 = jnp.bfloat16
Y, ZH, X, CORE, ZL = "seq_0", "seq_1", "seq_2", "seq_3", "tp"
SEQ = (Y, ZH, X, CORE)
MESH = pl.DeviceIdType.MESH

HEAD = 128
GROUP = 4
WINDOW = 4096
CHUNKS = 8
BAND = 4
FEATS = 4096
SCALE = 1.0 / math.sqrt(HEAD)
SCALE2 = SCALE * math.log2(math.e)
MASKED = -1e30
QROWS = 256
KROWS = 128
NSEM = 71
NSEND = 5
NLOCAL = 9


def key_chunks(cq):
    return list(range(max(0, cq - BAND), cq + 1))


TILE_AT = [KROWS * sum(len(key_chunks(c)) for c in range(cq)) for cq in range(CHUNKS)]
TILE_ROWS = KROWS * sum(len(key_chunks(c)) for c in range(CHUNKS))

UNIT_KV = (2, 4, 2, 16, HEAD)
UNIT_W = (2, 64, HEAD)


def reduce_buffers(name, unit):
    half = unit[1:]
    return {
        name + "_far": ((2, 4) + unit, BF16),
        name + "_rfar": ((2, 2, 4) + half, BF16),
        name + "_near": ((2, 2, 4) + unit, BF16),
        name + "_rnear": ((2, 2, 4) + unit, BF16),
        name + "_far2": ((2,) + unit, BF16),
        name + "_rfar2": ((2,) + unit, BF16),
        name + "_near2": ((2, 2) + unit, BF16),
        name + "_rnear2": ((2, 2) + unit, BF16),
    }


BUFFERS = {
    "kv": ((2, 4, 4) + UNIT_KV, BF16),
    "qg": ((2, CHUNKS, 4, GROUP, 16, HEAD), BF16),
    "kpb": ((32, KROWS, 128), F32),
    "e": ((4, TILE_ROWS, QROWS), F32),
    "dp": ((4, TILE_ROWS, QROWS), F32),
    "st": ((3, 4, BAND + 1, CHUNKS, QROWS), F32),
    "ss": ((3, CHUNKS, QROWS), F32),
    "sr": ((3, CHUNKS, QROWS), F32),
    "fac": ((4, BAND + 1, CHUNKS, QROWS), F32),
    "delta": ((CHUNKS, QROWS), F32),
    "acc": ((2, 2, 4) + UNIT_KV, F32),
    "dqf": ((CHUNKS, 2, 2, GROUP, 16, HEAD), F32),
    "dqr": ((CHUNKS, 2, GROUP, 16, HEAD), F32),
    "dqs": ((2, CHUNKS, GROUP, 16, HEAD), BF16),
    "kt": ((4, CHUNKS, HEAD, KROWS), BF16),
    "qp": ((CHUNKS, QROWS), F32),
    "xg": ((CHUNKS, 2, 16, FEATS), BF16),
    "xt": ((32, 2, 64, 256), BF16),
    "xo": ((32, 64, 256), BF16),
    "kst": ((2, CHUNKS, 16, 2 * HEAD), BF16),
    "mat": ((2, 2, FEATS // 2, 2 * HEAD), BF16),
    "d2": ((2, CHUNKS, 2, 16, HEAD), BF16),
    "d2o": ((2, CHUNKS, 2, 16, HEAD), BF16),
    "dd": ((2, 2, 2, CHUNKS, 16, HEAD), BF16),
    "wown": ((2, 4, 4) + UNIT_W, F32),
    "wmine": ((2,) + UNIT_W, BF16),
    "rp": ((64, 64), jnp.int32),
    **reduce_buffers("a", UNIT_KV),
    **reduce_buffers("w", UNIT_W),
}


def dot_tt(a, b):
    return lax.dot_general(a, b, (((1,), (1,)), ((), ())), preferred_element_type=F32)


def dot_nn(a, b):
    return lax.dot_general(a, b, (((1,), (0,)), ((), ())), preferred_element_type=F32)


def dot_tn(a, b):
    return lax.dot_general(a, b, (((0,), (0,)), ((), ())), preferred_element_type=F32)


def stack_rows(parts):
    return parts[0] if len(parts) == 1 else jnp.concatenate(parts, axis=0)


def positions(rp_in, kpb, qp, y, x, core):
    slots = rp_in[...].astype(F32).astype(BF16)

    def iota(shape, dim):
        return lax.broadcasted_iota(jnp.int32, shape, dim)

    def bits(a, at, width):
        return jnp.bitwise_and(jnp.right_shift(a, at), (1 << width) - 1)

    row, dev = iota((KROWS, 64), 0), iota((KROWS, 64), 1)
    p, zh, jj = bits(row, 5, 2), bits(row, 4, 1), bits(row, 1, 3)
    wide = iota((KROWS, 128), 0)
    inside = (bits(wide, 1, 3) * 128 + bits(wide, 0, 1)).astype(F32)
    ones = jnp.ones((64, 128), BF16)
    owner = [
        [((q * 2 + zh) * 4 + p) * 2 + core == dev for q in range(4)],
        [((p * 2 + zh) * 4 + q) * 2 + core == dev for q in range(4)],
    ]
    for c in range(CHUNKS):
        block = (dev == jj + 8 * c).astype(F32).astype(BF16)
        rows = dot_nn(block, slots)
        for q in range(4):
            picked = jnp.where(owner[c // 4][q], rows, 0.0).astype(BF16)
            kpb[c // 4 * 16 + q * 4 + c % 4] = (
                dot_nn(picked, ones) * 2.0 + (inside + float(c * 1024))
            )

    dev, lane = iota((64, QROWS), 0), iota((64, QROWS), 1)
    zh, co, jj = bits(lane, 7, 1), bits(lane, 6, 1), bits(lane, 1, 3)
    pick = (((y * 2 + zh) * 4 + x) * 2 + co == dev).astype(F32).astype(BF16)
    slot = dot_nn(slots, pick)
    here = bits(dev, 0, 3) == jj
    pos = jnp.where(here, slot * 2.0 + (dev * 128 + bits(lane, 0, 1)).astype(F32), 0.0)
    qp[...] = jnp.sum(pos.reshape(CHUNKS, 8, QROWS), axis=1)


def kernel(
    q_in, g_in, k_in, v_in, x_in, mk_in, mv_in, rp_in, dq_out, ig_out, w_out, *scratch
):
    ssem, rsem, lsem, relay = scratch[-4:]
    b = dict(zip(BUFFERS, scratch[:-4]))
    y, zh, x, core, zl = (lax.axis_index(a) for a in (Y, ZH, X, CORE, ZL))

    def turn(i, by):
        return lax.rem(i + by, 4)

    z = 2 * zh + zl
    zp, zm = turn(z, 1), turn(z, 3)
    zp_h, zp_l = lax.div(zp, 2), lax.rem(zp, 2)
    zm_h, zm_l = lax.div(zm, 2), lax.rem(zm, 2)
    oh, oc, ol = 1 - zh, 1 - core, 1 - zl
    d_core, d_tp = {CORE: oc}, {ZL: ol}
    across = ((d_tp, zh), ({ZH: oh, ZL: ol}, oh))
    d_zp, d_zm = {ZH: zp_h, ZL: zp_l}, {ZH: zm_h, ZL: zm_l}
    step_of = {a: ({a: turn(i, 1)}, {a: turn(i, 3)}) for a, i in ((X, x), (Y, y))}
    far_of = {X: {X: turn(x, 2)}, Y: {Y: turn(y, 2)}}
    d_zh = {ZH: oh}
    qi, pi = (y, x), (x, y)
    q_to = (step_of[Y], step_of[X])
    p_to = (step_of[X], step_of[Y])
    p_far = (far_of[X], far_of[Y])

    names = {}
    sent = {}
    filled = [0] * NSEND

    def remote(name, src, dst, dev, group=0):
        i = names.setdefault(name, len(names))
        return pltpu.make_async_remote_copy(
            src_ref=src,
            dst_ref=dst,
            send_sem=ssem.at[group],
            recv_sem=rsem.at[i],
            device_id=dev,
            device_id_type=MESH,
        )

    def send(name, part, src, dst, dev):
        kib = math.prod(src.shape) * src.dtype.itemsize // 1024
        if (name, part) not in sent:
            group = min(range(NSEND), key=lambda n: filled[n])
            filled[group] += kib
            sent[name, part] = group
        remote(name, src, dst, dev, sent[name, part]).start()

    def arrived(name, size_of):
        remote(name, size_of, size_of, d_core).wait_recv()

    local_names = {}

    def local(name, src, dst):
        i = local_names.setdefault(name, len(local_names))
        return pltpu.make_async_copy(src, dst, lsem.at[i])

    def lanes(start, width=128):
        return pl.ds(pl.multiple_of(start, 128), width)

    kv, qg, xg, mat = b["kv"], b["qg"], b["xg"], b["mat"]
    own_x = local("x", x_in, xg.at[:, zh, :, lanes(zl * (FEATS // 2), FEATS // 2)])
    half_feats = FEATS // 2
    quarter_feats = FEATS // 4
    own_m = [
        local(("m", t), ref.at[pl.ds(pl.multiple_of(zl * half_feats, half_feats), half_feats), :], mat.at[0, t])
        for t, ref in enumerate((mk_in, mv_in))
    ]
    kst = b["kst"]
    stage = [local(("kst", t), ref, kst.at[t]) for t, ref in enumerate((k_in, v_in))]
    stage_rp = local("rp", rp_in, b["rp"])
    for c in stage + [stage_rp]:
        c.start()

    barrier = pltpu.get_barrier_semaphore()
    peers = [d_core, *step_of[X], *step_of[Y], d_zp, d_zm]
    for dev in peers:
        pl.semaphore_signal(barrier, inc=1, device_id=dev, device_id_type=MESH)
    pl.semaphore_wait(barrier, len(peers))
    for a in (X, Y):
        pl.semaphore_signal(relay, inc=1, device_id=step_of[a][0], device_id_type=MESH)

    for c in stage:
        c.wait()

    for h in range(2):
        for r, (dev, head) in enumerate(across):
            for t in range(2):
                send(
                    ("zkv", h),
                    (t, r),
                    kst.at[t, pl.ds(4 * h, 4), :, lanes(head * HEAD)],
                    kv.at[h, qi[h], pi[h], t, :, zh],
                    dev,
                )
    for t, ref in enumerate((q_in, g_in)):
        for r, (dev, head) in enumerate(across):
            for g in range(GROUP):
                send(
                    ("qz", t, r),
                    g,
                    ref.at[:, :, lanes(head * GROUP * HEAD + g * HEAD)],
                    qg.at[t, :, 2 * zh + core, g],
                    dev,
                )

    unit_offs = (0, 3, 1, 2)

    def unit_piece(h, n, side):
        unit = kv.at[h, qi[h], turn(pi[h], unit_offs[n])]
        return ("q", h, n), side, unit, unit, q_to[h][side]

    def send_unit(h, n):
        for side in range(2):
            send(*unit_piece(h, n, side))

    def near_piece(h, n, side):
        return kv.at[h, turn(qi[h], 3 if side == 0 else 1), turn(pi[h], unit_offs[n])]

    def forward_piece(h, n, side):
        src = near_piece(h, n, side).at[side]
        return ("qf", h, side), n, src, src, q_to[h][side]

    def forward_unit(h, n):
        arrived(("q", h, n), kv.at[h, 0, pl.ds(0, 2)])
        for side in range(2):
            send(*forward_piece(h, n, side))

    pl.semaphore_wait(relay, 2)
    for h in range(2):
        arrived(("zkv", h), kv.at[h, qi[h], pi[h]])
        unit = kv.at[h, qi[h], pi[h]]
        for side in range(2):
            send(("p", h, side), 0, unit, unit, p_to[h][side])
    for h in range(2):
        unit = kv.at[h, qi[h], pi[h]]
        send(("pf", h), 0, unit, unit, p_far[h])

    for h in range(2):
        send_unit(h, 0)

    own_x.start()
    for c in own_m:
        c.start()
    b["st"][0] = jnp.full(b["st"].shape[1:], MASKED, F32)
    b["st"][1:] = jnp.zeros((2,) + b["st"].shape[1:], F32)
    stage_rp.wait()
    positions(b["rp"], b["kpb"], b["qp"], y, x, core)
    for h in range(2):
        for side in range(2):
            src = kv.at[h, qi[h], turn(pi[h], 3 if side == 0 else 1)]
            arrived(("p", h, side), src)
        for side in range(2):
            send_unit(h, 1 + side)
    for t in range(2):
        for r, (dev, head) in enumerate(across):
            src = qg.at[t, :, 2 * head + core]
            arrived(("qz", t, r), src)
            send(("qc", t), r, src, src, d_core)

    def send_matrix(t):
        ref = (mk_in, mv_in)[t]
        for r, (dev, _) in enumerate(across):
            at = (2 * r + core) * 512
            src = ref.at[pl.ds(pl.multiple_of(ol * half_feats + at, 512), 512), :]
            dst = mat.at[1, t, pl.ds(pl.multiple_of(at, 512), 512), :]
            yield ("m", t, r), 0, src, dst, dev

    def matrix_part(t, r, which):
        return mat.at[1, t, pl.ds(pl.multiple_of((2 * r + which) * 512, 512), 512), :]

    ring = (
        ("x+", d_zp, zm_h, zm_l, 0),
        ("x-", d_zm, zp_h, zp_l, quarter_feats),
    )
    for second in range(2):
        for name, dev, _, _, first in ring:
            at = quarter_feats - first if second else first
            send(
                (name, second),
                0,
                x_in.at[:, :, pl.ds(at, quarter_feats)],
                xg.at[:, zh, :, lanes(zl * half_feats + at, quarter_feats)],
                dev,
            )

    def ring_part(src_h, src_l, at):
        return xg.at[:, src_h, :, lanes(src_l * half_feats + at, quarter_feats)]

    def forward_input():
        for name, dev, src_h, src_l, first in ring:
            src = ring_part(src_h, src_l, first)
            arrived((name, 0), src)
            send((name, 2), 0, src, src, dev)

    def wait_input():
        own_x.wait()
        for name, _, src_h, src_l, first in ring:
            arrived((name, 1), ring_part(src_h, src_l, quarter_feats - first))
            arrived((name, 2), ring_part(oh, zl, first))

    for h in range(2):
        arrived(("pf", h), kv.at[h, qi[h], turn(pi[h], 2)])
        send_unit(h, 3)
    for t in range(2):
        arrived(("qc", t), qg.at[t, pl.ds(0, CHUNKS // 2)])

    def tile_rows(cq, ck):
        return pl.ds(TILE_AT[cq] + (ck - key_chunks(cq)[0]) * KROWS, KROWS)

    def queries(t, cq):
        return qg[t, cq].reshape(QROWS, HEAD)

    def keys(t, at, cks):
        return stack_rows(
            [kv[ck // 4, at[ck // 4], :, t, ck % 4].reshape(KROWS, HEAD) for ck in cks]
        )

    st, e_ref, dp_ref = b["st"], b["e"], b["dp"]

    def first_pass(s, carry):
        late = lax.div(s, 2)
        off = (1 - late) * s + late * (5 - s)

        @pl.when(s == 1)
        def _():
            for n in range(4):
                for h in range(2):
                    forward_unit(h, n)

        @pl.when(s == 3)
        def _():
            for h in range(2):
                for side in range(2):
                    arrived(("qf", h, side), kv.at[h, turn(qi[h], 2), :, side])
            forward_input()
            for t in range(2):
                for copy in send_matrix(t):
                    send(*copy)

        at = (turn(y, off), turn(x, off))
        for cq in range(CHUNKS):
            cks = key_chunks(cq)
            scores = dot_tt(keys(0, at, cks), queries(0, cq))
            dprobs = dot_tt(keys(1, at, cks), queries(1, cq))
            qpos = b["qp"][cq : cq + 1, :]
            for n, ck in enumerate(cks):
                part = slice(n * KROWS, (n + 1) * KROWS)
                score, dprob = scores[part] * SCALE2, dprobs[part]
                if ck == cq or ck == cq - BAND:
                    kpb = b["kpb"][ck // 4 * 16 + at[ck // 4] * 4 + ck % 4]
                    kpos = jnp.concatenate([kpb, kpb], axis=1)
                    seen = kpos <= qpos if ck == cq else kpos > qpos - WINDOW
                    score = jnp.where(seen, score, MASKED)
                top = jnp.max(score, axis=0, keepdims=True)
                expo = jnp.exp2(score - top)
                rows = tile_rows(cq, ck)
                e_ref[off, rows, :] = expo
                dp_ref[off, rows, :] = dprob
                row = slice(cq, cq + 1)
                st[0, off, cq - ck, row, :] = top
                st[1, off, cq - ck, row, :] = jnp.sum(expo, axis=0, keepdims=True)
                st[2, off, cq - ck, row, :] = jnp.sum(expo * dprob, axis=0, keepdims=True)
        return carry

    lax.fori_loop(0, 4, first_pass, 0)
    ss, sr = b["ss"], b["sr"]
    top_l = jnp.max(st[0], axis=(0, 1))
    fac_l = jnp.exp2(st[0] - top_l[None, None])
    sum_l = jnp.sum(st[1] * fac_l, axis=(0, 1))
    wgt_l = jnp.sum(st[2] * fac_l, axis=(0, 1))
    ss[0] = top_l
    ss[1] = sum_l
    ss[2] = wgt_l
    send("stat", 0, ss, sr, d_core)

    arrived("stat", sr)
    top = jnp.maximum(top_l, sr[0])
    mine_f = jnp.exp2(top_l - top)
    other_f = jnp.exp2(sr[0] - top)
    total = sum_l * mine_f + sr[1] * other_f
    b["delta"][...] = (wgt_l * mine_f + sr[2] * other_f) / total
    b["fac"][...] = fac_l * (mine_f / total)[None, None]

    offs = (2, 1, 3, 0)

    def reducer(name, unit_at, deliver=None):
        far, rfar = b[name + "_far"], b[name + "_rfar"]
        near, rnear = b[name + "_near"], b[name + "_rnear"]
        far2, rfar2 = b[name + "_far2"], b[name + "_rfar2"]
        near2, rnear2 = b[name + "_near2"], b[name + "_rnear2"]

        def place(h, n):
            return turn(pi[h], offs[n])

        def far_copy(h, n, side):
            p = place(h, n)
            return (
                (name, "far", n, side),
                h,
                far.at[h, p, side],
                rfar.at[h, side, p],
                q_to[h][side],
            )

        def near_copy(h, n, side):
            p = place(h, n)
            return (
                (name, "near", n),
                (h, side),
                near.at[h, side, p],
                rnear.at[h, side, p],
                q_to[h][side],
            )

        def start_far():
            for n in range(4):
                for h in range(2):
                    p = place(h, n)
                    far[h, p] = unit_at(h, turn(qi[h], 2), p, 0).astype(BF16)
                    for side in range(2):
                        send(*far_copy(h, n, side))

        def start_near(n):
            for side in (1, 0):
                arrived((name, "far", n, side), rfar.at[0, side, pl.ds(0, 2)])
                for h in range(2):
                    p = place(h, n)
                    value = unit_at(h, turn(qi[h], 1 if side == 0 else 3), p, 1 - side)
                    near[h, side, p, 1 - side] = value[1 - side].astype(BF16)
                    near[h, side, p, side] = (value[side] + rfar[h, side, p].astype(F32)).astype(
                        BF16
                    )
                    send(*near_copy(h, n, side))

        def own_unit(n):
            out = []
            arrived((name, "near", n), rnear.at[0, 0])
            for h in range(2):
                p = place(h, n)
                value = (
                    unit_at(h, qi[h], p, 0)
                    + rnear[h, 0, p].astype(F32)
                    + rnear[h, 1, p].astype(F32)
                )
                if deliver:
                    deliver(h, n, value.astype(BF16))
                elif n == 0:
                    far2[h] = value.astype(BF16)
                    send((name, "p", h), 2, far2.at[h], rfar2.at[h], p_far[h])
                elif n < 3:
                    side = n - 1
                    near2[h, side] = value.astype(BF16)
                    send(
                        (name, "p", h),
                        side,
                        near2.at[h, side],
                        rnear2.at[h, side],
                        p_to[h][side],
                    )
                else:
                    arrived((name, "p", h), rnear.at[0, 0, pl.ds(0, 3)])
                    out.append(
                        (value + rfar2[h].astype(F32))
                        + (rnear2[h, 0].astype(F32) + rnear2[h, 1].astype(F32))
                    )
            return out

        return start_far, start_near, own_unit

    acc = b["acc"]
    start_far, start_near, own_unit = reducer(
        "a", lambda h, q, p, slot: acc[slot, h, p]
    )

    fac, delta, kt = b["fac"], b["delta"], b["kt"]

    def second_pass(s, carry):
        late = lax.div(s, 2)
        off = (1 - late) * (2 + s) + late * (3 - s)
        slot = late * (3 - s)
        for ck in range(CHUNKS):
            probs, dscores = [], []
            cqs = [cq for cq in range(CHUNKS) if ck in key_chunks(cq)]
            for cq in cqs:
                rows = tile_rows(cq, ck)
                prob = e_ref[off, rows, :] * fac[off, cq - ck, cq : cq + 1, :]
                dscore = prob * (dp_ref[off, rows, :] - delta[cq : cq + 1, :])
                e_ref[off, rows, :] = dscore
                probs.append(prob.astype(BF16))
                dscores.append(dscore.astype(BF16))
            for t, parts in enumerate((dscores, probs)):
                depth = qg[t, ck : ck + len(cqs)].reshape(len(cqs) * QROWS, HEAD)
                grad = dot_nn(jnp.concatenate(parts, axis=1), depth)
                acc[slot, ck // 4, :, t, ck % 4] = grad.reshape(4, 2, 16, HEAD)

        @pl.when(s == 0)
        def _():
            start_far()

        @pl.when(s == 2)
        def _():
            for n in range(4):
                start_near(n)

        return carry

    lax.fori_loop(0, 4, second_pass, 0)
    dqf, dqr, dqs = b["dqf"], b["dqr"], b["dqs"]
    own_unit(0)
    wait_input()
    xt, xo = b["xt"], b["xo"]

    def flip_input(i, carry):
        for n in range(4):
            at = i * 4 + n
            block = xg[:, :, :, lanes(at * 128)].reshape(256, 128)
            xt[at] = block.T.reshape(2, 64, 256)
        return carry

    lax.fori_loop(0, 8, flip_input, 0)
    send("xt", 0, xt.at[:, oc], xo, d_core)
    own_unit(1)
    own_unit(2)
    for off in range(4):
        at = (turn(y, off), turn(x, off))
        for ck in range(CHUNKS):
            kt[off, ck] = keys(0, at, [ck]).T
    for cq in range(CHUNKS):
        cks = key_chunks(cq)
        rows = pl.ds(TILE_AT[cq], KROWS * len(cks))
        flipped = jnp.concatenate([kt[off, ck] for off in range(4) for ck in cks], axis=1)
        dscore = jnp.concatenate([e_ref[off, rows, :].astype(BF16) for off in range(4)], axis=0)
        dqf[cq] = (dot_nn(flipped, dscore).T * SCALE).reshape(2, 2, GROUP, 16, HEAD)
    send("dqc", 0, dqf.at[:, :, oc], dqr, d_core)
    d2, d2o, dd = b["d2"], b["d2o"], b["dd"]
    for h, value in enumerate(own_unit(3)):
        d2[0, 4 * h : 4 * h + 4] = (value[0] * SCALE).astype(BF16)
        d2[1, 4 * h : 4 * h + 4] = value[1].astype(BF16)
    send("d2", 0, d2, d2o, d_core)
    for r, (dev, other) in enumerate(across):
        for t in range(2):
            send("dz", (t, r), d2.at[t, :, other], dd.at[0, t, zh], dev)
    for t in range(2):
        send("dy", t, d2.at[t, :, oh], dd.at[1, t, zh], d_zh)
        dd[1, t, zh] = d2[t, :, zh]

    wown = b["wown"]

    def grad_cols(ref):
        return jnp.concatenate([ref[0].reshape(256, HEAD), ref[1].reshape(256, HEAD)], axis=1)

    def weight_blocks(first):
        cols = grad_cols(d2 if first else d2o)

        def body(i, carry):
            for wy in (2 * i, 2 * i + 1):
                rows = (xt[pl.ds(wy * 8, 8), core] if first else xo[pl.ds(wy * 8, 8)]).reshape(512, 256)
                part = dot_nn(rows, cols)
                for wz in range(2):
                    for wx in range(4):
                        for h, (wq, wp) in enumerate(((wy, wx), (wx, wy))):
                            base = (wz * 4 + wx) * 64
                            block = part[base : base + 64, h * HEAD : (h + 1) * HEAD]
                            if first:
                                wown[h, wq, wp, wz] = block
                            else:
                                wown[h, wq, wp, wz] = wown[h, wq, wp, wz] + block
            return carry

        lax.fori_loop(0, 2, body, 0)

    def far_blocks(first):
        cols = d2 if first else d2o
        fy, fx = turn(y, 2), turn(x, 2)

        def block(i, count):
            return xt[pl.ds(i, count), core] if first else xo[pl.ds(i, count)]

        rows = (
            block(fy * 8, 8).reshape(512, 256),
            jnp.concatenate([block(n * 4 + fx, 1).reshape(64, 256) for n in range(8)], axis=0),
        )
        for h in range(2):
            part = dot_nn(rows[h], cols[h].reshape(256, HEAD))
            for n in range(8):
                piece = part[n * 64 : (n + 1) * 64]
                at = (0, fy, n % 4, n // 4) if h == 0 else (1, fx, n // 2, n % 2)
                wown[at] = piece if first else wown[at] + piece

    far_blocks(True)
    arrived("xt", xo)
    arrived("d2", d2o)
    far_blocks(False)
    def deliver(h, n, value):
        kind, ref, hop = (
            (3, b["w_far2"].at[h], p_far[h]),
            (1, b["w_near2"].at[h, 0], p_to[h][0]),
            (2, b["w_near2"].at[h, 1], p_to[h][1]),
            (0, b["wmine"].at[h], {}),
        )[n]
        ref[...] = value
        for r, (dev, other) in enumerate(across):
            send("ws", (kind, h, r), ref.at[other], w_out.at[kind, h, zh], {**hop, **dev})

    w_far, w_near, w_unit = reducer("w", lambda h, q, p, slot: wown[h, q, p], deliver)
    w_far()
    weight_blocks(True)
    arrived("dqc", dqr)
    for n in range(2):
        dqs[n] = (dqf[:, n, core] + dqr[:, n]).astype(BF16)
    for r, (dev, other) in enumerate(across):
        send("dqz", r, dqs.at[other], dq_out.at[zh], dev)
    weight_blocks(False)

    for n in range(4):
        w_near(n)
    for c in own_m:
        c.wait()
    for t in range(2):
        for r in range(2):
            src = matrix_part(t, r, core)
            arrived(("m", t, r), src)
            send("mc", (t, r), src, src, d_core)
    for n in range(4):
        w_unit(n)
    arrived("dz", dd.at[0])
    arrived("dy", dd.at[1, :, oh])
    arrived("mc", mat.at[1, 0])

    def tokens(which, t):
        return jnp.concatenate(
            [dd[which, t, a].reshape(128, HEAD) for a in range(2)], axis=1
        )

    token_grads = jnp.concatenate([tokens(w, t) for w in range(2) for t in range(2)], axis=1)

    def input_block(i, carry):
        rows = pl.ds(pl.multiple_of(i * 512, 512), 512)
        cols = jnp.concatenate([mat[w, t, rows, :] for w in range(2) for t in range(2)], axis=1)
        ig_out[:, lanes(i * 512, 512)] = dot_tt(token_grads, cols).astype(BF16)
        return carry

    lax.fori_loop(0, 4, input_block, 0)
    arrived("dqz", dq_out)
    arrived("ws", w_out)

    for group, kib in enumerate(filled):
        size_of = e_ref.at[0, pl.ds(0, kib), :]
        pltpu.make_async_copy(size_of, size_of, ssem.at[group]).wait()
    assert len(names) <= NSEM and len(local_names) <= NLOCAL


def finish(dq_in, ig_in, w_in, dq_out, ig_out, kw_out, vw_out, dq, kv_w, sems):
    whole = [
        pltpu.make_async_copy(ig_in, ig_out, sems.at[0]),
        pltpu.make_async_copy(dq, dq_out, sems.at[1]),
        pltpu.make_async_copy(kv_w.at[0], kw_out, sems.at[2]),
        pltpu.make_async_copy(kv_w.at[1], vw_out, sems.at[3]),
    ]
    whole[0].start()
    for kvh in range(2):
        for g in range(GROUP):
            at = (kvh * GROUP + g) * HEAD
            dq[:, :, at : at + HEAD] = dq_in[kvh, :, g]
    whole[1].start()
    for t in range(2):
        for n in range(2):
            parts = [w_in[kind, t, n].astype(F32) for kind in range(4)]
            kv_w[t, :, n * HEAD : (n + 1) * HEAD] = (parts[0] + parts[1]) + (parts[2] + parts[3])
        whole[2 + t].start()
    for c in whole:
        c.wait()


def local_step(q, k, v, g, x, mk, mv, placement):
    anywhere = pl.BlockSpec(memory_space=pl.ANY)
    vmem = pl.BlockSpec(memory_space=pltpu.VMEM)
    dq, ig, w = pl.pallas_call(
        kernel,
        out_shape=(
            pltpu.VMEM((2, CHUNKS, GROUP, 16, HEAD), BF16),
            pltpu.VMEM((128, FEATS // 2), BF16),
            pltpu.VMEM((4, 2, 2, 64, HEAD), BF16),
        ),
        in_specs=[anywhere] * 8,
        out_specs=(vmem,) * 3,
        scratch_shapes=[pltpu.VMEM(shape, dtype) for shape, dtype in BUFFERS.values()]
        + [
            pltpu.SemaphoreType.DMA((NSEND,)),
            pltpu.SemaphoreType.DMA((NSEM,)),
            pltpu.SemaphoreType.DMA((NLOCAL,)),
            pltpu.SemaphoreType.REGULAR,
        ],
        compiler_params=pltpu.CompilerParams(
            collective_id=0, has_side_effects=True, vmem_limit_bytes=65 * 1000 * 1000
        ),
    )(
        q.reshape(CHUNKS, 16, -1),
        g.reshape(CHUNKS, 16, -1),
        k.reshape(CHUNKS, 16, -1),
        v.reshape(CHUNKS, 16, -1),
        x.reshape(CHUNKS, 16, -1),
        mk,
        mv,
        placement,
    )
    query_grad, *rest = pl.pallas_call(
        finish,
        out_shape=(
            jax.ShapeDtypeStruct((CHUNKS, 16, 2 * GROUP * HEAD), BF16),
            jax.ShapeDtypeStruct((128, FEATS // 2), BF16),
            jax.ShapeDtypeStruct((64, 2 * HEAD), F32),
            jax.ShapeDtypeStruct((64, 2 * HEAD), F32),
        ),
        in_specs=[vmem] * 3,
        out_specs=(anywhere,) * 4,
        scratch_shapes=[
            pltpu.VMEM((CHUNKS, 16, 2 * GROUP * HEAD), BF16),
            pltpu.VMEM((2, 64, 2 * HEAD), F32),
            pltpu.SemaphoreType.DMA((4,)),
        ],
    )(*[pltpu.with_memory_space_constraint(a, pltpu.VMEM) for a in (dq, ig, w)])
    return (query_grad.reshape(128, -1), *rest)


def solution(mesh):
    torus = Mesh(
        mesh.devices.reshape(4, 2, 4, 2, mesh.shape["tp"]), ("seq_0", "seq_1", "seq_2", "seq_3", "tp")
    )
    rows = P(SEQ, "tp")
    return jax.shard_map(
        local_step,
        mesh=torus,
        in_specs=(rows, rows, rows, rows, rows, P(None, "tp"), P(None, "tp"), P()),
        out_specs=(rows, rows, rows, rows),
        check_vma=False,
    )
```

```python
import math

import jax
import jax.numpy as jnp
from jax import lax
from jax.experimental import pallas as pl
from jax.experimental.pallas import tpu as pltpu
from jax.sharding import Mesh
from jax.sharding import PartitionSpec as P

F32 = jnp.float32
BF16 = jnp.bfloat16
Y, ZH, X, CORE, ZL = "seq_0", "seq_1", "seq_2", "seq_3", "tp"
SEQ = (Y, ZH, X, CORE)
MESH = pl.DeviceIdType.MESH

HEAD = 128
GROUP = 4
WINDOW = 4096
CHUNKS = 8
BAND = 4
FEATS = 4096
SCALE = 1.0 / math.sqrt(HEAD)
SCALE2 = SCALE * math.log2(math.e)
MASKED = -1e30
QROWS = 256
KROWS = 128
NSEM = 64
NSEND = 5
NLOCAL = 9


def key_chunks(cq):
    return list(range(max(0, cq - BAND), cq + 1))


TILE_AT = [KROWS * sum(len(key_chunks(c)) for c in range(cq)) for cq in range(CHUNKS)]
TILE_ROWS = KROWS * sum(len(key_chunks(c)) for c in range(CHUNKS))

UNIT_KV = (2, 4, 2, 16, HEAD)
UNIT_W = (2, 64, HEAD)


def reduce_buffers(name, unit):
    half = unit[1:]
    return {
        name + "_far": ((2, 4) + unit, BF16),
        name + "_rfar": ((2, 2, 4) + half, BF16),
        name + "_near": ((2, 2, 4) + unit, BF16),
        name + "_rnear": ((2, 2, 4) + unit, BF16),
        name + "_far2": ((2,) + unit, BF16),
        name + "_rfar2": ((2,) + unit, BF16),
        name + "_near2": ((2, 2) + unit, BF16),
        name + "_rnear2": ((2, 2) + unit, BF16),
    }


BUFFERS = {
    "kv": ((2, 4, 4) + UNIT_KV, BF16),
    "qg": ((2, CHUNKS, 4, GROUP, 16, HEAD), BF16),
    "kpb": ((32, KROWS, 128), F32),
    "e": ((4, TILE_ROWS, QROWS), F32),
    "dp": ((4, TILE_ROWS, QROWS), F32),
    "st": ((3, 4, BAND + 1, CHUNKS, QROWS), F32),
    "ss": ((3, CHUNKS, QROWS), F32),
    "sr": ((3, CHUNKS, QROWS), F32),
    "fac": ((4, BAND + 1, CHUNKS, QROWS), F32),
    "delta": ((CHUNKS, QROWS), F32),
    "acc": ((2, 2, 4) + UNIT_KV, F32),
    "dqf": ((CHUNKS, 2, 2, GROUP, 16, HEAD), F32),
    "dqr": ((CHUNKS, 2, GROUP, 16, HEAD), F32),
    "dqs": ((2, CHUNKS, GROUP, 16, HEAD), BF16),
    "kt": ((4, CHUNKS, HEAD, KROWS), BF16),
    "qp": ((CHUNKS, QROWS), F32),
    "xg": ((CHUNKS, 2, 16, FEATS), BF16),
    "xt": ((32, 2, 64, 256), BF16),
    "xo": ((32, 64, 256), BF16),
    "kst": ((2, CHUNKS, 16, 2 * HEAD), BF16),
    "mat": ((2, 2, FEATS // 2, 2 * HEAD), BF16),
    "d2": ((2, CHUNKS, 2, 16, HEAD), BF16),
    "d2o": ((2, CHUNKS, 2, 16, HEAD), BF16),
    "dd": ((2, 2, 2, CHUNKS, 16, HEAD), BF16),
    "wown": ((2, 4, 4) + UNIT_W, F32),
    "wmine": ((2,) + UNIT_W, BF16),
    "rp": ((64, 64), jnp.int32),
    **reduce_buffers("a", UNIT_KV),
    **reduce_buffers("w", UNIT_W),
}


def dot_tt(a, b):
    return lax.dot_general(a, b, (((1,), (1,)), ((), ())), preferred_element_type=F32)


def dot_nn(a, b):
    return lax.dot_general(a, b, (((1,), (0,)), ((), ())), preferred_element_type=F32)


def dot_tn(a, b):
    return lax.dot_general(a, b, (((0,), (0,)), ((), ())), preferred_element_type=F32)


def stack_rows(parts):
    return parts[0] if len(parts) == 1 else jnp.concatenate(parts, axis=0)


def positions(rp_in, kpb, qp, y, x, core):
    slots = rp_in[...].astype(F32).astype(BF16)

    def iota(shape, dim):
        return lax.broadcasted_iota(jnp.int32, shape, dim)

    def bits(a, at, width):
        return jnp.bitwise_and(jnp.right_shift(a, at), (1 << width) - 1)

    row, dev = iota((KROWS, 64), 0), iota((KROWS, 64), 1)
    p, zh, jj = bits(row, 5, 2), bits(row, 4, 1), bits(row, 1, 3)
    wide = iota((KROWS, 128), 0)
    inside = (bits(wide, 1, 3) * 128 + bits(wide, 0, 1)).astype(F32)
    ones = jnp.ones((64, 128), BF16)
    owner = [
        [((q * 2 + zh) * 4 + p) * 2 + core == dev for q in range(4)],
        [((p * 2 + zh) * 4 + q) * 2 + core == dev for q in range(4)],
    ]
    for c in range(CHUNKS):
        block = (dev == jj + 8 * c).astype(F32).astype(BF16)
        rows = dot_nn(block, slots)
        for q in range(4):
            picked = jnp.where(owner[c // 4][q], rows, 0.0).astype(BF16)
            kpb[c // 4 * 16 + q * 4 + c % 4] = (
                dot_nn(picked, ones) * 2.0 + (inside + float(c * 1024))
            )

    dev, lane = iota((64, QROWS), 0), iota((64, QROWS), 1)
    zh, co, jj = bits(lane, 7, 1), bits(lane, 6, 1), bits(lane, 1, 3)
    pick = (((y * 2 + zh) * 4 + x) * 2 + co == dev).astype(F32).astype(BF16)
    slot = dot_nn(slots, pick)
    here = bits(dev, 0, 3) == jj
    pos = jnp.where(here, slot * 2.0 + (dev * 128 + bits(lane, 0, 1)).astype(F32), 0.0)
    qp[...] = jnp.sum(pos.reshape(CHUNKS, 8, QROWS), axis=1)


def kernel(
    q_in, g_in, k_in, v_in, x_in, mk_in, mv_in, rp_in, dq_out, ig_out, w_out, *scratch
):
    ssem, rsem, lsem, relay = scratch[-4:]
    b = dict(zip(BUFFERS, scratch[:-4]))
    y, zh, x, core, zl = (lax.axis_index(a) for a in (Y, ZH, X, CORE, ZL))

    def turn(i, by):
        return lax.rem(i + by, 4)

    z = 2 * zh + zl
    zp, zm = turn(z, 1), turn(z, 3)
    zp_h, zp_l = lax.div(zp, 2), lax.rem(zp, 2)
    zm_h, zm_l = lax.div(zm, 2), lax.rem(zm, 2)
    oh, oc, ol = 1 - zh, 1 - core, 1 - zl
    d_core, d_tp = {CORE: oc}, {ZL: ol}
    across = ((d_tp, zh), ({ZH: oh, ZL: ol}, oh))
    d_zp, d_zm = {ZH: zp_h, ZL: zp_l}, {ZH: zm_h, ZL: zm_l}
    step_of = {a: ({a: turn(i, 1)}, {a: turn(i, 3)}) for a, i in ((X, x), (Y, y))}
    far_of = {X: {X: turn(x, 2)}, Y: {Y: turn(y, 2)}}
    d_zh = {ZH: oh}
    qi, pi = (y, x), (x, y)
    q_to = (step_of[Y], step_of[X])
    p_to = (step_of[X], step_of[Y])
    p_far = (far_of[X], far_of[Y])

    names = {}
    sent = {}
    filled = [0] * NSEND

    def remote(name, src, dst, dev, group=0):
        i = names.setdefault(name, len(names))
        return pltpu.make_async_remote_copy(
            src_ref=src,
            dst_ref=dst,
            send_sem=ssem.at[group],
            recv_sem=rsem.at[i],
            device_id=dev,
            device_id_type=MESH,
        )

    def send(name, part, src, dst, dev):
        kib = math.prod(src.shape) * src.dtype.itemsize // 1024
        if (name, part) not in sent:
            group = min(range(NSEND), key=lambda n: filled[n])
            filled[group] += kib
            sent[name, part] = group
        remote(name, src, dst, dev, sent[name, part]).start()

    def arrived(name, size_of):
        remote(name, size_of, size_of, d_core).wait_recv()

    local_names = {}

    def local(name, src, dst):
        i = local_names.setdefault(name, len(local_names))
        return pltpu.make_async_copy(src, dst, lsem.at[i])

    def lanes(start, width=128):
        return pl.ds(pl.multiple_of(start, 128), width)

    kv, qg, xg, mat = b["kv"], b["qg"], b["xg"], b["mat"]
    own_x = local("x", x_in, xg.at[:, zh, :, lanes(zl * (FEATS // 2), FEATS // 2)])
    half_feats = FEATS // 2
    quarter_feats = FEATS // 4
    own_m = [
        local(("m", t), ref.at[pl.ds(pl.multiple_of(zl * half_feats, half_feats), half_feats), :], mat.at[0, t])
        for t, ref in enumerate((mk_in, mv_in))
    ]
    kst = b["kst"]
    stage = [local(("kst", t), ref, kst.at[t]) for t, ref in enumerate((k_in, v_in))]
    stage_rp = local("rp", rp_in, b["rp"])
    for c in stage + [stage_rp]:
        c.start()

    barrier = pltpu.get_barrier_semaphore()
    peers = [d_core, *step_of[X], *step_of[Y], d_zp, d_zm]
    for dev in peers:
        pl.semaphore_signal(barrier, inc=1, device_id=dev, device_id_type=MESH)
    pl.semaphore_wait(barrier, len(peers))
    for a in (X, Y):
        pl.semaphore_signal(relay, inc=1, device_id=step_of[a][0], device_id_type=MESH)

    for c in stage:
        c.wait()

    for h in range(2):
        for r, (dev, head) in enumerate(across):
            for t in range(2):
                send(
                    ("zkv", h),
                    (t, r),
                    kst.at[t, pl.ds(4 * h, 4), :, lanes(head * HEAD)],
                    kv.at[h, qi[h], pi[h], t, :, zh],
                    dev,
                )
    for t, ref in enumerate((q_in, g_in)):
        for r, (dev, head) in enumerate(across):
            for g in range(GROUP):
                send(
                    ("qz", t, r),
                    g,
                    ref.at[:, :, lanes(head * GROUP * HEAD + g * HEAD)],
                    qg.at[t, :, 2 * zh + core, g],
                    dev,
                )

    unit_offs = (0, 3, 1, 2)

    def unit_piece(h, n, side):
        unit = kv.at[h, qi[h], turn(pi[h], unit_offs[n])]
        return ("q", h, n), side, unit, unit, q_to[h][side]

    def send_unit(h, n):
        for side in range(2):
            send(*unit_piece(h, n, side))

    def near_piece(h, n, side):
        return kv.at[h, turn(qi[h], 3 if side == 0 else 1), turn(pi[h], unit_offs[n])]

    def forward_piece(h, n, side):
        src = near_piece(h, n, side).at[side]
        return "qf", (h, n, side), src, src, q_to[h][side]

    def forward_unit(h, n):
        arrived(("q", h, n), kv.at[h, 0, pl.ds(0, 2)])
        for side in range(2):
            send(*forward_piece(h, n, side))

    pl.semaphore_wait(relay, 2)
    for h in range(2):
        arrived(("zkv", h), kv.at[h, qi[h], pi[h]])
        unit = kv.at[h, qi[h], pi[h]]
        for side in range(2):
            send(("p", h, side), 0, unit, unit, p_to[h][side])
    for h in range(2):
        unit = kv.at[h, qi[h], pi[h]]
        send(("pf", h), 0, unit, unit, p_far[h])

    for h in range(2):
        send_unit(h, 0)

    own_x.start()
    for c in own_m:
        c.start()
    b["st"][0] = jnp.full(b["st"].shape[1:], MASKED, F32)
    b["st"][1:] = jnp.zeros((2,) + b["st"].shape[1:], F32)
    stage_rp.wait()
    positions(b["rp"], b["kpb"], b["qp"], y, x, core)
    for h in range(2):
        for side in range(2):
            src = kv.at[h, qi[h], turn(pi[h], 3 if side == 0 else 1)]
            arrived(("p", h, side), src)
        for side in range(2):
            send_unit(h, 1 + side)
    for t in range(2):
        for r, (dev, head) in enumerate(across):
            src = qg.at[t, :, 2 * head + core]
            arrived(("qz", t, r), src)
            send("qc", (t, r), src, src, d_core)

    def send_matrix(t):
        ref = (mk_in, mv_in)[t]
        for r, (dev, _) in enumerate(across):
            at = (2 * r + core) * 512
            src = ref.at[pl.ds(pl.multiple_of(ol * half_feats + at, 512), 512), :]
            dst = mat.at[1, t, pl.ds(pl.multiple_of(at, 512), 512), :]
            yield "m", (t, r), src, dst, dev

    def matrix_part(t, r, which):
        return mat.at[1, t, pl.ds(pl.multiple_of((2 * r + which) * 512, 512), 512), :]

    ring = (
        ("x+", d_zp, zm_h, zm_l, 0),
        ("x-", d_zm, zp_h, zp_l, quarter_feats),
    )
    for second in range(2):
        for name, dev, _, _, first in ring:
            at = quarter_feats - first if second else first
            send(
                (name, second),
                0,
                x_in.at[:, :, pl.ds(at, quarter_feats)],
                xg.at[:, zh, :, lanes(zl * half_feats + at, quarter_feats)],
                dev,
            )

    def ring_part(src_h, src_l, at):
        return xg.at[:, src_h, :, lanes(src_l * half_feats + at, quarter_feats)]

    def forward_input():
        for name, dev, src_h, src_l, first in ring:
            src = ring_part(src_h, src_l, first)
            arrived((name, 0), src)
            send((name, 2), 0, src, src, dev)

    def wait_input():
        own_x.wait()
        for name, _, src_h, src_l, first in ring:
            arrived((name, 1), ring_part(src_h, src_l, quarter_feats - first))
            arrived((name, 2), ring_part(oh, zl, first))

    for h in range(2):
        arrived(("pf", h), kv.at[h, qi[h], turn(pi[h], 2)])
        send_unit(h, 3)
    arrived("qc", qg.at[0])

    def tile_rows(cq, ck):
        return pl.ds(TILE_AT[cq] + (ck - key_chunks(cq)[0]) * KROWS, KROWS)

    def queries(t, cq):
        return qg[t, cq].reshape(QROWS, HEAD)

    def keys(t, at, cks):
        return stack_rows(
            [kv[ck // 4, at[ck // 4], :, t, ck % 4].reshape(KROWS, HEAD) for ck in cks]
        )

    st, e_ref, dp_ref = b["st"], b["e"], b["dp"]

    def first_pass(s, carry):
        late = lax.div(s, 2)
        off = (1 - late) * s + late * (5 - s)

        @pl.when(s == 1)
        def _():
            for n in range(4):
                for h in range(2):
                    forward_unit(h, n)

        @pl.when(s == 3)
        def _():
            arrived("qf", kv.at[0, pl.ds(0, 2)])
            forward_input()
            for t in range(2):
                for copy in send_matrix(t):
                    send(*copy)

        at = (turn(y, off), turn(x, off))
        for cq in range(CHUNKS):
            cks = key_chunks(cq)
            scores = dot_tt(keys(0, at, cks), queries(0, cq))
            dprobs = dot_tt(keys(1, at, cks), queries(1, cq))
            qpos = b["qp"][cq : cq + 1, :]
            for n, ck in enumerate(cks):
                part = slice(n * KROWS, (n + 1) * KROWS)
                score, dprob = scores[part] * SCALE2, dprobs[part]
                if ck == cq or ck == cq - BAND:
                    kpb = b["kpb"][ck // 4 * 16 + at[ck // 4] * 4 + ck % 4]
                    kpos = jnp.concatenate([kpb, kpb], axis=1)
                    seen = kpos <= qpos if ck == cq else kpos > qpos - WINDOW
                    score = jnp.where(seen, score, MASKED)
                top = jnp.max(score, axis=0, keepdims=True)
                expo = jnp.exp2(score - top)
                rows = tile_rows(cq, ck)
                e_ref[off, rows, :] = expo
                dp_ref[off, rows, :] = dprob
                row = slice(cq, cq + 1)
                st[0, off, cq - ck, row, :] = top
                st[1, off, cq - ck, row, :] = jnp.sum(expo, axis=0, keepdims=True)
                st[2, off, cq - ck, row, :] = jnp.sum(expo * dprob, axis=0, keepdims=True)
        return carry

    lax.fori_loop(0, 4, first_pass, 0)
    ss, sr = b["ss"], b["sr"]
    top_l = jnp.max(st[0], axis=(0, 1))
    fac_l = jnp.exp2(st[0] - top_l[None, None])
    sum_l = jnp.sum(st[1] * fac_l, axis=(0, 1))
    wgt_l = jnp.sum(st[2] * fac_l, axis=(0, 1))
    ss[0] = top_l
    ss[1] = sum_l
    ss[2] = wgt_l
    send("stat", 0, ss, sr, d_core)

    arrived("stat", sr)
    top = jnp.maximum(top_l, sr[0])
    mine_f = jnp.exp2(top_l - top)
    other_f = jnp.exp2(sr[0] - top)
    total = sum_l * mine_f + sr[1] * other_f
    b["delta"][...] = (wgt_l * mine_f + sr[2] * other_f) / total
    b["fac"][...] = fac_l * (mine_f / total)[None, None]

    offs = (2, 1, 3, 0)

    def reducer(name, unit_at, deliver=None):
        far, rfar = b[name + "_far"], b[name + "_rfar"]
        near, rnear = b[name + "_near"], b[name + "_rnear"]
        far2, rfar2 = b[name + "_far2"], b[name + "_rfar2"]
        near2, rnear2 = b[name + "_near2"], b[name + "_rnear2"]

        def place(h, n):
            return turn(pi[h], offs[n])

        def far_copy(h, n, side):
            p = place(h, n)
            return (
                (name, "far", n, side),
                h,
                far.at[h, p, side],
                rfar.at[h, side, p],
                q_to[h][side],
            )

        def near_copy(h, n, side):
            p = place(h, n)
            return (
                (name, "near", n),
                (h, side),
                near.at[h, side, p],
                rnear.at[h, side, p],
                q_to[h][side],
            )

        def start_far():
            for n in range(4):
                for h in range(2):
                    p = place(h, n)
                    far[h, p] = unit_at(h, turn(qi[h], 2), p, 0).astype(BF16)
                    for side in range(2):
                        send(*far_copy(h, n, side))

        def start_near(n):
            for side in (1, 0):
                arrived((name, "far", n, side), rfar.at[0, side, pl.ds(0, 2)])
                for h in range(2):
                    p = place(h, n)
                    value = unit_at(h, turn(qi[h], 1 if side == 0 else 3), p, 1 - side)
                    near[h, side, p, 1 - side] = value[1 - side].astype(BF16)
                    near[h, side, p, side] = (value[side] + rfar[h, side, p].astype(F32)).astype(
                        BF16
                    )
                    send(*near_copy(h, n, side))

        def own_unit(n):
            out = []
            arrived((name, "near", n), rnear.at[0, 0])
            for h in range(2):
                p = place(h, n)
                value = (
                    unit_at(h, qi[h], p, 0)
                    + rnear[h, 0, p].astype(F32)
                    + rnear[h, 1, p].astype(F32)
                )
                if deliver:
                    deliver(h, n, value.astype(BF16))
                elif n == 0:
                    far2[h] = value.astype(BF16)
                    send((name, "p", h), 2, far2.at[h], rfar2.at[h], p_far[h])
                elif n < 3:
                    side = n - 1
                    near2[h, side] = value.astype(BF16)
                    send(
                        (name, "p", h),
                        side,
                        near2.at[h, side],
                        rnear2.at[h, side],
                        p_to[h][side],
                    )
                else:
                    arrived((name, "p", h), rnear.at[0, 0, pl.ds(0, 3)])
                    out.append(
                        (value + rfar2[h].astype(F32))
                        + (rnear2[h, 0].astype(F32) + rnear2[h, 1].astype(F32))
                    )
            return out

        return start_far, start_near, own_unit

    acc = b["acc"]
    start_far, start_near, own_unit = reducer(
        "a", lambda h, q, p, slot: acc[slot, h, p]
    )

    fac, delta, kt = b["fac"], b["delta"], b["kt"]

    def second_pass(s, carry):
        late = lax.div(s, 2)
        off = (1 - late) * (2 + s) + late * (3 - s)
        slot = late * (3 - s)
        for ck in range(CHUNKS):
            probs, dscores = [], []
            cqs = [cq for cq in range(CHUNKS) if ck in key_chunks(cq)]
            for cq in cqs:
                rows = tile_rows(cq, ck)
                prob = e_ref[off, rows, :] * fac[off, cq - ck, cq : cq + 1, :]
                dscore = prob * (dp_ref[off, rows, :] - delta[cq : cq + 1, :])
                e_ref[off, rows, :] = dscore
                probs.append(prob.astype(BF16))
                dscores.append(dscore.astype(BF16))
            for t, parts in enumerate((dscores, probs)):
                depth = qg[t, ck : ck + len(cqs)].reshape(len(cqs) * QROWS, HEAD)
                grad = dot_nn(jnp.concatenate(parts, axis=1), depth)
                acc[slot, ck // 4, :, t, ck % 4] = grad.reshape(4, 2, 16, HEAD)

        @pl.when(s == 0)
        def _():
            start_far()

        @pl.when(s == 2)
        def _():
            for n in range(4):
                start_near(n)

        return carry

    lax.fori_loop(0, 4, second_pass, 0)
    dqf, dqr, dqs = b["dqf"], b["dqr"], b["dqs"]
    own_unit(0)
    wait_input()
    xt, xo = b["xt"], b["xo"]

    def flip_input(i, carry):
        for n in range(4):
            at = i * 4 + n
            block = xg[:, :, :, lanes(at * 128)].reshape(256, 128)
            xt[at] = block.T.reshape(2, 64, 256)
        return carry

    lax.fori_loop(0, 8, flip_input, 0)
    send("xt", 0, xt.at[:, oc], xo, d_core)
    own_unit(1)
    own_unit(2)
    for off in range(4):
        at = (turn(y, off), turn(x, off))
        for ck in range(CHUNKS):
            kt[off, ck] = keys(0, at, [ck]).T
    for cq in range(CHUNKS):
        cks = key_chunks(cq)
        rows = pl.ds(TILE_AT[cq], KROWS * len(cks))
        flipped = jnp.concatenate([kt[off, ck] for off in range(4) for ck in cks], axis=1)
        dscore = jnp.concatenate([e_ref[off, rows, :].astype(BF16) for off in range(4)], axis=0)
        dqf[cq] = (dot_nn(flipped, dscore).T * SCALE).reshape(2, 2, GROUP, 16, HEAD)
    send("dqc", 0, dqf.at[:, :, oc], dqr, d_core)
    d2, d2o, dd = b["d2"], b["d2o"], b["dd"]
    for h, value in enumerate(own_unit(3)):
        d2[0, 4 * h : 4 * h + 4] = (value[0] * SCALE).astype(BF16)
        d2[1, 4 * h : 4 * h + 4] = value[1].astype(BF16)
    send("d2", 0, d2, d2o, d_core)
    for r, (dev, other) in enumerate(across):
        for t in range(2):
            send("dz", (t, r), d2.at[t, :, other], dd.at[0, t, zh], dev)
    for t in range(2):
        send("dy", t, d2.at[t, :, oh], dd.at[1, t, zh], d_zh)
        dd[1, t, zh] = d2[t, :, zh]

    wown = b["wown"]

    def grad_cols(ref):
        return jnp.concatenate([ref[0].reshape(256, HEAD), ref[1].reshape(256, HEAD)], axis=1)

    def weight_blocks(first):
        cols = grad_cols(d2 if first else d2o)

        def body(i, carry):
            for wy in (2 * i, 2 * i + 1):
                rows = (xt[pl.ds(wy * 8, 8), core] if first else xo[pl.ds(wy * 8, 8)]).reshape(512, 256)
                part = dot_nn(rows, cols)
                for wz in range(2):
                    for wx in range(4):
                        for h, (wq, wp) in enumerate(((wy, wx), (wx, wy))):
                            base = (wz * 4 + wx) * 64
                            block = part[base : base + 64, h * HEAD : (h + 1) * HEAD]
                            if first:
                                wown[h, wq, wp, wz] = block
                            else:
                                wown[h, wq, wp, wz] = wown[h, wq, wp, wz] + block
            return carry

        lax.fori_loop(0, 2, body, 0)

    def far_blocks(first):
        cols = d2 if first else d2o
        fy, fx = turn(y, 2), turn(x, 2)

        def block(i, count):
            return xt[pl.ds(i, count), core] if first else xo[pl.ds(i, count)]

        rows = (
            block(fy * 8, 8).reshape(512, 256),
            jnp.concatenate([block(n * 4 + fx, 1).reshape(64, 256) for n in range(8)], axis=0),
        )
        for h in range(2):
            part = dot_nn(rows[h], cols[h].reshape(256, HEAD))
            for n in range(8):
                piece = part[n * 64 : (n + 1) * 64]
                at = (0, fy, n % 4, n // 4) if h == 0 else (1, fx, n // 2, n % 2)
                wown[at] = piece if first else wown[at] + piece

    far_blocks(True)
    arrived("xt", xo)
    arrived("d2", d2o)
    far_blocks(False)
    def deliver(h, n, value):
        kind, ref, hop = (
            (3, b["w_far2"].at[h], p_far[h]),
            (1, b["w_near2"].at[h, 0], p_to[h][0]),
            (2, b["w_near2"].at[h, 1], p_to[h][1]),
            (0, b["wmine"].at[h], {}),
        )[n]
        ref[...] = value
        for r, (dev, other) in enumerate(across):
            send("ws", (kind, h, r), ref.at[other], w_out.at[kind, h, zh], {**hop, **dev})

    w_far, w_near, w_unit = reducer("w", lambda h, q, p, slot: wown[h, q, p], deliver)
    w_far()
    weight_blocks(True)
    arrived("dqc", dqr)
    for n in range(2):
        dqs[n] = (dqf[:, n, core] + dqr[:, n]).astype(BF16)
    for r, (dev, other) in enumerate(across):
        send("dqz", r, dqs.at[other], dq_out.at[zh], dev)
    weight_blocks(False)

    for n in range(4):
        w_near(n)
    for c in own_m:
        c.wait()
    arrived("m", mat.at[1, 0])
    for t in range(2):
        for r in range(2):
            src = matrix_part(t, r, core)
            send("mc", (t, r), src, src, d_core)
    for n in range(4):
        w_unit(n)
    arrived("dz", dd.at[0])
    arrived("dy", dd.at[1, :, oh])
    arrived("mc", mat.at[1, 0])

    def tokens(which, t):
        return jnp.concatenate(
            [dd[which, t, a].reshape(128, HEAD) for a in range(2)], axis=1
        )

    token_grads = jnp.concatenate([tokens(w, t) for w in range(2) for t in range(2)], axis=1)

    def input_block(i, carry):
        rows = pl.ds(pl.multiple_of(i * 512, 512), 512)
        cols = jnp.concatenate([mat[w, t, rows, :] for w in range(2) for t in range(2)], axis=1)
        ig_out[:, lanes(i * 512, 512)] = dot_tt(token_grads, cols).astype(BF16)
        return carry

    lax.fori_loop(0, 4, input_block, 0)
    arrived("dqz", dq_out)
    arrived("ws", w_out)

    for group, kib in enumerate(filled):
        size_of = e_ref.at[0, pl.ds(0, kib), :]
        pltpu.make_async_copy(size_of, size_of, ssem.at[group]).wait()
    assert len(names) <= NSEM and len(local_names) <= NLOCAL


def finish(dq_in, ig_in, w_in, dq_out, ig_out, kw_out, vw_out, dq, kv_w, sems):
    whole = [
        pltpu.make_async_copy(ig_in, ig_out, sems.at[0]),
        pltpu.make_async_copy(dq, dq_out, sems.at[1]),
        pltpu.make_async_copy(kv_w.at[0], kw_out, sems.at[2]),
        pltpu.make_async_copy(kv_w.at[1], vw_out, sems.at[3]),
    ]
    whole[0].start()
    for kvh in range(2):
        for g in range(GROUP):
            at = (kvh * GROUP + g) * HEAD
            dq[:, :, at : at + HEAD] = dq_in[kvh, :, g]
    whole[1].start()
    for t in range(2):
        for n in range(2):
            parts = [w_in[kind, t, n].astype(F32) for kind in range(4)]
            kv_w[t, :, n * HEAD : (n + 1) * HEAD] = (parts[0] + parts[1]) + (parts[2] + parts[3])
        whole[2 + t].start()
    for c in whole:
        c.wait()


def local_step(q, k, v, g, x, mk, mv, placement):
    anywhere = pl.BlockSpec(memory_space=pl.ANY)
    vmem = pl.BlockSpec(memory_space=pltpu.VMEM)
    dq, ig, w = pl.pallas_call(
        kernel,
        out_shape=(
            pltpu.VMEM((2, CHUNKS, GROUP, 16, HEAD), BF16),
            pltpu.VMEM((128, FEATS // 2), BF16),
            pltpu.VMEM((4, 2, 2, 64, HEAD), BF16),
        ),
        in_specs=[anywhere] * 8,
        out_specs=(vmem,) * 3,
        scratch_shapes=[pltpu.VMEM(shape, dtype) for shape, dtype in BUFFERS.values()]
        + [
            pltpu.SemaphoreType.DMA((NSEND,)),
            pltpu.SemaphoreType.DMA((NSEM,)),
            pltpu.SemaphoreType.DMA((NLOCAL,)),
            pltpu.SemaphoreType.REGULAR,
        ],
        compiler_params=pltpu.CompilerParams(
            collective_id=0, has_side_effects=True, vmem_limit_bytes=65 * 1000 * 1000
        ),
    )(
        q.reshape(CHUNKS, 16, -1),
        g.reshape(CHUNKS, 16, -1),
        k.reshape(CHUNKS, 16, -1),
        v.reshape(CHUNKS, 16, -1),
        x.reshape(CHUNKS, 16, -1),
        mk,
        mv,
        placement,
    )
    query_grad, *rest = pl.pallas_call(
        finish,
        out_shape=(
            jax.ShapeDtypeStruct((CHUNKS, 16, 2 * GROUP * HEAD), BF16),
            jax.ShapeDtypeStruct((128, FEATS // 2), BF16),
            jax.ShapeDtypeStruct((64, 2 * HEAD), F32),
            jax.ShapeDtypeStruct((64, 2 * HEAD), F32),
        ),
        in_specs=[vmem] * 3,
        out_specs=(anywhere,) * 4,
        scratch_shapes=[
            pltpu.VMEM((CHUNKS, 16, 2 * GROUP * HEAD), BF16),
            pltpu.VMEM((2, 64, 2 * HEAD), F32),
            pltpu.SemaphoreType.DMA((4,)),
        ],
    )(*[pltpu.with_memory_space_constraint(a, pltpu.VMEM) for a in (dq, ig, w)])
    return (query_grad.reshape(128, -1), *rest)


def solution(mesh):
    torus = Mesh(
        mesh.devices.reshape(4, 2, 4, 2, mesh.shape["tp"]), ("seq_0", "seq_1", "seq_2", "seq_3", "tp")
    )
    rows = P(SEQ, "tp")
    return jax.shard_map(
        local_step,
        mesh=torus,
        in_specs=(rows, rows, rows, rows, rows, P(None, "tp"), P(None, "tp"), P()),
        out_specs=(rows, rows, rows, rows),
        check_vma=False,
    )
```
